32 devices in a mesh: dp: 8 (over z, x), tensor: 4 (over y, core).
Axes of the slice: x: 2, y: 2, z: 4, core: 2. Of those that a mesh axis runs over, the one named last changes fastest.
Arguments:
- tokens: bfloat16 [8192, 1024], P('dp'), may hold values from -6 to 6
- memory: bfloat16 [8192, 1024], P('dp'), may hold values from -6 to 6
- decoder_length: int32 [8], P('dp'), may hold values from 512 to 1024, as said below
- memory_length: int32 [8], P('dp'), may hold values from 512 to 1024, as said below
- self_query: bfloat16 [1024, 1024], P(None, 'tensor'), may hold values from -0.1875 to 0.1875
- self_key: bfloat16 [1024, 1024], P(None, 'tensor'), may hold values from -0.1875 to 0.1875
- self_value: bfloat16 [1024, 1024], P(None, 'tensor'), may hold values from -0.1875 to 0.1875
- self_output: bfloat16 [1024, 1024], P('tensor'), may hold values from -2 to 2
- self_gain: float32 [1024], replicated, may hold values from 0.5 to 1.5
- self_bias: float32 [1024], replicated, may hold values from -3 to 3
- cross_query: bfloat16 [1024, 1024], P(None, 'tensor'), may hold values from -0.1875 to 0.1875
- cross_key: bfloat16 [1024, 1024], P(None, 'tensor'), may hold values from -0.1875 to 0.1875
- cross_value: bfloat16 [1024, 1024], P(None, 'tensor'), may hold values from -0.1875 to 0.1875
- cross_output: bfloat16 [1024, 1024], P('tensor'), may hold values from -2 to 2
- cross_gain: float32 [1024], replicated, may hold values from 0.5 to 1.5
- cross_bias: float32 [1024], replicated, may hold values from -3 to 3
- feed_in: bfloat16 [1024, 4096], P(None, 'tensor'), may hold values from -0.1875 to 0.1875
- feed_out: bfloat16 [4096, 1024], P('tensor'), may hold values from -0.09375 to 0.09375
- feed_gain: float32 [1024], replicated, may hold values from 0.5 to 1.5
- feed_bias: float32 [1024], replicated, may hold values from -3 to 3
- cotangent: bfloat16 [8192, 1024], P('dp'), may hold values from -6 to 6
Outputs:
- output: bfloat16 [8192, 1024], P('dp')
- tokens_grad: float32 [8192, 1024], P('dp')
- memory_grad: float32 [8192, 1024], P('dp')
- self_query_grad: float32 [1024, 1024], P(None, 'tensor')
- self_key_grad: float32 [1024, 1024], P(None, 'tensor')
- self_value_grad: float32 [1024, 1024], P(None, 'tensor')
- self_output_grad: float32 [1024, 1024], P('tensor')
- self_gain_grad: float32 [1024], replicated
- self_bias_grad: float32 [1024], replicated
- cross_query_grad: float32 [1024, 1024], P(None, 'tensor')
- cross_key_grad: float32 [1024, 1024], P(None, 'tensor')
- cross_value_grad: float32 [1024, 1024], P(None, 'tensor')
- cross_output_grad: float32 [1024, 1024], P('tensor')
- cross_gain_grad: float32 [1024], replicated
- cross_bias_grad: float32 [1024], replicated
- feed_in_grad: float32 [1024, 4096], P(None, 'tensor')
- feed_out_grad: float32 [4096, 1024], P('tensor')
- feed_gain_grad: float32 [1024], replicated
- feed_bias_grad: float32 [1024], replicated
The draws below stay inside these ranges and needn't reach their ends.
Inputs may be any that keep to these rules, and one draw needn't show every extreme that they name: Each item's decoder rows in use are its first decoder_length rows; some item uses all 1024. Each item's memory rows in use are its first memory_length rows; some item uses all 1024.
All inputs are finite; a program needn't handle non-finite values.
Results may differ from the reference program's by a relative error of at most 0.04.
Values may be sent and summed in bfloat16 or wider, within the bound.
A program may use at most 192 MiB of HBM per device.

```python
import jax
import jax.numpy as jnp
from jax import lax

D = 1024
HEADS = 16
HD = 64
FF = 4096
LEN = 1024
MEM = 1024
ITEMS = 8
TOKENS = 8192
MEMORY = 8192
N_TENSOR = 4


def length_draw(key, longest):
    values = jax.random.randint(key, (ITEMS,), longest // 2, longest + 1, dtype=jnp.int32)
    chosen = jax.random.randint(jax.random.fold_in(key, 7), (), 0, ITEMS, dtype=jnp.int32)
    return jnp.where(jnp.arange(ITEMS, dtype=jnp.int32) == chosen, longest, values).astype(jnp.int32)


def draw_decoder_length(key, part):
    return length_draw(jax.random.fold_in(key, 11), LEN)


def draw_memory_length(key, part):
    return length_draw(jax.random.fold_in(key, 23), MEM)


def steps_of(own_key, extent, pieces, smallest, top_value):
    loudness, own = 1.0, jax.random.fold_in(own_key, 6)
    for position, blocks in pieces:
        draws = jnp.exp(jax.random.uniform(jax.random.fold_in(own, position), (blocks,), jnp.float32, smallest / len(pieces), top_value / len(pieces)))
        loudness = loudness * jnp.repeat(draws, extent[position] // blocks).reshape([-1 if axis == position else 1 for axis in range(len(extent))])
    return loudness


def scatter_about(stream_key, extent, deviation, reach, shards=(), held_as=jnp.bfloat16):
    array = deviation * jax.random.normal(stream_key, extent, jnp.float32)
    if shards:
        array = array * steps_of(stream_key, extent, shards, -0.22, 0.18)
    return jnp.clip(array, -reach, reach).astype(held_as)


def setup_inputs(seed: int = 0) -> dict:
    splits = jax.random.split(jax.random.key(seed), 22)
    tokens = scatter_about(splits[0], (TOKENS, D), 1.0, 6.0, ((0, 8),))
    memory = scatter_about(splits[1], (MEMORY, D), 1.0, 6.0, ((0, 8),))
    decoder_length = draw_decoder_length(jax.random.fold_in(splits[21], 71), 0)
    memory_length = draw_memory_length(jax.random.fold_in(splits[21], 71), 0)
    self_query = scatter_about(splits[4], (D, D), D ** -0.5, 0.1875, ((1, 4),))
    self_key = scatter_about(splits[5], (D, D), D ** -0.5, 0.1875, ((1, 4),))
    self_value = scatter_about(splits[6], (D, D), D ** -0.5, 0.1875, ((1, 4),))
    self_output = scatter_about(splits[7], (D, D), (max(D // 128, 1)) ** -0.5, 2.0, ((0, 4),))
    self_gain = jnp.clip(1.0 + 0.1 * jax.random.normal(splits[8], (D,), jnp.float32), 0.5, 1.5)
    self_bias = scatter_about(splits[9], (D,), 0.5, 3.0, (), jnp.float32)
    cross_query = scatter_about(splits[10], (D, D), D ** -0.5, 0.1875, ((1, 4),))
    cross_key = scatter_about(splits[11], (D, D), D ** -0.5, 0.1875, ((1, 4),))
    cross_value = scatter_about(splits[12], (D, D), D ** -0.5, 0.1875, ((1, 4),))
    cross_output = scatter_about(splits[13], (D, D), (max(D // 128, 1)) ** -0.5, 2.0, ((0, 4),))
    cross_gain = jnp.clip(1.0 + 0.1 * jax.random.normal(splits[14], (D,), jnp.float32), 0.5, 1.5)
    cross_bias = scatter_about(splits[15], (D,), 0.5, 3.0, (), jnp.float32)
    feed_in = scatter_about(splits[16], (D, FF), D ** -0.5, 0.1875, ((1, 4),))
    feed_out = scatter_about(splits[17], (FF, D), FF ** -0.5, 0.09375, ((0, 4),))
    feed_gain = jnp.clip(1.0 + 0.1 * jax.random.normal(splits[18], (D,), jnp.float32), 0.5, 1.5)
    feed_bias = scatter_about(splits[19], (D,), 0.5, 3.0, (), jnp.float32)
    cotangent = scatter_about(splits[20], (TOKENS, D), 1.0, 6.0, ((0, 8),))
    return {"tokens": tokens, "memory": memory, "decoder_length": decoder_length, "memory_length": memory_length, "self_query": self_query, "self_key": self_key, "self_value": self_value, "self_output": self_output, "self_gain": self_gain, "self_bias": self_bias, "cross_query": cross_query, "cross_key": cross_key, "cross_value": cross_value, "cross_output": cross_output, "cross_gain": cross_gain, "cross_bias": cross_bias, "feed_in": feed_in, "feed_out": feed_out, "feed_gain": feed_gain, "feed_bias": feed_bias, "cotangent": cotangent}


EPSILON = 1e-05
NEGATIVE = -1e+30
HIGH = lax.Precision.HIGHEST

@jax.custom_vjp
def low(v):
    return lax.optimization_barrier(v.astype(jnp.bfloat16)).astype(jnp.float32)

@jax.custom_vjp
def low_back(v):
    return v

def low_keep(v):
    return (low(v), None)

def low_pass(kept, grad):
    return (grad,)

def back_keep(v):
    return (v, None)

def back_low(kept, grad):
    return (low(grad),)
low.defvjp(low_keep, low_pass)
low_back.defvjp(back_keep, back_low)

def matmul_high(left, right):
    return jnp.dot(left, right, precision=HIGH)

def layer_norm(summed, gain, bias):
    center = summed - lax.optimization_barrier(jnp.mean(summed, axis=-1, keepdims=True))
    spread = lax.optimization_barrier(jnp.mean(center * center, axis=-1, keepdims=True))
    return center * lax.rsqrt(spread + EPSILON) * gain + bias

def attention(queries, keys, values, allowed):
    rows = queries.shape[0]
    query_heads = queries.reshape(rows, HEADS, HD)
    key_heads = keys.reshape(keys.shape[0], HEADS, HD)
    value_heads = values.reshape(values.shape[0], HEADS, HD)
    scores = low_back(jnp.einsum('qhd,khd->hqk', query_heads, key_heads, precision=HIGH) * HD ** (-0.5))
    scores = jnp.where(allowed[None], scores, NEGATIVE)
    shares = jax.nn.softmax(scores, axis=-1)
    mixed = jnp.einsum('hqk,khd->qhd', low(shares), value_heads, precision=HIGH)
    return low(low_back(mixed.reshape(rows, HEADS * HD)))

def branch_sum(mixed, weight):
    rows = mixed.shape[0]
    terms = jnp.einsum('rgc,gce->gre', mixed.reshape(rows, N_TENSOR, -1), weight.reshape(N_TENSOR, -1, weight.shape[1]), precision=HIGH)
    return low_back(lax.optimization_barrier(jnp.sum(low(terms), axis=0)))

def forward(weights, tokens, memory, self_allowed, cross_allowed):
    self_query, self_key, self_value, self_output, self_gain, self_bias, cross_query, cross_key, cross_value, cross_output, cross_gain, cross_bias, feed_in, feed_out, feed_gain, feed_bias = weights
    queries = low(low_back(matmul_high(tokens, self_query)))
    keys_self = low(low_back(matmul_high(tokens, self_key)))
    values_self = low(low_back(matmul_high(tokens, self_value)))
    self_mixed = attention(queries, keys_self, values_self, self_allowed)
    first = layer_norm(tokens + branch_sum(self_mixed, self_output), self_gain, self_bias)
    first_low = low(first)
    cross_queries = low(low_back(matmul_high(first_low, cross_query)))
    cross_keys = low(low_back(matmul_high(memory, cross_key)))
    cross_values = low(low_back(matmul_high(memory, cross_value)))
    cross_mixed = attention(cross_queries, cross_keys, cross_values, cross_allowed)
    second = layer_norm(first + branch_sum(cross_mixed, cross_output), cross_gain, cross_bias)
    hidden_pre = low_back(matmul_high(low(second), feed_in))
    hidden = low(jax.nn.gelu(hidden_pre, approximate=False))
    third_sum = second + branch_sum(hidden, feed_out)
    return layer_norm(third_sum, feed_gain, feed_bias)

def reference(tokens, memory, decoder_length, memory_length, self_query, self_key, self_value, self_output, self_gain, self_bias, cross_query, cross_key, cross_value, cross_output, cross_gain, cross_bias, feed_in, feed_out, feed_gain, feed_bias, cotangent):
    weights = tuple((weight.astype(jnp.float32) for weight in (self_query, self_key, self_value, self_output, self_gain, self_bias, cross_query, cross_key, cross_value, cross_output, cross_gain, cross_bias, feed_in, feed_out, feed_gain, feed_bias)))
    token_items = tokens.astype(jnp.float32).reshape(ITEMS, LEN, D)
    memory_items = memory.astype(jnp.float32).reshape(ITEMS, MEM, D)
    seed_items = cotangent.astype(jnp.float32).reshape(ITEMS, LEN, D)
    row_ids = jnp.arange(LEN, dtype=jnp.int32)
    memory_ids = jnp.arange(MEM, dtype=jnp.int32)

    def one_item(totals, inputs):
        token_rows, memory_rows, decoded, encoded, seed_rows = inputs
        self_allowed = (row_ids[None, :] <= row_ids[:, None]) & (row_ids[None, :] < decoded)
        cross_allowed = jnp.broadcast_to((memory_ids < encoded)[None, :], (LEN, MEM))

        def run(weight_list, token_part, memory_part):
            return forward(weight_list, token_part, memory_part, self_allowed, cross_allowed)
        final, backward = jax.vjp(run, weights, token_rows, memory_rows)
        row_mask = (row_ids < decoded).astype(jnp.float32)[:, None]
        weight_grads, token_grads, memory_grads = backward(seed_rows * row_mask)
        totals = tuple((total + grad for total, grad in zip(totals, weight_grads)))
        return (totals, (final.astype(jnp.bfloat16), token_grads, memory_grads))
    zeros = tuple((jnp.zeros(weight.shape, jnp.float32) for weight in weights))
    totals, (finals, token_grads, memory_grads) = lax.scan(one_item, zeros, (token_items, memory_items, decoder_length, memory_length, seed_items))
    return (finals.reshape(TOKENS, D), token_grads.reshape(TOKENS, D), memory_grads.reshape(MEMORY, D), totals[0], totals[1], totals[2], totals[3], totals[4], totals[5], totals[6], totals[7], totals[8], totals[9], totals[10], totals[11], totals[12], totals[13], totals[14], totals[15])
```

```python
import jax
import jax.numpy as jnp
from jax import lax
from jax.experimental import pallas as pl
from jax.experimental.pallas import tpu as pltpu
from jax.sharding import PartitionSpec as P

BF = jnp.bfloat16
F32 = jnp.float32
HD = 64
CHUNKS = 4
EPSILON = 1e-05
NEGATIVE = -1e30
MESH = pl.DeviceIdType.MESH
STAGES = 7


def mm(a, b):
    return lax.dot_general(a, b, (((1,), (0,)), ((), ())), preferred_element_type=F32)


def mt(a, b):
    return lax.dot_general(a, b, (((1,), (1,)), ((), ())), preferred_element_type=F32)


def tm(a, b):
    return lax.dot_general(a, b, (((0,), (0,)), ((), ())), preferred_element_type=F32)


def layout(rows, slots, width, inner, hidden):
    heads = inner // HD
    chunk = rows // CHUNKS
    half, own = chunk // 2, chunk // 4
    v = pltpu.VMEM
    return dict(
        tok=v((rows, width), BF),
        mem=v((slots, width), BF),
        cot=v((CHUNKS, own, width), BF),
        wq=v((width, inner), BF),
        wk=v((width, inner), BF),
        wv=v((width, inner), BF),
        wo=v((inner, width), BF),
        cwq=v((width, inner), BF),
        cwk=v((width, inner), BF),
        cwv=v((width, inner), BF),
        cwo=v((inner, width), BF),
        win=v((width, hidden), BF),
        wout=v((hidden, width), BF),
        q=v((rows, inner), BF),
        k=v((rows, inner), BF),
        v=v((rows, inner), BF),
        kt=v((heads, HD, rows), BF),
        vt=v((heads, HD + 16, rows), BF),
        cq=v((rows, inner), BF),
        ck=v((slots, inner), BF),
        cv=v((slots, inner), BF),
        ckt=v((heads, HD, slots), BF),
        cvt=v((heads, HD + 16, slots), BF),
        mixed=v((rows, inner), BF),
        cmixed=v((rows, inner), BF),
        lse=v((CHUNKS, heads, 1, chunk), F32),
        clse=v((CHUNKS, heads, 1, chunk), F32),
        delta=v((heads, 1, chunk), F32),
        flat=v((inner, chunk), F32),
        dout=v((chunk, inner), BF),
        dk=v((rows, inner), F32),
        dv=v((rows, inner), F32),
        hid=v((rows, hidden), BF),
        slope=v((rows, hidden), BF),
        low0=v((rows, width), BF),
        low1=v((rows, width), BF),
        low2=v((rows, width), BF),
        low3=v((rows, width), BF),
        low4=v((rows, width), BF),
        outs=v((rows, width), BF),
        res=v((CHUNKS, own, width), F32),
        xh1=v((CHUNKS, own, width), F32),
        xh2=v((CHUNKS, own, width), F32),
        rs1=v((CHUNKS, own, 1), F32),
        rs2=v((CHUNKS, own, 1), F32),
        part=v((CHUNKS, chunk, width), BF),
        rc=v((CHUNKS, half, width), BF),
        ys=v((CHUNKS, half, width), BF),
        ry=v((CHUNKS, own, width), BF),
        vacc=v((8, 8, width), F32),
        gbuf=v((2 * hidden + 2 * width, width), BF),
        insem=pltpu.SemaphoreType.DMA((16,)),
        cotsem=pltpu.SemaphoreType.DMA((CHUNKS,)),
        osem=pltpu.SemaphoreType.DMA((4,)),
        ssem=pltpu.SemaphoreType.DMA((8, CHUNKS)),
        rsem=pltpu.SemaphoreType.DMA((8, CHUNKS)),
    )


INPUTS = (
    "tok", "wk", "wv", "wq", "wo", "mem", "cwk", "cwv", "cwq", "cwo",
    "win", "wout",
)


def layer_kernel(names, lens, vec, *refs):
    n_in = len(INPUTS)
    srcs = dict(zip(INPUTS, refs[:n_in]))
    cot_h = refs[n_in]
    out_h, tg_h, mg_h, g_h, vg_h = refs[n_in + 1:n_in + 6]
    S = dict(zip(names, refs[n_in + 6:]))

    rows, width = S["tok"].shape
    slots = S["mem"].shape[0]
    inner = S["wq"].shape[1]
    hidden = S["win"].shape[1]
    heads = inner // HD
    R = rows // CHUNKS
    HF, Q = R // 2, R // 4
    scale = HD ** -0.5
    t = lax.axis_index("tensor")
    yy = t // 2
    kk = t % 2
    core = {"tensor": t + 1 - 2 * kk}
    ypar = {"tensor": t + 2 - 4 * yy}

    def row(c):
        return pl.ds(pl.multiple_of(c * R, R), R)

    def own_rows(c):
        return pl.ds(pl.multiple_of(c * R + kk * HF + yy * Q, Q), Q)

    def y_rows(c):
        return pl.ds(pl.multiple_of(c * R + kk * HF + (1 - yy) * Q, Q), Q)

    loads = {n: pltpu.make_async_copy(srcs[n], S[n], S["insem"].at[j])
             for j, n in enumerate(INPUTS)}
    cots = [pltpu.make_async_copy(cot_h.at[own_rows(c)], S["cot"].at[c], S["cotsem"].at[c])
            for c in range(CHUNKS)]
    for n in INPUTS:
        loads[n].start()
    for c in cots:
        c.start()

    barrier = pltpu.get_barrier_semaphore()
    for peer in (core, ypar):
        pl.semaphore_signal(barrier, inc=1, device_id=peer, device_id_type=MESH)

    S["vt"][:, HD:, :] = jnp.ones((heads, 16, rows), BF)
    S["cvt"][:, HD:, :] = jnp.ones((heads, 16, slots), BF)
    S["vacc"][...] = jnp.zeros(S["vacc"].shape, F32)

    def wait_for(*which):
        for n in which:
            loads[n].wait()

    def project(src, wk, wv, kd, vd, ktd, vtd, count):
        def body(i, carry):
            r = row(i)
            x = src[r, :]
            kf = mm(x, wk[...])
            kd[r, :] = kf.astype(BF)
            kt = kf.T.astype(BF)
            vf = mm(x, wv[...])
            vd[r, :] = vf.astype(BF)
            vtt = vf.T.astype(BF)
            for h in range(heads):
                ktd[h, :, r] = kt[h * HD:(h + 1) * HD, :]
                vtd[h, :HD, r] = vtt[h * HD:(h + 1) * HD, :]
            return carry
        lax.fori_loop(0, count, body, 0)

    def project_q(src, w, dst):
        def body(i, carry):
            dst[row(i), :] = mm(src[row(i), :], w[...]).astype(BF)
            return carry
        lax.fori_loop(0, CHUNKS, body, 0)

    def lanes(h):
        return pl.ds(pl.multiple_of((h // 2) * 2 * HD, 2 * HD), 2 * HD)

    def pick(x, h):
        lane = lax.broadcasted_iota(jnp.int32, x.shape, 1) // HD
        return jnp.where(lane == h % 2, x, jnp.zeros_like(x))

    def masked(scores, c, causal, length):
        kid = lax.broadcasted_iota(jnp.int32, scores.shape, 0)
        ok = kid < length
        if causal:
            qid = c * R + lax.broadcasted_iota(jnp.int32, scores.shape, 1)
            ok = ok & (kid <= qid)
        return jnp.where(ok, scores * scale, NEGATIVE)

    def head_forward(h, c, q, k, vt, lse, causal, length):
        qm = pick(q[row(c), lanes(h)], h)
        s = masked(mt(k[:, lanes(h)], qm), c, causal, length)
        top = jnp.max(s, axis=0, keepdims=True)
        p = jnp.exp(s - top).astype(BF)
        o = mm(vt[h], p)
        total = o[HD:HD + 1, :]
        S["flat"][pl.ds(pl.multiple_of(h * HD, HD), HD), :] = o[:HD, :] / total
        lse[c, h] = top + jnp.log(total)

    def head_backward(h, c, q, k, v, kt, lse, causal, length):
        qm = pick(q[row(c), lanes(h)], h)
        s = masked(mt(k[:, lanes(h)], qm), c, causal, length)
        p = jnp.exp(s - lse[c, h])
        dom = pick(S["dout"][:, lanes(h)], h)
        dp = mt(v[:, lanes(h)], dom)
        S["dv"][:, lanes(h)] += mm(p.astype(BF), dom)
        ds = (p * (dp - S["delta"][h])).astype(BF)
        S["dk"][:, lanes(h)] += mm(ds, qm)
        S["flat"][pl.ds(pl.multiple_of(h * HD, HD), HD), :] = mm(kt[h], ds) * scale

    def unflatten():
        return S["flat"][...].T

    def wide(fn, dst, c):
        block = min(256, width)

        def body(j, carry):
            cols = pl.ds(pl.multiple_of(j * block, block), block)
            dst[c, :, cols] = fn(cols).astype(BF)
            return carry
        lax.fori_loop(0, width // block, body, 0)

    def set_delta(c, mixed, low, w):
        do = mt(low[row(c), :], w[...]).astype(BF)
        S["dout"][...] = do
        prod = do.astype(F32) * mixed[row(c), :].astype(F32)
        sel = (lax.broadcasted_iota(jnp.int32, (8, inner), 1) // HD
               == lax.broadcasted_iota(jnp.int32, (8, inner), 0)).astype(F32)
        d = lax.dot_general(sel, prod, (((1,), (1,)), ((), ())),
                            precision=lax.Precision.HIGHEST, preferred_element_type=F32)
        for h in range(heads):
            S["delta"][h] = d[h:h + 1, :]

    dec = lens[0]
    enc = lens[1]

    def each_head(fn, middle):
        def body(h, carry):
            @pl.when(h == heads // 2)
            def _():
                middle()
            fn(h)
            return carry
        lax.fori_loop(0, heads, body, 0)

    def compute(s, c, middle):
        part = S["part"]
        if s == 0:
            each_head(lambda h: head_forward(h, c, S["q"], S["k"], S["vt"], S["lse"], True, dec), middle)
            S["mixed"][row(c), :] = unflatten().astype(BF)
            wide(lambda n: mm(S["mixed"][row(c), :], S["wo"][:, n]), part, c)
        elif s == 1:
            S["cq"][row(c), :] = mm(S["low0"][row(c), :], S["cwq"][...]).astype(BF)
            each_head(lambda h: head_forward(h, c, S["cq"], S["ck"], S["cvt"], S["clse"], False, enc), middle)
            S["cmixed"][row(c), :] = unflatten().astype(BF)
            wide(lambda n: mm(S["cmixed"][row(c), :], S["cwo"][:, n]), part, c)
        elif s == 2:
            block = min(256, hidden)

            def body(j, carry):
                n = pl.ds(pl.multiple_of(j * block, block), block)
                v = mm(S["low1"][row(c), :], S["win"][:, n])
                cdf = 0.5 * (1.0 + lax.erf(v * 0.7071067811865476))
                S["hid"][row(c), n] = (v * cdf).astype(BF)
                S["slope"][row(c), n] = (
                    cdf + v * jnp.exp(-0.5 * v * v) * 0.3989422804014327).astype(BF)
                return carry
            lax.fori_loop(0, hidden // block, body, 0)
            middle()
            wide(lambda n: mm(S["hid"][row(c), :], S["wout"][:, n]), part, c)
        elif s == 3:
            block = min(256, hidden)

            def body(j, carry):
                n = pl.ds(pl.multiple_of(j * block, block), block)
                g = mt(S["low2"][row(c), :], S["wout"][n, :])
                S["slope"][row(c), n] = (g * S["slope"][row(c), n].astype(F32)).astype(BF)
                return carry
            lax.fori_loop(0, hidden // block, body, 0)
            middle()
            wide(lambda n: mt(S["slope"][row(c), :], S["win"][n, :]), part, c)
        elif s == 4:
            set_delta(c, S["cmixed"], S["low3"], S["cwo"])
            each_head(lambda h: head_backward(h, c, S["cq"], S["ck"], S["cv"], S["ckt"], S["clse"], False, enc), middle)
            S["cq"][row(c), :] = unflatten().astype(BF)
            wide(lambda n: mt(S["cq"][row(c), :], S["cwq"][n, :]), part, c)
        elif s == 5:
            set_delta(c, S["mixed"], S["low4"], S["wo"])
            each_head(lambda h: head_backward(h, c, S["q"], S["k"], S["v"], S["kt"], S["lse"], True, dec), middle)
            S["q"][row(c), :] = unflatten().astype(BF)
            S["k"][row(c), :] = (S["dk"][row(c), :] * scale).astype(BF)
            S["v"][row(c), :] = S["dv"][row(c), :].astype(BF)
            wide(lambda n: mt(S["q"][row(c), :], S["wq"][n, :])
                 + mt(S["k"][row(c), :], S["wk"][n, :])
                 + mt(S["v"][row(c), :], S["wv"][n, :]), part, c)
        else:
            middle()
            wide(lambda n: mt(S["ck"][row(c), :], S["cwk"][n, :])
                 + mt(S["cv"][row(c), :], S["cwv"][n, :]), part, c)

    lows = [S["low0"], S["low1"], S["low2"], S["low3"], S["low4"], S["low1"], S["low2"]]

    def remote(src, dst, phase, c, peer):
        return pltpu.make_async_remote_copy(
            src_ref=src, dst_ref=dst, send_sem=S["ssem"].at[phase, c],
            recv_sem=S["rsem"].at[phase, c], device_id=peer, device_id_type=MESH)

    def core_part(c):
        theirs = pl.ds(pl.multiple_of((1 - kk) * HF, HF), HF)
        return remote(S["part"].at[c, theirs], S["rc"].at[c], 0, c, core)

    def y_part(c):
        theirs = pl.ds(pl.multiple_of((1 - yy) * Q, Q), Q)
        return remote(S["ys"].at[c, theirs], S["ry"].at[c], 1, c, ypar)

    def gather(buf, c, which, base):
        r = y_rows(c) if which == 2 else own_rows(c)
        return remote(buf.at[r], buf.at[r], base + which, c, ypar if which == 0 else core)

    def p0(c):
        core_part(c).start()

    def p1(c):
        core_part(c).wait()
        step = min(32, HF)

        def body(j, carry):
            r = pl.ds(pl.multiple_of(j * step, step), step)
            m = pl.ds(pl.multiple_of(kk * HF + j * step, step), step)
            S["ys"][c, r, :] = (S["part"][c, m, :].astype(F32)
                                + S["rc"][c, r, :].astype(F32)).astype(BF)
            return carry
        lax.fori_loop(0, HF // step, body, 0)
        y_part(c).start()

    def mean(x):
        return jnp.sum(x, axis=-1, keepdims=True) * (1.0 / width)

    def norm(x, j):
        center = x - mean(x)
        inv = lax.rsqrt(mean(center * center) + EPSILON)
        xhat = center * inv
        return xhat, inv, xhat * vec[2 * j:2 * j + 1, :] + vec[2 * j + 1:2 * j + 2, :]

    def fold(x):
        return jnp.sum(x.reshape(x.shape[0] // 8, 8, width), axis=0)

    def norm_back(e, xhat, inv, j):
        S["vacc"][2 * j] += fold(e * xhat)
        S["vacc"][2 * j + 1] += fold(e)
        eg = e * vec[2 * j:2 * j + 1, :]
        return (eg - mean(eg) - xhat * mean(eg * xhat)) * inv

    def p2(s, c):
        y_part(c).wait()
        if s == 2:
            @pl.when(c == CHUNKS - 1)
            def _():
                for x in cots:
                    x.wait()
        step = min(16, Q)
        buf = lows[s]

        def body(j, carry):
            r = pl.ds(pl.multiple_of(j * step, step), step)
            m = pl.ds(pl.multiple_of(yy * Q + j * step, step), step)
            o = pl.ds(pl.multiple_of(c * R + kk * HF + yy * Q + j * step, step), step)
            x = S["ys"][c, m, :].astype(F32) + S["ry"][c, r, :].astype(F32)
            if s == 0:
                xhat, inv, y = norm(S["tok"][o, :].astype(F32) + x, 0)
                S["xh1"][c, r, :] = xhat
                S["rs1"][c, r, :] = inv
                S["res"][c, r, :] = y
            elif s == 1:
                xhat, inv, y = norm(S["res"][c, r, :] + x, 1)
                S["xh2"][c, r, :] = xhat
                S["rs2"][c, r, :] = inv
                S["res"][c, r, :] = y
            elif s == 2:
                xhat, inv, y = norm(S["res"][c, r, :] + x, 2)
                S["outs"][o, :] = y.astype(BF)
                rid = (c * R + kk * HF + yy * Q + j * step
                       + lax.broadcasted_iota(jnp.int32, (step, width), 0))
                seed = jnp.where(rid < dec, S["cot"][c, r, :].astype(F32), 0.0)
                y = norm_back(seed, xhat, inv, 2)
                S["res"][c, r, :] = y
            elif s == 3:
                y = norm_back(S["res"][c, r, :] + x, S["xh2"][c, r, :], S["rs2"][c, r, :], 1)
                S["res"][c, r, :] = y
            elif s == 4:
                y = norm_back(S["res"][c, r, :] + x, S["xh1"][c, r, :], S["rs1"][c, r, :], 0)
                S["res"][c, r, :] = y
            elif s == 5:
                y = S["res"][c, r, :] + x
            else:
                y = x
            buf[o, :] = y.astype(BF)
            return carry
        lax.fori_loop(0, Q // step, body, 0)
        gather(buf, c, 0, 2).start()
        gather(buf, c, 1, 2).start()
        if s == 2:
            gather(S["outs"], c, 0, 5).start()
            gather(S["outs"], c, 1, 5).start()

    def p3(s, c):
        sets = ((lows[s], 2), (S["outs"], 5)) if s == 2 else ((lows[s], 2),)
        for buf, base in sets:
            gather(buf, c, 0, base).wait()
            gather(buf, c, 2, base).start()

    def p4(s, c):
        sets = ((lows[s], 2), (S["outs"], 5)) if s == 2 else ((lows[s], 2),)
        for buf, base in sets:
            gather(buf, c, 1, base).wait()
            gather(buf, c, 2, base).wait()

    def grad_piece(g, i):
        if g == 0:
            n = pl.ds(pl.multiple_of(i * 256, 256), 256)
            S["gbuf"][pl.ds(pl.multiple_of(i * 256, 256), 256), :] = tm(
                S["hid"][:, n], S["low2"][...]).astype(BF)
        elif g == 1:
            n = pl.ds(pl.multiple_of(i * 256, 256), 256)
            S["gbuf"][pl.ds(pl.multiple_of(hidden + i * 256, 256), 256), :] = tm(
                S["low1"][:, n], S["slope"][...]).astype(BF)
        else:
            n = pl.ds(pl.multiple_of(i * 256, 256), 256)
            r = pl.ds(pl.multiple_of(hidden + (g - 1) * width + i * 256, 256), 256)
            if g == 2:
                a, b, d = S["low0"], S["mem"], S["low3"]
                x, y, z, w = S["cq"], S["ck"], S["cv"], S["cmixed"]
            else:
                a, b, d = S["tok"], S["tok"], S["low4"]
                x, y, z, w = S["q"], S["k"], S["v"], S["mixed"]
            S["gbuf"][r, 0 * inner:1 * inner] = tm(a[:, n], x[...]).astype(BF)
            S["gbuf"][r, 1 * inner:2 * inner] = tm(b[:, n], y[...]).astype(BF)
            S["gbuf"][r, 2 * inner:3 * inner] = tm(b[:, n], z[...]).astype(BF)
            S["gbuf"][r, 3 * inner:4 * inner] = tm(d[:, n], w[...]).astype(BF)

    wait_for("tok", "wk", "wv", "wq")
    project(S["tok"], S["wk"], S["wv"], S["k"], S["v"], S["kt"], S["vt"], CHUNKS)
    project_q(S["tok"], S["wq"], S["q"])
    pl.semaphore_wait(barrier, 2)
    wait_for("wo")

    def lagged(i, lag, fn, s):
        c = lax.rem(CHUNKS - 1 - i + lag, CHUNKS)

        @pl.when(i >= lag)
        def _():
            fn(s, c)
        if s > 0:
            @pl.when(i < lag)
            def _():
                fn(s - 1, c)

    for s in range(STAGES):
        if s == 1:
            wait_for("mem", "cwk", "cwv", "cwq", "cwo")
            project(S["mem"], S["cwk"], S["cwv"], S["ck"], S["cv"], S["ckt"], S["cvt"], CHUNKS)
        if s == 2:
            wait_for("win", "wout")
        if s in (4, 5):
            S["dk"][...] = jnp.zeros(S["dk"].shape, F32)
            S["dv"][...] = jnp.zeros(S["dv"].shape, F32)

        def slot(i, carry, s=s):
            c = CHUNKS - 1 - i
            if s > 0:
                p4(s - 1, c)

            def middle():
                lagged(i, 3, p3, s)
                lagged(i, 2, p2, s)
                if s > 0:
                    p1(lax.rem(c + 1, CHUNKS))
                else:
                    @pl.when(i >= 1)
                    def _():
                        p1(lax.rem(c + 1, CHUNKS))
            compute(s, c, middle)
            p0(c)
            if s == 4:
                grad_piece(0, i)
                grad_piece(1, i)
            elif s == 5:
                grad_piece(2, i)
            elif s == 6:
                grad_piece(3, i)
            return carry
        lax.fori_loop(0, CHUNKS, slot, 0)
        if s == 4:
            S["ck"][...] = (S["dk"][...] * scale).astype(BF)
            S["cv"][...] = S["dv"][...].astype(BF)

    last = STAGES - 1
    g_copy = pltpu.make_async_copy(S["gbuf"], g_h, S["osem"].at[0])
    g_copy.start()
    o_copy = pltpu.make_async_copy(S["outs"], out_h, S["osem"].at[1])
    o_copy.start()

    p1(0)
    p2(last, 1)
    p3(last, 2)
    p2(last, 0)
    p3(last, 1)
    p3(last, 0)
    for c in range(CHUNKS):
        p4(last, CHUNKS - 1 - c)
    t_copy = pltpu.make_async_copy(lows[5], tg_h, S["osem"].at[2])
    t_copy.start()
    m_copy = pltpu.make_async_copy(lows[6], mg_h, S["osem"].at[3])
    m_copy.start()
    vg_h[...] = jnp.sum(S["vacc"][...], axis=1)
    for x in (g_copy, o_copy, t_copy, m_copy):
        x.wait()


def shards(
    tokens, memory, decoder_length, memory_length,
    self_query, self_key, self_value, self_output, self_gain, self_bias,
    cross_query, cross_key, cross_value, cross_output, cross_gain, cross_bias,
    feed_in, feed_out, feed_gain, feed_bias, cotangent,
):
    rows, width = tokens.shape
    slots = memory.shape[0]
    inner = self_query.shape[1]
    hidden = feed_in.shape[1]
    lens = jnp.concatenate([decoder_length, memory_length])
    vec = jnp.stack([self_gain, self_bias, cross_gain, cross_bias, feed_gain, feed_bias,
                     feed_gain, feed_bias])
    scratch = layout(rows, slots, width, inner, hidden)
    names = tuple(scratch)
    given = dict(tok=tokens, mem=memory, wq=self_query, wk=self_key, wv=self_value,
                 wo=self_output, cwq=cross_query, cwk=cross_key, cwv=cross_value,
                 cwo=cross_output, win=feed_in, wout=feed_out)
    any_spec = pl.BlockSpec(memory_space=pl.ANY)
    total = 2 * hidden + 2 * width

    def kernel(*refs):
        layer_kernel(names, *refs)

    out, tg, mg, g, vg = pl.pallas_call(
        kernel,
        out_shape=(
            jax.ShapeDtypeStruct((rows, width), BF),
            jax.ShapeDtypeStruct((rows, width), BF),
            jax.ShapeDtypeStruct((slots, width), BF),
            jax.ShapeDtypeStruct((total, width), BF),
            jax.ShapeDtypeStruct((8, width), F32),
        ),
        in_specs=[pl.BlockSpec(memory_space=pltpu.SMEM), pl.BlockSpec(memory_space=pltpu.VMEM)]
        + [any_spec] * (len(INPUTS) + 1),
        out_specs=(any_spec,) * 4 + (pl.BlockSpec(memory_space=pltpu.VMEM),),
        scratch_shapes=list(scratch.values()),
        compiler_params=pltpu.CompilerParams(
            collective_id=0, has_side_effects=True, vmem_limit_bytes=67043328),
        name="layer",
    )(lens, vec, *[given[n] for n in INPUTS], cotangent)

    vecs = lax.psum(vg, ("dp", "tensor"))
    grads = lax.psum(g, "dp").astype(F32)

    def block(start):
        x = grads[start:start + width]
        return (x[:, :inner], x[:, inner:2 * inner], x[:, 2 * inner:3 * inner],
                x[:, 3 * inner:].T)

    cq, ck, cv, co = block(2 * hidden)
    sq, sk, sv, so = block(2 * hidden + width)
    return (
        out, tg.astype(F32), mg.astype(F32),
        sq, sk, sv, so, vecs[0], vecs[1],
        cq, ck, cv, co, vecs[2], vecs[3],
        grads[hidden:2 * hidden], grads[:hidden], vecs[4], vecs[5],
    )


def solution(mesh):
    rows = P("dp", None)
    tail = P(None, "tensor")
    head = P("tensor", None)
    whole = P()
    return jax.shard_map(
        shards,
        mesh=mesh,
        in_specs=(
            rows, rows, P("dp"), P("dp"),
            tail, tail, tail, head, whole, whole,
            tail, tail, tail, head, whole, whole,
            tail, head, whole, whole, rows,
        ),
        out_specs=(
            rows, rows, rows,
            tail, tail, tail, head, whole, whole,
            tail, tail, tail, head, whole, whole,
            tail, head, whole, whole,
        ),
        check_vma=False,
    )
```

```python
import jax
import jax.numpy as jnp
from jax import lax
from jax.experimental import pallas as pl
from jax.experimental.pallas import tpu as pltpu
from jax.sharding import PartitionSpec as P

BF = jnp.bfloat16
F32 = jnp.float32
HD = 64
CHUNKS = 4
EPSILON = 1e-05
NEGATIVE = -1e30
MESH = pl.DeviceIdType.MESH
STAGES = 7


def mm(a, b):
    return lax.dot_general(a, b, (((1,), (0,)), ((), ())), preferred_element_type=F32)


def mt(a, b):
    return lax.dot_general(a, b, (((1,), (1,)), ((), ())), preferred_element_type=F32)


def tm(a, b):
    return lax.dot_general(a, b, (((0,), (0,)), ((), ())), preferred_element_type=F32)


PIECE = 256
RING = 8


def split_sizes(copies):
    sizes, rows = [], PIECE
    for _ in range(copies.bit_length() - 1):
        halve = rows // 2 >= 16
        rows = rows // 2 if halve else rows
        sizes.append((rows, halve))
    return sizes


def layout(rows, slots, width, inner, hidden, copies):
    sizes = split_sizes(copies)
    pieces = (2 * hidden + 2 * width) // PIECE
    heads = inner // HD
    chunk = rows // CHUNKS
    half, own = chunk // 2, chunk // 4
    v = pltpu.VMEM
    return dict(
        tok=v((rows, width), BF),
        mem=v((slots, width), BF),
        cot=v((CHUNKS, own, width), BF),
        wq=v((width, inner), BF),
        wk=v((width, inner), BF),
        wv=v((width, inner), BF),
        wo=v((inner, width), BF),
        cwq=v((width, inner), BF),
        cwk=v((width, inner), BF),
        cwv=v((width, inner), BF),
        cwo=v((inner, width), BF),
        win=v((width, hidden), BF),
        wout=v((hidden, width), BF),
        q=v((rows, inner), BF),
        k=v((rows, inner), BF),
        v=v((rows, inner), BF),
        kt=v((heads, HD, rows), BF),
        vt=v((heads, HD + 16, rows), BF),
        cq=v((rows, inner), BF),
        ck=v((slots, inner), BF),
        cv=v((slots, inner), BF),
        ckt=v((heads, HD, slots), BF),
        cvt=v((heads, HD + 16, slots), BF),
        mixed=v((rows, inner), BF),
        cmixed=v((rows, inner), BF),
        lse=v((CHUNKS, heads, 1, chunk), F32),
        clse=v((CHUNKS, heads, 1, chunk), F32),
        delta=v((heads, 1, chunk), F32),
        flat=v((inner, chunk), F32),
        dout=v((chunk, inner), BF),
        dk=v((rows, inner), F32),
        dv=v((rows, inner), F32),
        hid=v((rows, hidden), BF),
        slope=v((rows, hidden), BF),
        low0=v((rows, width), BF),
        low1=v((rows, width), BF),
        low2=v((rows, width), BF),
        low3=v((rows, width), BF),
        low4=v((rows, width), BF),
        outs=v((rows, width), BF),
        res=v((CHUNKS, own, width), F32),
        xh1=v((CHUNKS, own, width), F32),
        xh2=v((CHUNKS, own, width), F32),
        rs1=v((CHUNKS, own, 1), F32),
        rs2=v((CHUNKS, own, 1), F32),
        part=v((CHUNKS, chunk, width), BF),
        rc=v((CHUNKS, half, width), BF),
        ys=v((CHUNKS, half, width), BF),
        ry=v((CHUNKS, own, width), BF),
        vacc=v((8, 8, width), F32),
        gbuf=v((2 * hidden + 2 * width, width), BF),
        vsum=v((8, width), F32),
        vrec=v((len(sizes) + 2, 8, width), F32),
        **{f"dr{j}": v((RING, n, width), BF) for j, (n, _) in enumerate(sizes)},
        ag=v((RING, [n for n, h in sizes if h][-1], width), BF),
        freed=pltpu.SemaphoreType.REGULAR((len(sizes), RING)),
        dssem=pltpu.SemaphoreType.DMA((2 * len(sizes), RING)),
        drsem=pltpu.SemaphoreType.DMA((2 * len(sizes), RING)),
        gsem=pltpu.SemaphoreType.DMA((4, pieces)),
        vssem=pltpu.SemaphoreType.DMA((len(sizes) + 2,)),
        vrsem=pltpu.SemaphoreType.DMA((len(sizes) + 2,)),
        insem=pltpu.SemaphoreType.DMA((16,)),
        cotsem=pltpu.SemaphoreType.DMA((CHUNKS,)),
        osem=pltpu.SemaphoreType.DMA((4,)),
        ssem=pltpu.SemaphoreType.DMA((8, CHUNKS)),
        rsem=pltpu.SemaphoreType.DMA((8, CHUNKS)),
    )


INPUTS = (
    "tok", "wk", "wv", "wq", "wo", "mem", "cwk", "cwv", "cwq", "cwo",
    "win", "wout",
)


def layer_kernel(names, copies, lens, vec, *refs):
    n_in = len(INPUTS)
    srcs = dict(zip(INPUTS, refs[:n_in]))
    cot_h = refs[n_in]
    out_h, tg_h, mg_h, gf_h, gq_h, go_h, vg_h = refs[n_in + 1:n_in + 8]
    S = dict(zip(names, refs[n_in + 8:]))

    rows, width = S["tok"].shape
    slots = S["mem"].shape[0]
    inner = S["wq"].shape[1]
    hidden = S["win"].shape[1]
    heads = inner // HD
    R = rows // CHUNKS
    HF, Q = R // 2, R // 4
    scale = HD ** -0.5
    t = lax.axis_index("tensor")
    yy = t // 2
    kk = t % 2
    core = {"tensor": t + 1 - 2 * kk}
    ypar = {"tensor": t + 2 - 4 * yy}

    me = lax.axis_index("dp")
    sizes = split_sizes(copies)
    bits = len(sizes)
    pieces = (2 * hidden + 2 * width) // PIECE

    def side(weight):
        return lax.rem(lax.div(me, weight), 2)

    def dp_peer(weight):
        return {"dp": me + weight * (1 - 2 * side(weight))}

    def row(c):
        return pl.ds(pl.multiple_of(c * R, R), R)

    def own_rows(c):
        return pl.ds(pl.multiple_of(c * R + kk * HF + yy * Q, Q), Q)

    def y_rows(c):
        return pl.ds(pl.multiple_of(c * R + kk * HF + (1 - yy) * Q, Q), Q)

    loads = {n: pltpu.make_async_copy(srcs[n], S[n], S["insem"].at[j])
             for j, n in enumerate(INPUTS)}
    cots = [pltpu.make_async_copy(cot_h.at[own_rows(c)], S["cot"].at[c], S["cotsem"].at[c])
            for c in range(CHUNKS)]
    for n in INPUTS:
        loads[n].start()
    for c in cots:
        c.start()

    barrier = pltpu.get_barrier_semaphore()
    for peer in [core, ypar] + [dp_peer(1 << j) for j in range(bits)]:
        pl.semaphore_signal(barrier, inc=1, device_id=peer, device_id_type=MESH)

    S["vt"][:, HD:, :] = jnp.ones((heads, 16, rows), BF)
    S["cvt"][:, HD:, :] = jnp.ones((heads, 16, slots), BF)
    S["vacc"][...] = jnp.zeros(S["vacc"].shape, F32)

    def wait_for(*which):
        for n in which:
            loads[n].wait()

    def project(src, wk, wv, kd, vd, ktd, vtd, count):
        def body(i, carry):
            r = row(i)
            x = src[r, :]
            kf = mm(x, wk[...])
            kd[r, :] = kf.astype(BF)
            kt = kf.T.astype(BF)
            vf = mm(x, wv[...])
            vd[r, :] = vf.astype(BF)
            vtt = vf.T.astype(BF)
            for h in range(heads):
                ktd[h, :, r] = kt[h * HD:(h + 1) * HD, :]
                vtd[h, :HD, r] = vtt[h * HD:(h + 1) * HD, :]
            return carry
        lax.fori_loop(0, count, body, 0)

    def project_q(src, w, dst):
        def body(i, carry):
            dst[row(i), :] = mm(src[row(i), :], w[...]).astype(BF)
            return carry
        lax.fori_loop(0, CHUNKS, body, 0)

    def lanes(h):
        return pl.ds(pl.multiple_of((h // 2) * 2 * HD, 2 * HD), 2 * HD)

    def pick(x, h):
        lane = lax.broadcasted_iota(jnp.int32, x.shape, 1) // HD
        return jnp.where(lane == h % 2, x, jnp.zeros_like(x))

    def masked(scores, c, causal, length):
        kid = lax.broadcasted_iota(jnp.int32, scores.shape, 0)
        ok = kid < length
        if causal:
            qid = c * R + lax.broadcasted_iota(jnp.int32, scores.shape, 1)
            ok = ok & (kid <= qid)
        return jnp.where(ok, scores * scale, NEGATIVE)

    def head_forward(h, c, q, k, vt, lse, causal, length):
        qm = pick(q[row(c), lanes(h)], h)
        s = masked(mt(k[:, lanes(h)], qm), c, causal, length)
        top = jnp.max(s, axis=0, keepdims=True)
        p = jnp.exp(s - top).astype(BF)
        o = mm(vt[h], p)
        total = o[HD:HD + 1, :]
        S["flat"][pl.ds(pl.multiple_of(h * HD, HD), HD), :] = o[:HD, :] / total
        lse[c, h] = top + jnp.log(total)

    def head_backward(h, c, q, k, v, kt, lse, causal, length):
        qm = pick(q[row(c), lanes(h)], h)
        s = masked(mt(k[:, lanes(h)], qm), c, causal, length)
        p = jnp.exp(s - lse[c, h])
        dom = pick(S["dout"][:, lanes(h)], h)
        dp = mt(v[:, lanes(h)], dom)
        S["dv"][:, lanes(h)] += mm(p.astype(BF), dom)
        ds = (p * (dp - S["delta"][h])).astype(BF)
        S["dk"][:, lanes(h)] += mm(ds, qm)
        S["flat"][pl.ds(pl.multiple_of(h * HD, HD), HD), :] = mm(kt[h], ds) * scale

    def unflatten():
        return S["flat"][...].T

    def wide(fn, dst, c):
        block = min(256, width)

        def body(j, carry):
            cols = pl.ds(pl.multiple_of(j * block, block), block)
            dst[c, :, cols] = fn(cols).astype(BF)
            return carry
        lax.fori_loop(0, width // block, body, 0)

    def set_delta(c, mixed, low, w):
        do = mt(low[row(c), :], w[...]).astype(BF)
        S["dout"][...] = do
        prod = do.astype(F32) * mixed[row(c), :].astype(F32)
        sel = (lax.broadcasted_iota(jnp.int32, (8, inner), 1) // HD
               == lax.broadcasted_iota(jnp.int32, (8, inner), 0)).astype(F32)
        d = lax.dot_general(sel, prod, (((1,), (1,)), ((), ())),
                            precision=lax.Precision.HIGHEST, preferred_element_type=F32)
        for h in range(heads):
            S["delta"][h] = d[h:h + 1, :]

    dec = lens[0]
    enc = lens[1]

    def each_head(fn, middle):
        def body(h, carry):
            @pl.when(h == heads // 2)
            def _():
                middle()
            fn(h)
            return carry
        lax.fori_loop(0, heads, body, 0)

    def compute(s, c, middle):
        part = S["part"]
        if s == 0:
            each_head(lambda h: head_forward(h, c, S["q"], S["k"], S["vt"], S["lse"], True, dec), middle)
            S["mixed"][row(c), :] = unflatten().astype(BF)
            wide(lambda n: mm(S["mixed"][row(c), :], S["wo"][:, n]), part, c)
        elif s == 1:
            S["cq"][row(c), :] = mm(S["low0"][row(c), :], S["cwq"][...]).astype(BF)
            each_head(lambda h: head_forward(h, c, S["cq"], S["ck"], S["cvt"], S["clse"], False, enc), middle)
            S["cmixed"][row(c), :] = unflatten().astype(BF)
            wide(lambda n: mm(S["cmixed"][row(c), :], S["cwo"][:, n]), part, c)
        elif s == 2:
            block = min(256, hidden)

            def body(j, carry):
                n = pl.ds(pl.multiple_of(j * block, block), block)
                v = mm(S["low1"][row(c), :], S["win"][:, n])
                cdf = 0.5 * (1.0 + lax.erf(v * 0.7071067811865476))
                S["hid"][row(c), n] = (v * cdf).astype(BF)
                S["slope"][row(c), n] = (
                    cdf + v * jnp.exp(-0.5 * v * v) * 0.3989422804014327).astype(BF)
                return carry
            lax.fori_loop(0, hidden // block, body, 0)
            middle()
            wide(lambda n: mm(S["hid"][row(c), :], S["wout"][:, n]), part, c)
        elif s == 3:
            block = min(256, hidden)

            def body(j, carry):
                n = pl.ds(pl.multiple_of(j * block, block), block)
                g = mt(S["low2"][row(c), :], S["wout"][n, :])
                S["slope"][row(c), n] = (g * S["slope"][row(c), n].astype(F32)).astype(BF)
                return carry
            lax.fori_loop(0, hidden // block, body, 0)
            middle()
            wide(lambda n: mt(S["slope"][row(c), :], S["win"][n, :]), part, c)
        elif s == 4:
            set_delta(c, S["cmixed"], S["low3"], S["cwo"])
            each_head(lambda h: head_backward(h, c, S["cq"], S["ck"], S["cv"], S["ckt"], S["clse"], False, enc), middle)
            S["cq"][row(c), :] = unflatten().astype(BF)
            wide(lambda n: mt(S["cq"][row(c), :], S["cwq"][n, :]), part, c)
        elif s == 5:
            set_delta(c, S["mixed"], S["low4"], S["wo"])
            each_head(lambda h: head_backward(h, c, S["q"], S["k"], S["v"], S["kt"], S["lse"], True, dec), middle)
            S["q"][row(c), :] = unflatten().astype(BF)
            S["k"][row(c), :] = (S["dk"][row(c), :] * scale).astype(BF)
            S["v"][row(c), :] = S["dv"][row(c), :].astype(BF)
            wide(lambda n: mt(S["q"][row(c), :], S["wq"][n, :])
                 + mt(S["k"][row(c), :], S["wk"][n, :])
                 + mt(S["v"][row(c), :], S["wv"][n, :]), part, c)
        else:
            middle()
            wide(lambda n: mt(S["ck"][row(c), :], S["cwk"][n, :])
                 + mt(S["cv"][row(c), :], S["cwv"][n, :]), part, c)

    lows = [S["low0"], S["low1"], S["low2"], S["low3"], S["low4"], S["low2"], S["low1"]]

    def remote(src, dst, phase, c, peer):
        return pltpu.make_async_remote_copy(
            src_ref=src, dst_ref=dst, send_sem=S["ssem"].at[phase, c],
            recv_sem=S["rsem"].at[phase, c], device_id=peer, device_id_type=MESH)

    def core_part(c):
        theirs = pl.ds(pl.multiple_of((1 - kk) * HF, HF), HF)
        return remote(S["part"].at[c, theirs], S["rc"].at[c], 0, c, core)

    def y_part(c):
        theirs = pl.ds(pl.multiple_of((1 - yy) * Q, Q), Q)
        return remote(S["ys"].at[c, theirs], S["ry"].at[c], 1, c, ypar)

    def gather(buf, c, which, base):
        r = y_rows(c) if which == 2 else own_rows(c)
        return remote(buf.at[r], buf.at[r], base + which, c, ypar if which == 0 else core)

    def p0(c):
        core_part(c).start()

    def p1(c):
        core_part(c).wait()
        step = min(32, HF)

        def body(j, carry):
            r = pl.ds(pl.multiple_of(j * step, step), step)
            m = pl.ds(pl.multiple_of(kk * HF + j * step, step), step)
            S["ys"][c, r, :] = (S["part"][c, m, :].astype(F32)
                                + S["rc"][c, r, :].astype(F32)).astype(BF)
            return carry
        lax.fori_loop(0, HF // step, body, 0)
        y_part(c).start()

    def mean(x):
        return jnp.sum(x, axis=-1, keepdims=True) * (1.0 / width)

    def norm(x, j):
        center = x - mean(x)
        inv = lax.rsqrt(mean(center * center) + EPSILON)
        xhat = center * inv
        return xhat, inv, xhat * vec[2 * j:2 * j + 1, :] + vec[2 * j + 1:2 * j + 2, :]

    def fold(x):
        return jnp.sum(x.reshape(x.shape[0] // 8, 8, width), axis=0)

    def norm_back(e, xhat, inv, j):
        S["vacc"][2 * j] += fold(e * xhat)
        S["vacc"][2 * j + 1] += fold(e)
        eg = e * vec[2 * j:2 * j + 1, :]
        return (eg - mean(eg) - xhat * mean(eg * xhat)) * inv

    def p2(s, c):
        y_part(c).wait()
        if s == 2:
            @pl.when(c == CHUNKS - 1)
            def _():
                for x in cots:
                    x.wait()
        step = min(16, Q)
        buf = lows[s]

        def body(j, carry):
            r = pl.ds(pl.multiple_of(j * step, step), step)
            m = pl.ds(pl.multiple_of(yy * Q + j * step, step), step)
            o = pl.ds(pl.multiple_of(c * R + kk * HF + yy * Q + j * step, step), step)
            x = S["ys"][c, m, :].astype(F32) + S["ry"][c, r, :].astype(F32)
            if s == 0:
                xhat, inv, y = norm(S["tok"][o, :].astype(F32) + x, 0)
                S["xh1"][c, r, :] = xhat
                S["rs1"][c, r, :] = inv
                S["res"][c, r, :] = y
            elif s == 1:
                xhat, inv, y = norm(S["res"][c, r, :] + x, 1)
                S["xh2"][c, r, :] = xhat
                S["rs2"][c, r, :] = inv
                S["res"][c, r, :] = y
            elif s == 2:
                xhat, inv, y = norm(S["res"][c, r, :] + x, 2)
                S["outs"][o, :] = y.astype(BF)
                rid = (c * R + kk * HF + yy * Q + j * step
                       + lax.broadcasted_iota(jnp.int32, (step, width), 0))
                seed = jnp.where(rid < dec, S["cot"][c, r, :].astype(F32), 0.0)
                y = norm_back(seed, xhat, inv, 2)
                S["res"][c, r, :] = y
            elif s == 3:
                y = norm_back(S["res"][c, r, :] + x, S["xh2"][c, r, :], S["rs2"][c, r, :], 1)
                S["res"][c, r, :] = y
            elif s == 4:
                y = norm_back(S["res"][c, r, :] + x, S["xh1"][c, r, :], S["rs1"][c, r, :], 0)
                S["res"][c, r, :] = y
            elif s == 5:
                y = S["res"][c, r, :] + x
            else:
                y = x
            buf[o, :] = y.astype(BF)
            return carry
        lax.fori_loop(0, Q // step, body, 0)
        gather(buf, c, 0, 2).start()
        gather(buf, c, 1, 2).start()
        if s == 2:
            gather(S["outs"], c, 0, 5).start()
            gather(S["outs"], c, 1, 5).start()

    def p3(s, c):
        sets = ((lows[s], 2), (S["outs"], 5)) if s == 2 else ((lows[s], 2),)
        for buf, base in sets:
            gather(buf, c, 0, base).wait()
            gather(buf, c, 2, base).start()

    def p4(s, c):
        sets = ((lows[s], 2), (S["outs"], 5)) if s == 2 else ((lows[s], 2),)
        for buf, base in sets:
            gather(buf, c, 1, base).wait()
            gather(buf, c, 2, base).wait()

    def grad_piece(g, i):
        n = pl.ds(pl.multiple_of(i * PIECE, PIECE), PIECE)
        r = pl.ds(pl.multiple_of((g * CHUNKS + i) * PIECE, PIECE), PIECE)
        if g == 0:
            S["gbuf"][r, :] = tm(S["hid"][:, n], S["low2"][...]).astype(BF)
        elif g == 1:
            S["gbuf"][r, :] = tm(S["low1"][:, n], S["slope"][...]).astype(BF)
        else:
            if g == 2:
                a, b, d = S["low0"], S["mem"], S["low3"]
                x, y, z, w = S["cq"], S["ck"], S["cv"], S["cmixed"]
            else:
                a, b, d = S["tok"], S["tok"], S["low4"]
                x, y, z, w = S["q"], S["k"], S["v"], S["mixed"]
            S["gbuf"][r, 0 * inner:1 * inner] = tm(a[:, n], x[...]).astype(BF)
            S["gbuf"][r, 1 * inner:2 * inner] = tm(b[:, n], y[...]).astype(BF)
            S["gbuf"][r, 2 * inner:3 * inner] = tm(b[:, n], z[...]).astype(BF)
            S["gbuf"][r, 3 * inner:4 * inner] = tm(w[...], d[:, n]).astype(BF)

    def weight(step, p):
        if bits < 2 or step > 1:
            return 1 << step
        swap = lax.div(lax.rem(p, 4), 3)
        return 1 + swap if step == 0 else 2 - swap

    def start_of(step, p):
        at = p * PIECE
        for j in range(step):
            if sizes[j][1]:
                at = at + side(weight(j, p)) * sizes[j][0]
        return at

    def piece_rows(at, n):
        return pl.ds(pl.multiple_of(at, n), n)

    def reduce_copy(step, p):
        n, halve = sizes[step]
        w = weight(step, p)
        at = start_of(step, p)
        if halve:
            at = at + (1 - side(w)) * n
        slot = lax.rem(p, RING)
        return pltpu.make_async_remote_copy(
            src_ref=S["gbuf"].at[piece_rows(at, n)], dst_ref=S[f"dr{step}"].at[slot],
            send_sem=S["dssem"].at[step, slot], recv_sem=S["drsem"].at[step, slot],
            device_id=dp_peer(w), device_id_type=MESH)

    def reduce_add(step, p):
        n, halve = sizes[step]
        at = start_of(step + 1, p)
        slot = lax.rem(p, RING)
        block = min(32, n)

        def body(j, carry):
            r = pl.ds(pl.multiple_of(at + j * block, block), block)
            m = pl.ds(pl.multiple_of(j * block, block), block)
            S["gbuf"][r, :] = (S["gbuf"][r, :].astype(F32)
                               + S[f"dr{step}"][slot, m, :].astype(F32)).astype(BF)
            return carry
        lax.fori_loop(0, n // block, body, 0)

    halved = sum(1 for _, h in sizes if h)
    steps = bits + halved

    def gather_copy(step, p):
        n, _ = sizes[step]
        r = S["gbuf"].at[piece_rows(start_of(step + 1, p), n)]
        slot = lax.rem(p, RING)
        return pltpu.make_async_remote_copy(
            src_ref=r, dst_ref=S["ag"].at[slot] if step == halved - 1 else r,
            send_sem=S["dssem"].at[bits + step, slot], recv_sem=S["drsem"].at[bits + step, slot],
            device_id=dp_peer(weight(step, p)), device_id_type=MESH)

    def gather_end(step, p):
        gather_copy(step, p).wait()
        if step == halved - 1:
            n, _ = sizes[step]
            at = start_of(step, p) + (1 - side(weight(step, p))) * n
            S["gbuf"][piece_rows(at, n), :] = S["ag"][lax.rem(p, RING)]

    def gather_begin(step, p):
        if step < halved - 1:
            pl.semaphore_wait(S["freed"].at[step, lax.rem(p, RING)], 1)
        gather_copy(step, p).start()

    def result_copies(p, ff):
        r = pl.ds(pl.multiple_of(p * PIECE, PIECE), PIECE)
        if ff:
            return [pltpu.make_async_copy(S["gbuf"].at[r], gf_h.at[r], S["gsem"].at[0, p])]
        g = lax.div(p - 2 * CHUNKS, CHUNKS)
        n = pl.ds(pl.multiple_of(lax.rem(p, CHUNKS) * PIECE, PIECE), PIECE)
        block = [S["gbuf"].at[r, pl.ds(j * inner, inner)] for j in range(4)]
        return [pltpu.make_async_copy(block[j], gq_h.at[g, j, n], S["gsem"].at[j, p])
                for j in range(3)] + [
            pltpu.make_async_copy(block[3], go_h.at[g, :, n], S["gsem"].at[3, p])]

    def dp_step(k, p):
        if 1 <= k <= bits:
            reduce_copy(k - 1, p).wait()
            if k < halved:
                pl.semaphore_signal(S["freed"].at[k - 1, lax.rem(p, RING)], inc=1,
                                    device_id=dp_peer(weight(k - 1, p)), device_id_type=MESH)
            reduce_add(k - 1, p)
        elif k > bits:
            gather_end(halved - (k - bits), p)
        if k < bits:
            reduce_copy(k, p).start()
        elif k < steps:
            gather_begin(halved - 1 - (k - bits), p)
        else:
            @pl.when(p < 2 * CHUNKS)
            def _():
                for x in result_copies(p, True):
                    x.start()

            @pl.when(p >= 2 * CHUNKS)
            def _():
                for x in result_copies(p, False):
                    x.start()

    dp_order = [0] + [k for k in range(steps - 1, 1, -1)] + [steps, 1]

    def dp_slot(j):
        for k in dp_order:
            p = j - k

            @pl.when((p >= 0) & (p < pieces))
            def _(k=k, p=p):
                dp_step(k, p)

    peers = [core, ypar] + [dp_peer(1 << j) for j in range(bits)]

    def vec_copy(k):
        return pltpu.make_async_remote_copy(
            src_ref=S["vsum"], dst_ref=S["vrec"].at[k], send_sem=S["vssem"].at[k],
            recv_sem=S["vrsem"].at[k], device_id=peers[k], device_id_type=MESH)

    def vec_step(k):
        if k == 0:
            S["vsum"][...] = jnp.sum(S["vacc"][...], axis=1)
        else:
            vec_copy(k - 1).wait()
            S["vsum"][...] += S["vrec"][k - 1]
        if k < len(peers):
            vec_copy(k).start()

    wait_for("tok", "wk", "wv", "wq")
    project(S["tok"], S["wk"], S["wv"], S["k"], S["v"], S["kt"], S["vt"], CHUNKS)
    project_q(S["tok"], S["wq"], S["q"])
    pl.semaphore_wait(barrier, 2 + bits)
    wait_for("wo")

    def lagged(i, lag, fn, s):
        c = lax.rem(CHUNKS - 1 - i + lag, CHUNKS)

        @pl.when(i >= lag)
        def _():
            fn(s, c)
        if s > 0:
            @pl.when(i < lag)
            def _():
                fn(s - 1, c)

    for s in range(STAGES):
        if s == 1:
            wait_for("mem", "cwk", "cwv", "cwq", "cwo")
            project(S["mem"], S["cwk"], S["cwv"], S["ck"], S["cv"], S["ckt"], S["cvt"], CHUNKS)
        if s == 2:
            wait_for("win", "wout")
        if s in (4, 5):
            S["dk"][...] = jnp.zeros(S["dk"].shape, F32)
            S["dv"][...] = jnp.zeros(S["dv"].shape, F32)

        def slot(i, carry, s=s):
            c = CHUNKS - 1 - i
            if s > 0:
                p4(s - 1, c)

            def middle():
                lagged(i, 3, p3, s)
                lagged(i, 2, p2, s)
                if s > 0:
                    p1(lax.rem(c + 1, CHUNKS))
                else:
                    @pl.when(i >= 1)
                    def _():
                        p1(lax.rem(c + 1, CHUNKS))
            compute(s, c, middle)
            p0(c)
            if s >= 4:
                grad_piece(s - 4, i)
                dp_slot((s - 4) * CHUNKS + i)
            if s == 6:
                for k in range(CHUNKS):
                    @pl.when(i == k)
                    def _(k=k):
                        vec_step(k)
            return carry
        lax.fori_loop(0, CHUNKS, slot, 0)
        if s == 4:
            S["ck"][...] = (S["dk"][...] * scale).astype(BF)
            S["cv"][...] = S["dv"][...].astype(BF)

    last = STAGES - 1
    o_copy = pltpu.make_async_copy(S["outs"], out_h, S["osem"].at[1])
    o_copy.start()
    vec_step(CHUNKS)

    p1(0)
    p2(last, 1)
    p3(last, 2)
    p2(last, 0)
    p3(last, 1)
    p3(last, 0)
    for c in range(CHUNKS):
        p4(last, CHUNKS - 1 - c)
    t_copy = pltpu.make_async_copy(lows[5], tg_h, S["osem"].at[2])
    t_copy.start()
    m_copy = pltpu.make_async_copy(lows[6], mg_h, S["osem"].at[3])
    m_copy.start()
    for k in range(CHUNKS + 1, len(peers) + 1):
        vec_step(k)
    vg_h[...] = S["vsum"][...]

    def tail_slot(j, carry):
        @pl.when(j < pieces)
        def _():
            grad_piece(3, lax.rem(j, CHUNKS))
        dp_slot(j)
        return carry
    lax.fori_loop(3 * CHUNKS, pieces + steps, tail_slot, 0)

    def finish(p, carry, ff):
        for x in result_copies(p, ff):
            x.wait()
        return carry
    lax.fori_loop(0, 2 * CHUNKS, lambda p, x: finish(p, x, True), 0)
    lax.fori_loop(2 * CHUNKS, pieces, lambda p, x: finish(p, x, False), 0)
    for x in (o_copy, t_copy, m_copy):
        x.wait()


def shards(
    tokens, memory, decoder_length, memory_length,
    self_query, self_key, self_value, self_output, self_gain, self_bias,
    cross_query, cross_key, cross_value, cross_output, cross_gain, cross_bias,
    feed_in, feed_out, feed_gain, feed_bias, cotangent,
):
    rows, width = tokens.shape
    slots = memory.shape[0]
    inner = self_query.shape[1]
    hidden = feed_in.shape[1]
    lens = jnp.concatenate([decoder_length, memory_length])
    vec = jnp.stack([self_gain, self_bias, cross_gain, cross_bias, feed_gain, feed_bias,
                     feed_gain, feed_bias])
    copies = lax.axis_size("dp")
    scratch = layout(rows, slots, width, inner, hidden, copies)
    names = tuple(scratch)
    given = dict(tok=tokens, mem=memory, wq=self_query, wk=self_key, wv=self_value,
                 wo=self_output, cwq=cross_query, cwk=cross_key, cwv=cross_value,
                 cwo=cross_output, win=feed_in, wout=feed_out)
    any_spec = pl.BlockSpec(memory_space=pl.ANY)

    def kernel(*refs):
        layer_kernel(names, copies, *refs)

    out, tg, mg, gf, gq, go, vg = pl.pallas_call(
        kernel,
        out_shape=(
            jax.ShapeDtypeStruct((rows, width), BF),
            jax.ShapeDtypeStruct((rows, width), BF),
            jax.ShapeDtypeStruct((slots, width), BF),
            jax.ShapeDtypeStruct((2 * hidden, width), BF),
            jax.ShapeDtypeStruct((2, 3, width, inner), BF),
            jax.ShapeDtypeStruct((2, inner, width), BF),
            jax.ShapeDtypeStruct((8, width), F32),
        ),
        in_specs=[pl.BlockSpec(memory_space=pltpu.SMEM), pl.BlockSpec(memory_space=pltpu.VMEM)]
        + [any_spec] * (len(INPUTS) + 1),
        out_specs=(any_spec,) * 6 + (pl.BlockSpec(memory_space=pltpu.VMEM),),
        scratch_shapes=list(scratch.values()),
        compiler_params=pltpu.CompilerParams(
            collective_id=0, has_side_effects=True, vmem_limit_bytes=67043328),
        name="layer",
    )(lens, vec, *[given[n] for n in INPUTS], cotangent)

    def wide_grads(j):
        return tuple(gq[j, i].astype(F32) for i in range(3)) + (go[j].astype(F32),)

    return (
        out, tg.astype(F32), mg.astype(F32),
        *wide_grads(1), vg[0], vg[1],
        *wide_grads(0), vg[2], vg[3],
        gf[hidden:].astype(F32), gf[:hidden].astype(F32), vg[4], vg[5],
    )


def solution(mesh):
    rows = P("dp", None)
    tail = P(None, "tensor")
    head = P("tensor", None)
    whole = P()
    return jax.shard_map(
        shards,
        mesh=mesh,
        in_specs=(
            rows, rows, P("dp"), P("dp"),
            tail, tail, tail, head, whole, whole,
            tail, tail, tail, head, whole, whole,
            tail, head, whole, whole, rows,
        ),
        out_specs=(
            rows, rows, rows,
            tail, tail, tail, head, whole, whole,
            tail, tail, tail, head, whole, whole,
            tail, head, whole, whole,
        ),
        check_vma=False,
    )
```

```python
import jax
import jax.numpy as jnp
from jax import lax
from jax.experimental import pallas as pl
from jax.experimental.pallas import tpu as pltpu
from jax.sharding import PartitionSpec as P

BF = jnp.bfloat16
F32 = jnp.float32
HD = 64
CHUNKS = 4
EPSILON = 1e-05
NEGATIVE = -1e30
MESH = pl.DeviceIdType.MESH
STAGES = 7


def mm(a, b):
    return lax.dot_general(a, b, (((1,), (0,)), ((), ())), preferred_element_type=F32)


def mt(a, b):
    return lax.dot_general(a, b, (((1,), (1,)), ((), ())), preferred_element_type=F32)


def tm(a, b):
    return lax.dot_general(a, b, (((0,), (0,)), ((), ())), preferred_element_type=F32)


PIECE = 256
RING = 8


def split_sizes(copies):
    sizes, rows = [], PIECE
    for _ in range(copies.bit_length() - 1):
        halve = rows // 2 >= 16
        rows = rows // 2 if halve else rows
        sizes.append((rows, halve))
    return sizes


def layout(rows, slots, width, inner, hidden, copies):
    sizes = split_sizes(copies)
    pieces = (2 * hidden + 2 * width) // PIECE
    heads = inner // HD
    chunk = rows // CHUNKS
    half, own = chunk // 2, chunk // 4
    v = pltpu.VMEM
    return dict(
        tok=v((rows, width), BF),
        mem=v((slots, width), BF),
        cot=v((CHUNKS, own, width), BF),
        wq=v((width, inner), BF),
        wk=v((width, inner), BF),
        wv=v((width, inner), BF),
        wo=v((inner, width), BF),
        cwq=v((width, inner), BF),
        cwk=v((width, inner), BF),
        cwv=v((width, inner), BF),
        cwo=v((inner, width), BF),
        win=v((width, hidden), BF),
        wout=v((hidden, width), BF),
        q=v((rows, inner), BF),
        k=v((rows, inner), BF),
        v=v((rows, inner), BF),
        kt=v((heads, HD, rows), BF),
        vt=v((heads, HD + 16, rows), BF),
        cq=v((rows, inner), BF),
        ck=v((slots, inner), BF),
        cv=v((slots, inner), BF),
        ckt=v((heads, HD, slots), BF),
        cvt=v((heads, HD + 16, slots), BF),
        mixed=v((rows, inner), BF),
        cmixed=v((rows, inner), BF),
        lse=v((CHUNKS, heads, 1, chunk), F32),
        clse=v((CHUNKS, heads, 1, chunk), F32),
        delta=v((heads, 1, chunk), F32),
        flat=v((inner, chunk), F32),
        dout=v((chunk, inner), BF),
        dk=v((rows, inner), F32),
        dv=v((rows, inner), F32),
        hid=v((rows, hidden), BF),
        slope=v((rows, hidden), BF),
        low0=v((rows, width), BF),
        low1=v((rows, width), BF),
        low2=v((rows, width), BF),
        low3=v((rows, width), BF),
        low4=v((rows, width), BF),
        outs=v((rows, width), BF),
        res=v((CHUNKS, own, width), F32),
        xh1=v((CHUNKS, own, width), F32),
        xh2=v((CHUNKS, own, width), F32),
        rs1=v((CHUNKS, own, 1), F32),
        rs2=v((CHUNKS, own, 1), F32),
        part=v((CHUNKS, chunk, width), BF),
        rc=v((CHUNKS, half, width), BF),
        ys=v((CHUNKS, half, width), BF),
        ry=v((CHUNKS, own, width), BF),
        vacc=v((8, 8, width), F32),
        gbuf=v((2 * hidden + 2 * width, width), BF),
        vsum=v((8, width), F32),
        vrec=v((len(sizes) + 2, 8, width), F32),
        **{f"dr{j}": v((RING, n, width), BF) for j, (n, _) in enumerate(sizes)},
        ag=v((RING, [n for n, h in sizes if h][-1], width), BF),
        freed=pltpu.SemaphoreType.REGULAR((len(sizes), RING)),
        dssem=pltpu.SemaphoreType.DMA((2 * len(sizes), RING)),
        drsem=pltpu.SemaphoreType.DMA((2 * len(sizes), RING)),
        gsem=pltpu.SemaphoreType.DMA((4, pieces)),
        vssem=pltpu.SemaphoreType.DMA((len(sizes) + 2,)),
        vrsem=pltpu.SemaphoreType.DMA((len(sizes) + 2,)),
        insem=pltpu.SemaphoreType.DMA((16,)),
        cotsem=pltpu.SemaphoreType.DMA((CHUNKS,)),
        osem=pltpu.SemaphoreType.DMA((4,)),
        ssem=pltpu.SemaphoreType.DMA((8, CHUNKS)),
        rsem=pltpu.SemaphoreType.DMA((8, CHUNKS)),
    )


INPUTS = (
    "tok", "wk", "wv", "wq", "wo", "mem", "cwk", "cwv", "cwq", "cwo",
    "win", "wout",
)


def layer_kernel(names, copies, lens, vec, *refs):
    n_in = len(INPUTS)
    srcs = dict(zip(INPUTS, refs[:n_in]))
    cot_h = refs[n_in]
    out_h, tg_h, mg_h, gf_h, gq_h, go_h, vg_h = refs[n_in + 1:n_in + 8]
    S = dict(zip(names, refs[n_in + 8:]))

    rows, width = S["tok"].shape
    slots = S["mem"].shape[0]
    inner = S["wq"].shape[1]
    hidden = S["win"].shape[1]
    heads = inner // HD
    R = rows // CHUNKS
    HF, Q = R // 2, R // 4
    scale = HD ** -0.5
    t = lax.axis_index("tensor")
    yy = t // 2
    kk = t % 2
    core = {"tensor": t + 1 - 2 * kk}
    ypar = {"tensor": t + 2 - 4 * yy}

    me = lax.axis_index("dp")
    sizes = split_sizes(copies)
    bits = len(sizes)
    pieces = (2 * hidden + 2 * width) // PIECE

    def side(weight):
        return lax.rem(lax.div(me, weight), 2)

    def dp_peer(weight):
        return {"dp": me + weight * (1 - 2 * side(weight))}

    def row(c):
        return pl.ds(pl.multiple_of(c * R, R), R)

    def own_rows(c):
        return pl.ds(pl.multiple_of(c * R + kk * HF + yy * Q, Q), Q)

    def y_rows(c):
        return pl.ds(pl.multiple_of(c * R + kk * HF + (1 - yy) * Q, Q), Q)

    loads = {n: pltpu.make_async_copy(srcs[n], S[n], S["insem"].at[j])
             for j, n in enumerate(INPUTS)}
    cots = [pltpu.make_async_copy(cot_h.at[own_rows(c)], S["cot"].at[c], S["cotsem"].at[c])
            for c in range(CHUNKS)]
    for n in INPUTS:
        loads[n].start()
    for c in cots:
        c.start()

    barrier = pltpu.get_barrier_semaphore()
    for peer in [core, ypar] + [dp_peer(1 << j) for j in range(bits)]:
        pl.semaphore_signal(barrier, inc=1, device_id=peer, device_id_type=MESH)

    S["vt"][:, HD:, :] = jnp.ones((heads, 16, rows), BF)
    S["cvt"][:, HD:, :] = jnp.ones((heads, 16, slots), BF)
    S["vacc"][...] = jnp.zeros(S["vacc"].shape, F32)

    pl.semaphore_wait(barrier, 2 + bits)

    def wait_for(*which):
        for n in which:
            loads[n].wait()

    def project(c, src, wk, wv, kd, vd, ktd, vtd):
        r = row(c)
        x = src[r, :]
        kf = mm(x, wk[...])
        kd[r, :] = kf.astype(BF)
        kt = kf.T.astype(BF)
        vf = mm(x, wv[...])
        vd[r, :] = vf.astype(BF)
        vtt = vf.T.astype(BF)
        for h in range(heads):
            ktd[h, :, r] = kt[h * HD:(h + 1) * HD, :]
            vtd[h, :HD, r] = vtt[h * HD:(h + 1) * HD, :]

    def lanes(h):
        return pl.ds(pl.multiple_of((h // 2) * 2 * HD, 2 * HD), 2 * HD)

    def pick(x, h):
        lane = lax.broadcasted_iota(jnp.int32, x.shape, 1) // HD
        return jnp.where(lane == h % 2, x, jnp.zeros_like(x))

    def masked(scores, c, causal, length):
        kid = lax.broadcasted_iota(jnp.int32, scores.shape, 0)
        ok = kid < length
        if causal:
            qid = c * R + lax.broadcasted_iota(jnp.int32, scores.shape, 1)
            ok = ok & (kid <= qid)
        return jnp.where(ok, scores * scale, NEGATIVE)

    def head_forward(h, c, q, k, vt, lse, causal, length, keys):
        qm = pick(q[row(c), lanes(h)], h)
        s = masked(mt(k[:keys, lanes(h)], qm), c, causal, length)
        top = jnp.max(s, axis=0, keepdims=True)
        p = jnp.exp(s - top).astype(BF)
        o = mm(vt[h, :, :keys], p)
        total = o[HD:HD + 1, :]
        S["flat"][pl.ds(pl.multiple_of(h * HD, HD), HD), :] = o[:HD, :] / total
        lse[c, h] = top + jnp.log(total)

    def head_backward(h, c, q, k, v, kt, lse, causal, length):
        qm = pick(q[row(c), lanes(h)], h)
        s = masked(mt(k[:, lanes(h)], qm), c, causal, length)
        p = jnp.exp(s - lse[c, h])
        dom = pick(S["dout"][:, lanes(h)], h)
        dp = mt(v[:, lanes(h)], dom)
        S["dv"][:, lanes(h)] += mm(p.astype(BF), dom)
        ds = (p * (dp - S["delta"][h])).astype(BF)
        S["dk"][:, lanes(h)] += mm(ds, qm)
        S["flat"][pl.ds(pl.multiple_of(h * HD, HD), HD), :] = mm(kt[h], ds) * scale

    def unflatten():
        return S["flat"][...].T

    def wide(fn, dst, c):
        block = min(256, width)

        def body(j, carry):
            cols = pl.ds(pl.multiple_of(j * block, block), block)
            dst[c, :, cols] = fn(cols).astype(BF)
            return carry
        lax.fori_loop(0, width // block, body, 0)

    def set_delta(c, mixed, low, w):
        do = mt(low[row(c), :], w[...]).astype(BF)
        S["dout"][...] = do
        prod = do.astype(F32) * mixed[row(c), :].astype(F32)
        sel = (lax.broadcasted_iota(jnp.int32, (8, inner), 1) // HD
               == lax.broadcasted_iota(jnp.int32, (8, inner), 0)).astype(F32)
        d = lax.dot_general(sel, prod, (((1,), (1,)), ((), ())),
                            precision=lax.Precision.HIGHEST, preferred_element_type=F32)
        for h in range(heads):
            S["delta"][h] = d[h:h + 1, :]

    dec = lens[0]
    enc = lens[1]

    def each_head(fn, middle):
        def body(h, carry):
            @pl.when(h == heads // 2)
            def _():
                middle()
            fn(h)
            return carry
        lax.fori_loop(0, heads, body, 0)

    def compute(s, c, middle):
        part = S["part"]
        if s == 0:
            project(c, S["tok"], S["wk"], S["wv"], S["k"], S["v"], S["kt"], S["vt"])
            S["q"][row(c), :] = mm(S["tok"][row(c), :], S["wq"][...]).astype(BF)
            each_head(lambda h: head_forward(h, c, S["q"], S["k"], S["vt"], S["lse"], True, dec,
                                             (c + 1) * R), middle)
            S["mixed"][row(c), :] = unflatten().astype(BF)
            wide(lambda n: mm(S["mixed"][row(c), :], S["wo"][:, n]), part, c)
        elif s == 1:
            S["cq"][row(c), :] = mm(S["low0"][row(c), :], S["cwq"][...]).astype(BF)
            each_head(lambda h: head_forward(h, c, S["cq"], S["ck"], S["cvt"], S["clse"], False, enc, slots), middle)
            S["cmixed"][row(c), :] = unflatten().astype(BF)
            wide(lambda n: mm(S["cmixed"][row(c), :], S["cwo"][:, n]), part, c)
        elif s == 2:
            block = min(256, hidden)

            def body(j, carry):
                n = pl.ds(pl.multiple_of(j * block, block), block)
                v = mm(S["low1"][row(c), :], S["win"][:, n])
                cdf = 0.5 * (1.0 + lax.erf(v * 0.7071067811865476))
                S["hid"][row(c), n] = (v * cdf).astype(BF)
                S["slope"][row(c), n] = (
                    cdf + v * jnp.exp(-0.5 * v * v) * 0.3989422804014327).astype(BF)
                return carry
            lax.fori_loop(0, hidden // block, body, 0)
            middle()
            wide(lambda n: mm(S["hid"][row(c), :], S["wout"][:, n]), part, c)
        elif s == 3:
            block = min(256, hidden)

            def body(j, carry):
                n = pl.ds(pl.multiple_of(j * block, block), block)
                g = mt(S["low2"][row(c), :], S["wout"][n, :])
                S["slope"][row(c), n] = (g * S["slope"][row(c), n].astype(F32)).astype(BF)
                return carry
            lax.fori_loop(0, hidden // block, body, 0)
            middle()
            wide(lambda n: mt(S["slope"][row(c), :], S["win"][n, :]), part, c)
        elif s == 4:
            set_delta(c, S["cmixed"], S["low3"], S["cwo"])
            each_head(lambda h: head_backward(h, c, S["cq"], S["ck"], S["cv"], S["ckt"], S["clse"], False, enc), middle)
            S["cq"][row(c), :] = unflatten().astype(BF)
            wide(lambda n: mt(S["cq"][row(c), :], S["cwq"][n, :]), part, c)
        elif s == 5:
            set_delta(c, S["mixed"], S["low4"], S["wo"])
            each_head(lambda h: head_backward(h, c, S["q"], S["k"], S["v"], S["kt"], S["lse"], True, dec), middle)
            S["q"][row(c), :] = unflatten().astype(BF)
            S["k"][row(c), :] = (S["dk"][row(c), :] * scale).astype(BF)
            S["v"][row(c), :] = S["dv"][row(c), :].astype(BF)
            wide(lambda n: mt(S["q"][row(c), :], S["wq"][n, :])
                 + mt(S["k"][row(c), :], S["wk"][n, :])
                 + mt(S["v"][row(c), :], S["wv"][n, :]), part, c)
        else:
            middle()
            wide(lambda n: mt(S["ck"][row(c), :], S["cwk"][n, :])
                 + mt(S["cv"][row(c), :], S["cwv"][n, :]), part, c)

    lows = [S["low0"], S["low1"], S["low2"], S["low3"], S["low4"], S["low2"], S["low1"]]

    def remote(src, dst, phase, c, peer):
        return pltpu.make_async_remote_copy(
            src_ref=src, dst_ref=dst, send_sem=S["ssem"].at[phase, c],
            recv_sem=S["rsem"].at[phase, c], device_id=peer, device_id_type=MESH)

    def core_part(c):
        theirs = pl.ds(pl.multiple_of((1 - kk) * HF, HF), HF)
        return remote(S["part"].at[c, theirs], S["rc"].at[c], 0, c, core)

    def y_part(c):
        theirs = pl.ds(pl.multiple_of((1 - yy) * Q, Q), Q)
        return remote(S["ys"].at[c, theirs], S["ry"].at[c], 1, c, ypar)

    def gather(buf, c, which, base):
        r = y_rows(c) if which == 2 else own_rows(c)
        return remote(buf.at[r], buf.at[r], base + which, c, ypar if which == 0 else core)

    def p0(c):
        core_part(c).start()

    def p1(c):
        core_part(c).wait()
        step = min(32, HF)

        def body(j, carry):
            r = pl.ds(pl.multiple_of(j * step, step), step)
            m = pl.ds(pl.multiple_of(kk * HF + j * step, step), step)
            S["ys"][c, r, :] = (S["part"][c, m, :].astype(F32)
                                + S["rc"][c, r, :].astype(F32)).astype(BF)
            return carry
        lax.fori_loop(0, HF // step, body, 0)
        y_part(c).start()

    def mean(x):
        return jnp.sum(x, axis=-1, keepdims=True) * (1.0 / width)

    def norm(x, j):
        center = x - mean(x)
        inv = lax.rsqrt(mean(center * center) + EPSILON)
        xhat = center * inv
        return xhat, inv, xhat * vec[2 * j:2 * j + 1, :] + vec[2 * j + 1:2 * j + 2, :]

    def fold(x):
        return jnp.sum(x.reshape(x.shape[0] // 8, 8, width), axis=0)

    def norm_back(e, xhat, inv, j):
        S["vacc"][2 * j] += fold(e * xhat)
        S["vacc"][2 * j + 1] += fold(e)
        eg = e * vec[2 * j:2 * j + 1, :]
        return (eg - mean(eg) - xhat * mean(eg * xhat)) * inv

    def p2(s, c):
        y_part(c).wait()
        if s == 2:
            @pl.when(c == 0)
            def _():
                for x in cots:
                    x.wait()
        step = min(16, Q)
        buf = lows[s]

        def body(j, carry):
            r = pl.ds(pl.multiple_of(j * step, step), step)
            m = pl.ds(pl.multiple_of(yy * Q + j * step, step), step)
            o = pl.ds(pl.multiple_of(c * R + kk * HF + yy * Q + j * step, step), step)
            x = S["ys"][c, m, :].astype(F32) + S["ry"][c, r, :].astype(F32)
            if s == 0:
                xhat, inv, y = norm(S["tok"][o, :].astype(F32) + x, 0)
                S["xh1"][c, r, :] = xhat
                S["rs1"][c, r, :] = inv
                S["res"][c, r, :] = y
            elif s == 1:
                xhat, inv, y = norm(S["res"][c, r, :] + x, 1)
                S["xh2"][c, r, :] = xhat
                S["rs2"][c, r, :] = inv
                S["res"][c, r, :] = y
            elif s == 2:
                xhat, inv, y = norm(S["res"][c, r, :] + x, 2)
                S["outs"][o, :] = y.astype(BF)
                rid = (c * R + kk * HF + yy * Q + j * step
                       + lax.broadcasted_iota(jnp.int32, (step, width), 0))
                seed = jnp.where(rid < dec, S["cot"][c, r, :].astype(F32), 0.0)
                y = norm_back(seed, xhat, inv, 2)
                S["res"][c, r, :] = y
            elif s == 3:
                y = norm_back(S["res"][c, r, :] + x, S["xh2"][c, r, :], S["rs2"][c, r, :], 1)
                S["res"][c, r, :] = y
            elif s == 4:
                y = norm_back(S["res"][c, r, :] + x, S["xh1"][c, r, :], S["rs1"][c, r, :], 0)
                S["res"][c, r, :] = y
            elif s == 5:
                y = S["res"][c, r, :] + x
            else:
                y = x
            buf[o, :] = y.astype(BF)
            return carry
        lax.fori_loop(0, Q // step, body, 0)
        gather(buf, c, 0, 2).start()
        gather(buf, c, 1, 2).start()

    def p3(s, c):
        gather(lows[s], c, 0, 2).wait()
        gather(lows[s], c, 2, 2).start()

    def p4(s, c):
        gather(lows[s], c, 1, 2).wait()
        gather(lows[s], c, 2, 2).wait()

    def grad_piece(g, i):
        n = pl.ds(pl.multiple_of(i * PIECE, PIECE), PIECE)
        r = pl.ds(pl.multiple_of((g * CHUNKS + i) * PIECE, PIECE), PIECE)
        if g == 0:
            S["gbuf"][r, :] = tm(S["hid"][:, n], S["low2"][...]).astype(BF)
        elif g == 1:
            S["gbuf"][r, :] = tm(S["low1"][:, n], S["slope"][...]).astype(BF)
        else:
            if g == 2:
                a, b, d = S["low0"], S["mem"], S["low3"]
                x, y, z, w = S["cq"], S["ck"], S["cv"], S["cmixed"]
            else:
                a, b, d = S["tok"], S["tok"], S["low4"]
                x, y, z, w = S["q"], S["k"], S["v"], S["mixed"]
            S["gbuf"][r, 0 * inner:1 * inner] = tm(a[:, n], x[...]).astype(BF)
            S["gbuf"][r, 1 * inner:2 * inner] = tm(b[:, n], y[...]).astype(BF)
            S["gbuf"][r, 2 * inner:3 * inner] = tm(b[:, n], z[...]).astype(BF)
            S["gbuf"][r, 3 * inner:4 * inner] = tm(w[...], d[:, n]).astype(BF)

    def weight(step, p):
        if bits < 2 or step > 1:
            return 1 << step
        swap = lax.div(lax.rem(p, 4), 3)
        return 1 + swap if step == 0 else 2 - swap

    def start_of(step, p):
        at = p * PIECE
        for j in range(step):
            if sizes[j][1]:
                at = at + side(weight(j, p)) * sizes[j][0]
        return at

    def piece_rows(at, n):
        return pl.ds(pl.multiple_of(at, n), n)

    def reduce_copy(step, p):
        n, halve = sizes[step]
        w = weight(step, p)
        at = start_of(step, p)
        if halve:
            at = at + (1 - side(w)) * n
        slot = lax.rem(p, RING)
        return pltpu.make_async_remote_copy(
            src_ref=S["gbuf"].at[piece_rows(at, n)], dst_ref=S[f"dr{step}"].at[slot],
            send_sem=S["dssem"].at[step, slot], recv_sem=S["drsem"].at[step, slot],
            device_id=dp_peer(w), device_id_type=MESH)

    def reduce_add(step, p):
        n, halve = sizes[step]
        at = start_of(step + 1, p)
        slot = lax.rem(p, RING)
        block = min(32, n)

        def body(j, carry):
            r = pl.ds(pl.multiple_of(at + j * block, block), block)
            m = pl.ds(pl.multiple_of(j * block, block), block)
            S["gbuf"][r, :] = (S["gbuf"][r, :].astype(F32)
                               + S[f"dr{step}"][slot, m, :].astype(F32)).astype(BF)
            return carry
        lax.fori_loop(0, n // block, body, 0)

    halved = sum(1 for _, h in sizes if h)
    steps = bits + halved

    def gather_copy(step, p):
        n, _ = sizes[step]
        r = S["gbuf"].at[piece_rows(start_of(step + 1, p), n)]
        slot = lax.rem(p, RING)
        return pltpu.make_async_remote_copy(
            src_ref=r, dst_ref=S["ag"].at[slot] if step == halved - 1 else r,
            send_sem=S["dssem"].at[bits + step, slot], recv_sem=S["drsem"].at[bits + step, slot],
            device_id=dp_peer(weight(step, p)), device_id_type=MESH)

    def gather_end(step, p):
        gather_copy(step, p).wait()
        if step == halved - 1:
            n, _ = sizes[step]
            at = start_of(step, p) + (1 - side(weight(step, p))) * n
            S["gbuf"][piece_rows(at, n), :] = S["ag"][lax.rem(p, RING)]

    def gather_begin(step, p):
        if step < halved - 1:
            pl.semaphore_wait(S["freed"].at[step, lax.rem(p, RING)], 1)
        gather_copy(step, p).start()

    def result_copies(p, ff):
        r = pl.ds(pl.multiple_of(p * PIECE, PIECE), PIECE)
        if ff:
            return [pltpu.make_async_copy(S["gbuf"].at[r], gf_h.at[r], S["gsem"].at[0, p])]
        g = lax.div(p - 2 * CHUNKS, CHUNKS)
        n = pl.ds(pl.multiple_of(lax.rem(p, CHUNKS) * PIECE, PIECE), PIECE)
        block = [S["gbuf"].at[r, pl.ds(j * inner, inner)] for j in range(4)]
        return [pltpu.make_async_copy(block[j], gq_h.at[g, j, n], S["gsem"].at[j, p])
                for j in range(3)] + [
            pltpu.make_async_copy(block[3], go_h.at[g, :, n], S["gsem"].at[3, p])]

    def dp_step(k, p):
        if 1 <= k <= bits:
            reduce_copy(k - 1, p).wait()
            if k < halved:
                pl.semaphore_signal(S["freed"].at[k - 1, lax.rem(p, RING)], inc=1,
                                    device_id=dp_peer(weight(k - 1, p)), device_id_type=MESH)
            reduce_add(k - 1, p)
        elif k > bits:
            gather_end(halved - (k - bits), p)
        if k < bits:
            reduce_copy(k, p).start()
        elif k < steps:
            gather_begin(halved - 1 - (k - bits), p)
        else:
            @pl.when(p < 2 * CHUNKS)
            def _():
                for x in result_copies(p, True):
                    x.start()

            @pl.when(p >= 2 * CHUNKS)
            def _():
                for x in result_copies(p, False):
                    x.start()

    lag = [0, 2] + [2 + k for k in range(1, steps - 1)] + [steps + 2]
    FIRST = 2 * CHUNKS
    GAP = FIRST + 2
    LAST = GAP + 4 * CHUNKS - 2

    def dp_slot(m):
        for k in [steps] + list(range(steps - 1, 1, -1)) + [0, 1]:
            e = m - lag[k]
            early = e < FIRST
            p = jnp.where(early, e, FIRST + lax.div(e - GAP, 2))

            @pl.when((e >= 0) & (e <= LAST)
                     & (early | ((e >= GAP) & (lax.rem(e, 2) == 0))))
            def _(k=k, p=p):
                dp_step(k, p)

    peers = [core, ypar] + [dp_peer(1 << j) for j in range(bits)]

    def vec_copy(k):
        return pltpu.make_async_remote_copy(
            src_ref=S["vsum"], dst_ref=S["vrec"].at[k], send_sem=S["vssem"].at[k],
            recv_sem=S["vrsem"].at[k], device_id=peers[k], device_id_type=MESH)

    def vec_step(k):
        if k == 0:
            S["vsum"][...] = jnp.sum(S["vacc"][...], axis=1)
        else:
            vec_copy(k - 1).wait()
            S["vsum"][...] += S["vrec"][k - 1]
        if k < len(peers):
            vec_copy(k).start()

    def chunk_of(s, i):
        return i if s <= 4 else CHUNKS - 1 - i

    def lagged(i, n, fn, s):
        def now():
            fn(s, chunk_of(s, i - n))

        def before():
            fn(s - 1, chunk_of(s - 1, i - n + CHUNKS))
        fresh = s in (0, 5)
        if isinstance(i, int):
            if i >= n:
                now()
            elif not fresh:
                before()
            return
        pl.when(i >= n)(now)
        if not fresh:
            pl.when(i < n)(before)

    def phases(i, s):
        lagged(i, 3, p3, s)
        lagged(i, 2, p2, s)
        lagged(i, 1, lambda _, c: p1(c), s)

    def ff_piece(m):
        @pl.when(m < CHUNKS)
        def _():
            grad_piece(0, m)

        @pl.when(m >= CHUNKS)
        def _():
            grad_piece(1, m - CHUNKS)

    def slot(i, s):
        c = chunk_of(s, i)
        if s > 0:
            p4(s - 1, c)
        if s == 5:
            gather(S["outs"], c, 0, 5).start()
            gather(S["outs"], c, 1, 5).start()

        def middle():
            phases(i, s)
            if s == 4:
                ff_piece(2 * i)
                dp_slot(2 * i)
            elif s > 4:
                grad_piece(s - 3, i)
                dp_slot(GAP + 2 * CHUNKS * (s - 5) + 2 * i)
            if s == 6:
                gather(S["outs"], c, 0, 5).wait()
                gather(S["outs"], c, 2, 5).start()
                for k in range(CHUNKS):
                    @pl.when(i == k)
                    def _(k=k):
                        vec_step(k)
        compute(s, c, middle)
        p0(c)
        if s == 4:
            ff_piece(2 * i + 1)
            dp_slot(2 * i + 1)
        elif s > 4:
            dp_slot(GAP + 2 * CHUNKS * (s - 5) + 2 * i + 1)

    def drain(s, t):
        a, b, d = (chunk_of(s, i) for i in (1, 2, 3))

        @pl.when(t == 0)
        def _():
            p3(s, a)
            p2(s, b)
            p1(d)

        @pl.when(t == 1)
        def _():
            p3(s, b)
            p2(s, d)

        @pl.when(t == 2)
        def _():
            p3(s, d)

    wait_for("tok", "wk", "wv", "wq", "wo")
    for i in range(CHUNKS):
        slot(i, 0)
        if i == 0:
            wait_for("mem", "cwk", "cwv")
        project(i, S["mem"], S["cwk"], S["cwv"], S["ck"], S["cv"], S["ckt"], S["cvt"])

    for s in range(1, STAGES):
        if s == 1:
            wait_for("cwq", "cwo")
        if s == 2:
            wait_for("win", "wout")
        if s in (4, 5):
            S["dk"][...] = jnp.zeros(S["dk"].shape, F32)
            S["dv"][...] = jnp.zeros(S["dv"].shape, F32)

        def body(i, carry, s=s):
            slot(i, s)
            return carry
        lax.fori_loop(0, CHUNKS, body, 0)
        if s == 4:
            S["ck"][...] = (S["dk"][...] * scale).astype(BF)
            S["cv"][...] = S["dv"][...].astype(BF)

            def between(t, carry):
                drain(4, t)

                @pl.when(t < 2)
                def _():
                    dp_slot(FIRST + t)
                return carry
            lax.fori_loop(0, 3, between, 0)

    last = STAGES - 1
    tail = LAST + 2
    outputs = [pltpu.make_async_copy(a, b, S["osem"].at[j])
               for j, (a, b) in enumerate(((S["outs"], out_h), (lows[5], tg_h), (lows[6], mg_h)))]

    def ending(m, carry):
        t = m - tail
        drain(last, t)

        @pl.when(t == 0)
        def _():
            for c in range(CHUNKS):
                gather(S["outs"], c, 1, 5).wait()
                gather(S["outs"], c, 2, 5).wait()
            outputs[0].start()
            outputs[1].start()

        @pl.when(t == 3)
        def _():
            for c in range(CHUNKS):
                p4(last, c)
            outputs[2].start()
        for k in range(CHUNKS, len(peers) + 1):
            @pl.when(t == k - CHUNKS)
            def _(k=k):
                vec_step(k)
        dp_slot(m)
        return carry
    lax.fori_loop(tail, LAST + lag[-1] + 1, ending, 0)
    vg_h[...] = S["vsum"][...]

    def finish(p, carry, ff):
        for x in result_copies(p, ff):
            x.wait()
        return carry
    lax.fori_loop(0, 2 * CHUNKS, lambda p, x: finish(p, x, True), 0)
    lax.fori_loop(2 * CHUNKS, pieces, lambda p, x: finish(p, x, False), 0)
    for x in outputs:
        x.wait()


def shards(
    tokens, memory, decoder_length, memory_length,
    self_query, self_key, self_value, self_output, self_gain, self_bias,
    cross_query, cross_key, cross_value, cross_output, cross_gain, cross_bias,
    feed_in, feed_out, feed_gain, feed_bias, cotangent,
):
    rows, width = tokens.shape
    slots = memory.shape[0]
    inner = self_query.shape[1]
    hidden = feed_in.shape[1]
    lens = jnp.concatenate([decoder_length, memory_length])
    vec = jnp.stack([self_gain, self_bias, cross_gain, cross_bias, feed_gain, feed_bias,
                     feed_gain, feed_bias])
    copies = lax.axis_size("dp")
    scratch = layout(rows, slots, width, inner, hidden, copies)
    names = tuple(scratch)
    given = dict(tok=tokens, mem=memory, wq=self_query, wk=self_key, wv=self_value,
                 wo=self_output, cwq=cross_query, cwk=cross_key, cwv=cross_value,
                 cwo=cross_output, win=feed_in, wout=feed_out)
    any_spec = pl.BlockSpec(memory_space=pl.ANY)

    def kernel(*refs):
        layer_kernel(names, copies, *refs)

    out, tg, mg, gf, gq, go, vg = pl.pallas_call(
        kernel,
        out_shape=(
            jax.ShapeDtypeStruct((rows, width), BF),
            jax.ShapeDtypeStruct((rows, width), BF),
            jax.ShapeDtypeStruct((slots, width), BF),
            jax.ShapeDtypeStruct((2 * hidden, width), BF),
            jax.ShapeDtypeStruct((2, 3, width, inner), BF),
            jax.ShapeDtypeStruct((2, inner, width), BF),
            jax.ShapeDtypeStruct((8, width), F32),
        ),
        in_specs=[pl.BlockSpec(memory_space=pltpu.SMEM), pl.BlockSpec(memory_space=pltpu.VMEM)]
        + [any_spec] * (len(INPUTS) + 1),
        out_specs=(any_spec,) * 6 + (pl.BlockSpec(memory_space=pltpu.VMEM),),
        scratch_shapes=list(scratch.values()),
        compiler_params=pltpu.CompilerParams(
            collective_id=0, has_side_effects=True, vmem_limit_bytes=67043328),
        name="layer",
    )(lens, vec, *[given[n] for n in INPUTS], cotangent)

    def wide_grads(j):
        return tuple(gq[j, i].astype(F32) for i in range(3)) + (go[j].astype(F32),)

    return (
        out, tg.astype(F32), mg.astype(F32),
        *wide_grads(1), vg[0], vg[1],
        *wide_grads(0), vg[2], vg[3],
        gf[hidden:].astype(F32), gf[:hidden].astype(F32), vg[4], vg[5],
    )


def solution(mesh):
    rows = P("dp", None)
    tail = P(None, "tensor")
    head = P("tensor", None)
    whole = P()
    return jax.shard_map(
        shards,
        mesh=mesh,
        in_specs=(
            rows, rows, P("dp"), P("dp"),
            tail, tail, tail, head, whole, whole,
            tail, tail, tail, head, whole, whole,
            tail, head, whole, whole, rows,
        ),
        out_specs=(
            rows, rows, rows,
            tail, tail, tail, head, whole, whole,
            tail, tail, tail, head, whole, whole,
            tail, head, whole, whole,
        ),
        check_vma=False,
    )
```

```python
import jax
import jax.numpy as jnp
from jax import lax
from jax.experimental import pallas as pl
from jax.experimental.pallas import tpu as pltpu
from jax.sharding import PartitionSpec as P

BF = jnp.bfloat16
F32 = jnp.float32
HD = 64
CHUNKS = 4
EPSILON = 1e-05
NEGATIVE = -1e30
MESH = pl.DeviceIdType.MESH
STAGES = 7


def mm(a, b):
    return lax.dot_general(a, b, (((1,), (0,)), ((), ())), preferred_element_type=F32)


def mt(a, b):
    return lax.dot_general(a, b, (((1,), (1,)), ((), ())), preferred_element_type=F32)


def tm(a, b):
    return lax.dot_general(a, b, (((0,), (0,)), ((), ())), preferred_element_type=F32)


PIECE = 256
RING = 12


def split_sizes(copies):
    sizes, rows = [], PIECE
    for _ in range(copies.bit_length() - 1):
        halve = rows // 2 >= 16
        rows = rows // 2 if halve else rows
        sizes.append((rows, halve))
    return sizes


def layout(rows, slots, width, inner, hidden, copies):
    sizes = split_sizes(copies)
    pieces = (2 * hidden + 2 * width) // PIECE
    heads = inner // HD
    chunk = rows // CHUNKS
    half, own = chunk // 2, chunk // 4
    v = pltpu.VMEM
    return dict(
        tok=v((rows, width), BF),
        mem=v((slots, width), BF),
        cot=v((CHUNKS, own, width), BF),
        wq=v((width, inner), BF),
        wk=v((width, inner), BF),
        wv=v((width, inner), BF),
        wo=v((inner, width), BF),
        cwq=v((width, inner), BF),
        cwk=v((width, inner), BF),
        cwv=v((width, inner), BF),
        cwo=v((inner, width), BF),
        win=v((width, hidden), BF),
        wout=v((hidden, width), BF),
        q=v((rows, inner), BF),
        k=v((rows, inner), BF),
        v=v((rows, inner), BF),
        kt=v((heads, HD, rows), BF),
        vt=v((heads, HD + 16, rows), BF),
        cq=v((rows, inner), BF),
        ck=v((slots, inner), BF),
        cv=v((slots, inner), BF),
        ckt=v((heads, HD, slots), BF),
        cvt=v((heads, HD + 16, slots), BF),
        mixed=v((rows, inner), BF),
        cmixed=v((rows, inner), BF),
        lse=v((CHUNKS, heads, 1, chunk), F32),
        clse=v((CHUNKS, heads, 1, chunk), F32),
        delta=v((heads, 1, chunk), F32),
        flat=v((inner, chunk), F32),
        dout=v((chunk, inner), BF),
        dk=v((rows, inner), F32),
        dv=v((rows, inner), F32),
        hid=v((rows, hidden), BF),
        slope=v((rows, hidden), BF),
        low0=v((rows, width), BF),
        low1=v((rows, width), BF),
        low2=v((rows, width), BF),
        low3=v((rows, width), BF),
        low4=v((rows, width), BF),
        outs=v((rows, width), BF),
        res=v((CHUNKS, own, width), F32),
        xh1=v((CHUNKS, own, width), F32),
        xh2=v((CHUNKS, own, width), F32),
        rs1=v((CHUNKS, own, 1), F32),
        rs2=v((CHUNKS, own, 1), F32),
        part=v((CHUNKS, chunk, width), BF),
        rc=v((CHUNKS, half, width), BF),
        ys=v((CHUNKS, half, width), BF),
        ry=v((CHUNKS, own, width), BF),
        vacc=v((8, 8, width), F32),
        gbuf=v((2 * hidden + 2 * width, width), BF),
        vsum=v((8, width), F32),
        vrec=v((len(sizes) + 2, 8, width), F32),
        **{f"dr{j}": v((RING, n, width), BF) for j, (n, _) in enumerate(sizes)},
        ag=v((RING, [n for n, h in sizes if h][-1], width), BF),
        freed=pltpu.SemaphoreType.REGULAR((len(sizes), RING)),
        dssem=pltpu.SemaphoreType.DMA((2 * len(sizes), RING)),
        drsem=pltpu.SemaphoreType.DMA((2 * len(sizes), RING)),
        gsem=pltpu.SemaphoreType.DMA((4, pieces)),
        vssem=pltpu.SemaphoreType.DMA((len(sizes) + 2,)),
        vrsem=pltpu.SemaphoreType.DMA((len(sizes) + 2,)),
        insem=pltpu.SemaphoreType.DMA((16,)),
        cotsem=pltpu.SemaphoreType.DMA((CHUNKS,)),
        osem=pltpu.SemaphoreType.DMA((4,)),
        ssem=pltpu.SemaphoreType.DMA((8, CHUNKS)),
        rsem=pltpu.SemaphoreType.DMA((8, CHUNKS)),
    )


INPUTS = (
    "tok", "wk", "wv", "wq", "wo", "mem", "cwk", "cwv", "cwq", "cwo",
    "win", "wout",
)


def layer_kernel(names, copies, *refs):
    dec_ref, enc_ref = refs[:2]
    vec = refs[2:8]
    refs = refs[8:]
    n_in = len(INPUTS)
    srcs = dict(zip(INPUTS, refs[:n_in]))
    cot_h = refs[n_in]
    out_h, tg_h, mg_h, gf_h, gq_h, go_h, vg_h = refs[n_in + 1:n_in + 8]
    S = dict(zip(names, refs[n_in + 8:]))

    rows, width = S["tok"].shape
    slots = S["mem"].shape[0]
    inner = S["wq"].shape[1]
    hidden = S["win"].shape[1]
    heads = inner // HD
    R = rows // CHUNKS
    HF, Q = R // 2, R // 4
    scale = HD ** -0.5
    t = lax.axis_index("tensor")
    yy = t // 2
    kk = t % 2
    core = {"tensor": t + 1 - 2 * kk}
    ypar = {"tensor": t + 2 - 4 * yy}

    me = lax.axis_index("dp")
    sizes = split_sizes(copies)
    bits = len(sizes)
    pieces = (2 * hidden + 2 * width) // PIECE

    def side(weight):
        return lax.rem(lax.div(me, weight), 2)

    def dp_peer(weight):
        return {"dp": me + weight * (1 - 2 * side(weight))}

    def row(c):
        return pl.ds(pl.multiple_of(c * R, R), R)

    def own_rows(c):
        return pl.ds(pl.multiple_of(c * R + kk * HF + yy * Q, Q), Q)

    def y_rows(c):
        return pl.ds(pl.multiple_of(c * R + kk * HF + (1 - yy) * Q, Q), Q)

    loads = {n: pltpu.make_async_copy(srcs[n], S[n], S["insem"].at[j])
             for j, n in enumerate(INPUTS)}
    cots = [pltpu.make_async_copy(cot_h.at[own_rows(c)], S["cot"].at[c], S["cotsem"].at[c])
            for c in range(CHUNKS)]
    for n in INPUTS[:5]:
        loads[n].start()

    barrier = pltpu.get_barrier_semaphore()
    for peer in [core, ypar] + [dp_peer(1 << j) for j in range(bits)]:
        pl.semaphore_signal(barrier, inc=1, device_id=peer, device_id_type=MESH)

    S["vt"][:, HD:, :] = jnp.ones((heads, 16, rows), BF)
    S["cvt"][:, HD:, :] = jnp.ones((heads, 16, slots), BF)
    S["vacc"][...] = jnp.zeros(S["vacc"].shape, F32)

    def wait_for(*which):
        for n in which:
            loads[n].wait()

    def project(c, src, wk, wv, kd, vd, ktd, vtd):
        r = row(c)
        x = src[r, :]
        kf = mm(x, wk[...])
        kd[r, :] = kf.astype(BF)
        kt = kf.T.astype(BF)
        vf = mm(x, wv[...])
        vd[r, :] = vf.astype(BF)
        vtt = vf.T.astype(BF)
        for h in range(heads):
            ktd[h, :, r] = kt[h * HD:(h + 1) * HD, :]
            vtd[h, :HD, r] = vtt[h * HD:(h + 1) * HD, :]

    def lanes(h):
        return pl.ds(pl.multiple_of((h // 2) * 2 * HD, 2 * HD), 2 * HD)

    def pick(x, h):
        lane = lax.broadcasted_iota(jnp.int32, x.shape, 1) // HD
        return jnp.where(lane == h % 2, x, jnp.zeros_like(x))

    def masked(scores, c, causal, length):
        kid = lax.broadcasted_iota(jnp.int32, scores.shape, 0)
        ok = kid < length
        if causal:
            qid = c * R + lax.broadcasted_iota(jnp.int32, scores.shape, 1)
            ok = ok & (kid <= qid)
        return jnp.where(ok, scores * scale, NEGATIVE)

    def head_forward(h, c, q, k, vt, lse, causal, length, keys):
        qm = pick(q[row(c), lanes(h)], h)
        s = masked(mt(k[:keys, lanes(h)], qm), c, causal, length)
        top = jnp.max(s, axis=0, keepdims=True)
        p = jnp.exp(s - top).astype(BF)
        o = mm(vt[h, :, :keys], p)
        total = o[HD:HD + 1, :]
        S["flat"][pl.ds(pl.multiple_of(h * HD, HD), HD), :] = o[:HD, :] / total
        lse[c, h] = top + jnp.log(total)

    def head_backward(h, c, q, k, v, kt, lse, causal, length):
        qm = pick(q[row(c), lanes(h)], h)
        s = masked(mt(k[:, lanes(h)], qm), c, causal, length)
        p = jnp.exp(s - lse[c, h])
        dom = pick(S["dout"][:, lanes(h)], h)
        dp = mt(v[:, lanes(h)], dom)
        S["dv"][:, lanes(h)] += mm(p.astype(BF), dom)
        ds = (p * (dp - S["delta"][h])).astype(BF)
        S["dk"][:, lanes(h)] += mm(ds, qm)
        S["flat"][pl.ds(pl.multiple_of(h * HD, HD), HD), :] = mm(kt[h], ds) * scale

    def unflatten():
        return S["flat"][...].T

    def wide(fn, dst, c):
        block = min(256, width)

        def body(j, carry):
            cols = pl.ds(pl.multiple_of(j * block, block), block)
            dst[c, :, cols] = fn(cols).astype(BF)
            return carry
        lax.fori_loop(0, width // block, body, 0)

    def set_delta(c, mixed, low, w):
        do = mt(low[row(c), :], w[...]).astype(BF)
        S["dout"][...] = do
        prod = do.astype(F32) * mixed[row(c), :].astype(F32)
        sel = (lax.broadcasted_iota(jnp.int32, (8, inner), 1) // HD
               == lax.broadcasted_iota(jnp.int32, (8, inner), 0)).astype(F32)
        d = lax.dot_general(sel, prod, (((1,), (1,)), ((), ())),
                            precision=lax.Precision.HIGHEST, preferred_element_type=F32)
        for h in range(heads):
            S["delta"][h] = d[h:h + 1, :]

    dec = dec_ref[0]
    enc = enc_ref[0]

    def each_head(fn, middle):
        def body(h, carry):
            @pl.when(h == heads // 2)
            def _():
                middle()
            fn(h)
            return carry
        lax.fori_loop(0, heads, body, 0)

    def compute(s, c, middle):
        part = S["part"]
        if s == 0:
            project(c, S["tok"], S["wk"], S["wv"], S["k"], S["v"], S["kt"], S["vt"])
            S["q"][row(c), :] = mm(S["tok"][row(c), :], S["wq"][...]).astype(BF)
            each_head(lambda h: head_forward(h, c, S["q"], S["k"], S["vt"], S["lse"], True, dec,
                                             (c + 1) * R), middle)
            S["mixed"][row(c), :] = unflatten().astype(BF)
            wide(lambda n: mm(S["mixed"][row(c), :], S["wo"][:, n]), part, c)
        elif s == 1:
            S["cq"][row(c), :] = mm(S["low0"][row(c), :], S["cwq"][...]).astype(BF)
            each_head(lambda h: head_forward(h, c, S["cq"], S["ck"], S["cvt"], S["clse"], False, enc, slots), middle)
            S["cmixed"][row(c), :] = unflatten().astype(BF)
            wide(lambda n: mm(S["cmixed"][row(c), :], S["cwo"][:, n]), part, c)
        elif s == 2:
            block = min(256, hidden)

            def body(j, carry):
                n = pl.ds(pl.multiple_of(j * block, block), block)
                v = mm(S["low1"][row(c), :], S["win"][:, n])
                cdf = 0.5 * (1.0 + lax.erf(v * 0.7071067811865476))
                S["hid"][row(c), n] = (v * cdf).astype(BF)
                S["slope"][row(c), n] = (
                    cdf + v * jnp.exp(-0.5 * v * v) * 0.3989422804014327).astype(BF)
                return carry
            lax.fori_loop(0, hidden // block, body, 0)
            middle()
            wide(lambda n: mm(S["hid"][row(c), :], S["wout"][:, n]), part, c)
        elif s == 3:
            block = min(256, hidden)

            def body(j, carry):
                n = pl.ds(pl.multiple_of(j * block, block), block)
                g = mt(S["low2"][row(c), :], S["wout"][n, :])
                S["slope"][row(c), n] = (g * S["slope"][row(c), n].astype(F32)).astype(BF)
                return carry
            lax.fori_loop(0, hidden // block, body, 0)
            middle()
            wide(lambda n: mt(S["slope"][row(c), :], S["win"][n, :]), part, c)
        elif s == 4:
            set_delta(c, S["cmixed"], S["low3"], S["cwo"])
            each_head(lambda h: head_backward(h, c, S["cq"], S["ck"], S["cv"], S["ckt"], S["clse"], False, enc), middle)
            S["cq"][row(c), :] = unflatten().astype(BF)
            wide(lambda n: mt(S["cq"][row(c), :], S["cwq"][n, :]), part, c)
        elif s == 5:
            set_delta(c, S["mixed"], S["low4"], S["wo"])
            each_head(lambda h: head_backward(h, c, S["q"], S["k"], S["v"], S["kt"], S["lse"], True, dec), middle)
            S["q"][row(c), :] = unflatten().astype(BF)
            S["k"][row(c), :] = (S["dk"][row(c), :] * scale).astype(BF)
            S["v"][row(c), :] = S["dv"][row(c), :].astype(BF)
            wide(lambda n: mt(S["q"][row(c), :], S["wq"][n, :])
                 + mt(S["k"][row(c), :], S["wk"][n, :])
                 + mt(S["v"][row(c), :], S["wv"][n, :]), part, c)
        else:
            middle()
            wide(lambda n: mt(S["ck"][row(c), :], S["cwk"][n, :])
                 + mt(S["cv"][row(c), :], S["cwv"][n, :]), part, c)

    lows = [S["low0"], S["low1"], S["low2"], S["low3"], S["low4"], S["low2"], S["low1"]]

    def remote(src, dst, phase, c, peer):
        return pltpu.make_async_remote_copy(
            src_ref=src, dst_ref=dst, send_sem=S["ssem"].at[phase, c],
            recv_sem=S["rsem"].at[phase, c], device_id=peer, device_id_type=MESH)

    def core_part(c):
        theirs = pl.ds(pl.multiple_of((1 - kk) * HF, HF), HF)
        return remote(S["part"].at[c, theirs], S["rc"].at[c], 0, c, core)

    def y_part(c):
        theirs = pl.ds(pl.multiple_of((1 - yy) * Q, Q), Q)
        return remote(S["ys"].at[c, theirs], S["ry"].at[c], 1, c, ypar)

    def gather(buf, c, which, base):
        r = y_rows(c) if which == 2 else own_rows(c)
        return remote(buf.at[r], buf.at[r], base + which, c, ypar if which == 0 else core)

    def p0(c):
        core_part(c).start()

    def p1(c):
        core_part(c).wait()
        step = min(32, HF)

        def body(j, carry):
            r = pl.ds(pl.multiple_of(j * step, step), step)
            m = pl.ds(pl.multiple_of(kk * HF + j * step, step), step)
            S["ys"][c, r, :] = (S["part"][c, m, :].astype(F32)
                                + S["rc"][c, r, :].astype(F32)).astype(BF)
            return carry
        lax.fori_loop(0, HF // step, body, 0)
        y_part(c).start()

    def mean(x):
        return jnp.sum(x, axis=-1, keepdims=True) * (1.0 / width)

    def norm(x, j):
        center = x - mean(x)
        inv = lax.rsqrt(mean(center * center) + EPSILON)
        xhat = center * inv
        return xhat, inv, xhat * vec[2 * j][...] + vec[2 * j + 1][...]

    def fold(x):
        return jnp.sum(x.reshape(x.shape[0] // 8, 8, width), axis=0)

    def norm_back(e, xhat, inv, j):
        S["vacc"][2 * j] += fold(e * xhat)
        S["vacc"][2 * j + 1] += fold(e)
        eg = e * vec[2 * j][...]
        return (eg - mean(eg) - xhat * mean(eg * xhat)) * inv

    def p2(s, c):
        y_part(c).wait()
        if s == 2:
            @pl.when(c == 0)
            def _():
                for x in cots:
                    x.wait()
        step = min(16, Q)
        buf = lows[s]

        def body(j, carry):
            r = pl.ds(pl.multiple_of(j * step, step), step)
            m = pl.ds(pl.multiple_of(yy * Q + j * step, step), step)
            o = pl.ds(pl.multiple_of(c * R + kk * HF + yy * Q + j * step, step), step)
            x = S["ys"][c, m, :].astype(F32) + S["ry"][c, r, :].astype(F32)
            if s == 0:
                xhat, inv, y = norm(S["tok"][o, :].astype(F32) + x, 0)
                S["xh1"][c, r, :] = xhat
                S["rs1"][c, r, :] = inv
                S["res"][c, r, :] = y
            elif s == 1:
                xhat, inv, y = norm(S["res"][c, r, :] + x, 1)
                S["xh2"][c, r, :] = xhat
                S["rs2"][c, r, :] = inv
                S["res"][c, r, :] = y
            elif s == 2:
                xhat, inv, y = norm(S["res"][c, r, :] + x, 2)
                S["outs"][o, :] = y.astype(BF)
                rid = (c * R + kk * HF + yy * Q + j * step
                       + lax.broadcasted_iota(jnp.int32, (step, width), 0))
                seed = jnp.where(rid < dec, S["cot"][c, r, :].astype(F32), 0.0)
                y = norm_back(seed, xhat, inv, 2)
                S["res"][c, r, :] = y
            elif s == 3:
                y = norm_back(S["res"][c, r, :] + x, S["xh2"][c, r, :], S["rs2"][c, r, :], 1)
                S["res"][c, r, :] = y
            elif s == 4:
                y = norm_back(S["res"][c, r, :] + x, S["xh1"][c, r, :], S["rs1"][c, r, :], 0)
                S["res"][c, r, :] = y
            elif s == 5:
                y = S["res"][c, r, :] + x
            else:
                y = x
            buf[o, :] = y.astype(BF)
            return carry
        lax.fori_loop(0, Q // step, body, 0)
        gather(buf, c, 0, 2).start()
        gather(buf, c, 1, 2).start()

    def p3(s, c):
        gather(lows[s], c, 0, 2).wait()
        gather(lows[s], c, 2, 2).start()

    def p4(s, c):
        gather(lows[s], c, 1, 2).wait()
        gather(lows[s], c, 2, 2).wait()

    def grad_piece(g, i):
        n = pl.ds(pl.multiple_of(i * PIECE, PIECE), PIECE)
        r = pl.ds(pl.multiple_of((g * CHUNKS + i) * PIECE, PIECE), PIECE)
        if g == 0:
            S["gbuf"][r, :] = tm(S["hid"][:, n], S["low2"][...]).astype(BF)
        elif g == 1:
            S["gbuf"][r, :] = tm(S["low1"][:, n], S["slope"][...]).astype(BF)
        else:
            if g == 2:
                a, b, d = S["low0"], S["mem"], S["low3"]
                x, y, z, w = S["cq"], S["ck"], S["cv"], S["cmixed"]
            else:
                a, b, d = S["tok"], S["tok"], S["low4"]
                x, y, z, w = S["q"], S["k"], S["v"], S["mixed"]
            S["gbuf"][r, 0 * inner:1 * inner] = tm(a[:, n], x[...]).astype(BF)
            S["gbuf"][r, 1 * inner:2 * inner] = tm(b[:, n], y[...]).astype(BF)
            S["gbuf"][r, 2 * inner:3 * inner] = tm(b[:, n], z[...]).astype(BF)
            S["gbuf"][r, 3 * inner:4 * inner] = tm(w[...], d[:, n]).astype(BF)

    def weight(step, p):
        if bits < 2 or step > 1:
            return 1 << step
        swap = lax.div(lax.rem(p, 4), 3)
        return 1 + swap if step == 0 else 2 - swap

    def start_of(step, p):
        at = p * PIECE
        for j in range(step):
            if sizes[j][1]:
                at = at + side(weight(j, p)) * sizes[j][0]
        return at

    def piece_rows(at, n):
        return pl.ds(pl.multiple_of(at, n), n)

    def reduce_copy(step, p):
        n, halve = sizes[step]
        w = weight(step, p)
        at = start_of(step, p)
        if halve:
            at = at + (1 - side(w)) * n
        slot = lax.rem(p, RING)
        return pltpu.make_async_remote_copy(
            src_ref=S["gbuf"].at[piece_rows(at, n)], dst_ref=S[f"dr{step}"].at[slot],
            send_sem=S["dssem"].at[step, slot], recv_sem=S["drsem"].at[step, slot],
            device_id=dp_peer(w), device_id_type=MESH)

    def reduce_add(step, p):
        n, halve = sizes[step]
        at = start_of(step + 1, p)
        slot = lax.rem(p, RING)
        block = min(32, n)

        def body(j, carry):
            r = pl.ds(pl.multiple_of(at + j * block, block), block)
            m = pl.ds(pl.multiple_of(j * block, block), block)
            S["gbuf"][r, :] = (S["gbuf"][r, :].astype(F32)
                               + S[f"dr{step}"][slot, m, :].astype(F32)).astype(BF)
            return carry
        lax.fori_loop(0, n // block, body, 0)

    halved = sum(1 for _, h in sizes if h)
    steps = bits + halved

    def gather_copy(step, p):
        n, _ = sizes[step]
        r = S["gbuf"].at[piece_rows(start_of(step + 1, p), n)]
        slot = lax.rem(p, RING)
        return pltpu.make_async_remote_copy(
            src_ref=r, dst_ref=S["ag"].at[slot] if step == halved - 1 else r,
            send_sem=S["dssem"].at[bits + step, slot], recv_sem=S["drsem"].at[bits + step, slot],
            device_id=dp_peer(weight(step, p)), device_id_type=MESH)

    def gather_end(step, p):
        gather_copy(step, p).wait()
        if step == halved - 1:
            n, _ = sizes[step]
            at = start_of(step, p) + (1 - side(weight(step, p))) * n
            S["gbuf"][piece_rows(at, n), :] = S["ag"][lax.rem(p, RING)]

    def gather_begin(step, p):
        if step < halved - 1:
            pl.semaphore_wait(S["freed"].at[step, lax.rem(p, RING)], 1)
        gather_copy(step, p).start()

    def result_copies(p, ff):
        r = pl.ds(pl.multiple_of(p * PIECE, PIECE), PIECE)
        if ff:
            return [pltpu.make_async_copy(S["gbuf"].at[r], gf_h.at[r], S["gsem"].at[0, p])]
        g = lax.div(p - 2 * CHUNKS, CHUNKS)
        n = pl.ds(pl.multiple_of(lax.rem(p, CHUNKS) * PIECE, PIECE), PIECE)
        block = [S["gbuf"].at[r, pl.ds(j * inner, inner)] for j in range(4)]
        return [pltpu.make_async_copy(block[j], gq_h.at[g, j, n], S["gsem"].at[j, p])
                for j in range(3)] + [
            pltpu.make_async_copy(block[3], go_h.at[g, :, n], S["gsem"].at[3, p])]

    def dp_step(k, p):
        if 1 <= k <= bits:
            reduce_copy(k - 1, p).wait()
            if k < halved:
                pl.semaphore_signal(S["freed"].at[k - 1, lax.rem(p, RING)], inc=1,
                                    device_id=dp_peer(weight(k - 1, p)), device_id_type=MESH)
            reduce_add(k - 1, p)
        elif k > bits:
            gather_end(halved - (k - bits), p)
        if k < bits:
            reduce_copy(k, p).start()
        elif k < steps:
            gather_begin(halved - 1 - (k - bits), p)
        else:
            @pl.when(p < 2 * CHUNKS)
            def _():
                for x in result_copies(p, True):
                    x.start()

            @pl.when(p >= 2 * CHUNKS)
            def _():
                for x in result_copies(p, False):
                    x.start()

    lag = [2 * k for k in range(steps + 1)]
    FIRST = 2 * CHUNKS
    GAP = FIRST + 2
    LAST = GAP + 4 * CHUNKS - 2

    def dp_slot(m):
        for k in list(range(steps - 1, -1, -1)) + [steps]:
            e = m - lag[k]
            early = e < FIRST
            p = jnp.where(early, e, FIRST + lax.div(e - GAP, 2))

            @pl.when((e >= 0) & (e <= LAST)
                     & (early | ((e >= GAP) & (lax.rem(e, 2) == 0))))
            def _(k=k, p=p):
                dp_step(k, p)

    peers = [core, ypar] + [dp_peer(1 << j) for j in range(bits)]

    def vec_copy(k):
        return pltpu.make_async_remote_copy(
            src_ref=S["vsum"], dst_ref=S["vrec"].at[k], send_sem=S["vssem"].at[k],
            recv_sem=S["vrsem"].at[k], device_id=peers[k], device_id_type=MESH)

    def vec_step(k):
        if k == 0:
            S["vsum"][...] = jnp.sum(S["vacc"][...], axis=1)
        else:
            vec_copy(k - 1).wait()
            S["vsum"][...] += S["vrec"][k - 1]
        if k < len(peers):
            vec_copy(k).start()

    def chunk_of(s, i):
        return i if s <= 4 else CHUNKS - 1 - i

    def lagged(i, n, fn, s):
        def now():
            fn(s, chunk_of(s, i - n))

        def before():
            fn(s - 1, chunk_of(s - 1, i - n + CHUNKS))
        fresh = s in (0, 5)
        if isinstance(i, int):
            if i >= n:
                now()
            elif not fresh:
                before()
            return
        pl.when(i >= n)(now)
        if not fresh:
            pl.when(i < n)(before)

    def phases(i, s):
        lagged(i, 1, lambda _, c: p1(c), s)
        lagged(i, 2, p2, s)
        lagged(i, 3, p3, s)

    def ff_piece(m):
        @pl.when(m < CHUNKS)
        def _():
            grad_piece(0, m)

        @pl.when(m >= CHUNKS)
        def _():
            grad_piece(1, m - CHUNKS)

    def slot(i, s):
        c = chunk_of(s, i)
        if s > 0:
            p4(s - 1, c)
        if s == 5:
            gather(S["outs"], c, 0, 5).start()
            gather(S["outs"], c, 1, 5).start()

        def middle():
            phases(i, s)
            if s == 4:
                ff_piece(2 * i)
                dp_slot(2 * i)
            elif s > 4:
                grad_piece(s - 3, i)
                dp_slot(GAP + 2 * CHUNKS * (s - 5) + 2 * i)
            if s == 6:
                gather(S["outs"], c, 0, 5).wait()
                gather(S["outs"], c, 2, 5).start()
                for k in range(CHUNKS):
                    @pl.when(i == k)
                    def _(k=k):
                        vec_step(k)
        compute(s, c, middle)
        if s == 0 and i == 0:
            pl.semaphore_wait(barrier, 2 + bits)
        p0(c)
        if s == 4:
            ff_piece(2 * i + 1)
            dp_slot(2 * i + 1)
        elif s > 4:
            dp_slot(GAP + 2 * CHUNKS * (s - 5) + 2 * i + 1)

    def drain(s, t):
        a, b, d = (chunk_of(s, i) for i in (1, 2, 3))

        @pl.when(t == 0)
        def _():
            p3(s, a)
            p2(s, b)
            p1(d)

        @pl.when(t == 1)
        def _():
            p3(s, b)
            p2(s, d)

        @pl.when(t == 2)
        def _():
            p3(s, d)

    wait_for("tok", "wk", "wv", "wq", "wo")
    for n in INPUTS[5:]:
        loads[n].start()
    for x in cots:
        x.start()
    for i in range(CHUNKS):
        slot(i, 0)
        if i == 0:
            wait_for("mem", "cwk", "cwv")
        project(i, S["mem"], S["cwk"], S["cwv"], S["ck"], S["cv"], S["ckt"], S["cvt"])

    for s in range(1, STAGES):
        if s == 1:
            wait_for("cwq", "cwo")
        if s == 2:
            wait_for("win", "wout")
        if s in (4, 5):
            S["dk"][...] = jnp.zeros(S["dk"].shape, F32)
            S["dv"][...] = jnp.zeros(S["dv"].shape, F32)

        def body(i, carry, s=s):
            slot(i, s)
            return carry
        lax.fori_loop(0, CHUNKS, body, 0)
        if s == 4:
            S["ck"][...] = (S["dk"][...] * scale).astype(BF)
            S["cv"][...] = S["dv"][...].astype(BF)

            def between(t, carry):
                drain(4, t)

                @pl.when(t < 2)
                def _():
                    dp_slot(FIRST + t)
                return carry
            lax.fori_loop(0, 3, between, 0)

    last = STAGES - 1
    tail = LAST + 2
    outputs = [pltpu.make_async_copy(a, b, S["osem"].at[j])
               for j, (a, b) in enumerate(((S["outs"], out_h), (lows[5], tg_h), (lows[6], mg_h)))]

    def ending(m, carry):
        t = m - tail
        dp_slot(m)
        drain(last, t)

        @pl.when(t == 0)
        def _():
            for c in range(CHUNKS):
                gather(S["outs"], c, 1, 5).wait()
                gather(S["outs"], c, 2, 5).wait()
            outputs[0].start()
            outputs[1].start()

        @pl.when(t == 3)
        def _():
            for c in range(CHUNKS):
                p4(last, c)
            outputs[2].start()
        for k in range(CHUNKS, len(peers) + 1):
            @pl.when(t == k - CHUNKS)
            def _(k=k):
                vec_step(k)
        return carry
    lax.fori_loop(tail, LAST + lag[-1] + 1, ending, 0)
    vg_h[...] = S["vsum"][...]

    def finish(p, carry, ff):
        for x in result_copies(p, ff):
            x.wait()
        return carry
    lax.fori_loop(0, 2 * CHUNKS, lambda p, x: finish(p, x, True), 0)
    lax.fori_loop(2 * CHUNKS, pieces, lambda p, x: finish(p, x, False), 0)
    for x in outputs:
        x.wait()


def widen(out, tg, mg, gf, gq, go):
    parts = 8
    width = out.shape[1]
    hidden = gf.shape[0] // 2
    inner = gq.shape[-1]
    row_specs, shapes, ins, in_specs = [], [], [], []

    def add(x, rows, columns, spec, dtype=F32):
        ins.append(x)
        in_specs.append(spec)
        row_specs.append(pl.BlockSpec((rows // parts, columns), lambda i: (i, 0)))
        shapes.append(jax.ShapeDtypeStruct((rows, columns), dtype))

    for x, dtype in ((out, BF), (tg, F32), (mg, F32)):
        n = x.shape[0]
        add(x, n, width, pl.BlockSpec((n // parts, width), lambda i: (i, 0)), dtype)
    for g in (1, 0):
        for j in range(3):
            add(gq, width, inner, pl.BlockSpec(
                (None, None, width // parts, inner), lambda i, g=g, j=j: (g, j, i, 0)))
        add(go, inner, width, pl.BlockSpec(
            (None, inner // parts, width), lambda i, g=g: (g, i, 0)))
    for g in range(2):
        add(gf, hidden, width, pl.BlockSpec(
            (hidden // parts, width), lambda i, g=g: (g * parts + i, 0)))

    def body(*refs):
        n = len(ins)
        for a, b in zip(refs[:n], refs[n:]):
            b[...] = a[...].astype(b.dtype)

    return pl.pallas_call(
        body, out_shape=tuple(shapes), grid=(parts,), in_specs=in_specs,
        out_specs=tuple(row_specs), name="widen",
        compiler_params=pltpu.CompilerParams(dimension_semantics=("arbitrary",)),
    )(*ins)


def shards(
    tokens, memory, decoder_length, memory_length,
    self_query, self_key, self_value, self_output, self_gain, self_bias,
    cross_query, cross_key, cross_value, cross_output, cross_gain, cross_bias,
    feed_in, feed_out, feed_gain, feed_bias, cotangent,
):
    rows, width = tokens.shape
    slots = memory.shape[0]
    inner = self_query.shape[1]
    hidden = feed_in.shape[1]
    vecs = [x.reshape(1, width) for x in (
        self_gain, self_bias, cross_gain, cross_bias, feed_gain, feed_bias)]
    copies = lax.axis_size("dp")
    scratch = layout(rows, slots, width, inner, hidden, copies)
    names = tuple(scratch)
    given = dict(tok=tokens, mem=memory, wq=self_query, wk=self_key, wv=self_value,
                 wo=self_output, cwq=cross_query, cwk=cross_key, cwv=cross_value,
                 cwo=cross_output, win=feed_in, wout=feed_out)
    any_spec = pl.BlockSpec(memory_space=pl.ANY)

    def kernel(*refs):
        layer_kernel(names, copies, *refs)

    out, tg, mg, gf, gq, go, vg = pl.pallas_call(
        kernel,
        out_shape=(
            jax.ShapeDtypeStruct((rows, width), BF),
            jax.ShapeDtypeStruct((rows, width), BF),
            jax.ShapeDtypeStruct((slots, width), BF),
            jax.ShapeDtypeStruct((2 * hidden, width), BF),
            jax.ShapeDtypeStruct((2, 3, width, inner), BF),
            jax.ShapeDtypeStruct((2, inner, width), BF),
            jax.ShapeDtypeStruct((8, width), F32),
        ),
        in_specs=[pl.BlockSpec(memory_space=pltpu.SMEM)] * 2
        + [pl.BlockSpec(memory_space=pltpu.VMEM)] * 6 + [any_spec] * (len(INPUTS) + 1),
        out_specs=(any_spec,) * 6 + (pl.BlockSpec(memory_space=pltpu.VMEM),),
        scratch_shapes=list(scratch.values()),
        compiler_params=pltpu.CompilerParams(
            collective_id=0, has_side_effects=True, vmem_limit_bytes=67043328),
        name="layer",
    )(decoder_length, memory_length, *vecs, *[given[n] for n in INPUTS], cotangent)

    wide = widen(out, tg, mg, gf, gq, go)
    return (
        *wide[:3],
        *wide[3:7], vg[0], vg[1],
        *wide[7:11], vg[2], vg[3],
        wide[12], wide[11], vg[4], vg[5],
    )


def solution(mesh):
    rows = P("dp", None)
    tail = P(None, "tensor")
    head = P("tensor", None)
    whole = P()
    return jax.shard_map(
        shards,
        mesh=mesh,
        in_specs=(
            rows, rows, P("dp"), P("dp"),
            tail, tail, tail, head, whole, whole,
            tail, tail, tail, head, whole, whole,
            tail, head, whole, whole, rows,
        ),
        out_specs=(
            rows, rows, rows,
            tail, tail, tail, head, whole, whole,
            tail, tail, tail, head, whole, whole,
            tail, head, whole, whole,
        ),
        check_vma=False,
    )
```

```python
import jax
import jax.numpy as jnp
from jax import lax
from jax.experimental import pallas as pl
from jax.experimental.pallas import tpu as pltpu
from jax.sharding import PartitionSpec as P

BF = jnp.bfloat16
F32 = jnp.float32
HD = 64
CHUNKS = 4
EPSILON = 1e-05
NEGATIVE = -1e30
MESH = pl.DeviceIdType.MESH
STAGES = 7


def mm(a, b):
    return lax.dot_general(a, b, (((1,), (0,)), ((), ())), preferred_element_type=F32)


def mt(a, b):
    return lax.dot_general(a, b, (((1,), (1,)), ((), ())), preferred_element_type=F32)


def tm(a, b):
    return lax.dot_general(a, b, (((0,), (0,)), ((), ())), preferred_element_type=F32)


PIECE = 256
RING = 12
SWAPPED = 0b0101000000001010
WAITS = (2, 2, 2, 3, 4, 4)


def split_sizes(copies):
    sizes, rows = [], PIECE
    for _ in range(copies.bit_length() - 1):
        halve = rows // 2 >= 16
        rows = rows // 2 if halve else rows
        sizes.append((rows, halve))
    return sizes


def layout(rows, slots, width, inner, hidden, copies):
    sizes = split_sizes(copies)
    pieces = (2 * hidden + 2 * width) // PIECE
    heads = inner // HD
    chunk = rows // CHUNKS
    half, own = chunk // 2, chunk // 4
    v = pltpu.VMEM
    return dict(
        tok=v((rows, width), BF),
        mem=v((slots, width), BF),
        cot=v((CHUNKS, own, width), BF),
        wq=v((width, inner), BF),
        wk=v((width, inner), BF),
        wv=v((width, inner), BF),
        wo=v((inner, width), BF),
        cwq=v((width, inner), BF),
        cwk=v((width, inner), BF),
        cwv=v((width, inner), BF),
        cwo=v((inner, width), BF),
        win=v((width, hidden), BF),
        wout=v((hidden, width), BF),
        q=v((rows, inner), BF),
        k=v((rows, inner), BF),
        v=v((rows, inner), BF),
        kt=v((heads, HD, rows), BF),
        vt=v((heads, HD + 16, rows), BF),
        cq=v((rows, inner), BF),
        ck=v((slots, inner), BF),
        cv=v((slots, inner), BF),
        ckt=v((heads, HD, slots), BF),
        cvt=v((heads, HD + 16, slots), BF),
        mixed=v((rows, inner), BF),
        cmixed=v((rows, inner), BF),
        lse=v((CHUNKS, heads, 1, chunk), F32),
        clse=v((CHUNKS, heads, 1, chunk), F32),
        delta=v((heads, 1, chunk), F32),
        flat=v((inner, chunk), F32),
        dout=v((chunk, inner), BF),
        dk=v((rows, inner), F32),
        dv=v((rows, inner), F32),
        hid=v((rows, hidden), BF),
        slope=v((rows, hidden), BF),
        low0=v((rows, width), BF),
        low1=v((rows, width), BF),
        low2=v((rows, width), BF),
        low3=v((rows, width), BF),
        low4=v((rows, width), BF),
        outs=v((rows, width), BF),
        res=v((CHUNKS, own, width), F32),
        xh1=v((CHUNKS, own, width), F32),
        xh2=v((CHUNKS, own, width), F32),
        rs1=v((CHUNKS, own, 1), F32),
        rs2=v((CHUNKS, own, 1), F32),
        part=v((CHUNKS, chunk, width), BF),
        rc=v((CHUNKS, half, width), BF),
        ys=v((CHUNKS, half, width), BF),
        ry=v((CHUNKS, own, width), BF),
        vacc=v((8, 8, width), F32),
        gbuf=v((2 * hidden + 2 * width, width), BF),
        vsum=v((8, width), F32),
        vrec=v((len(sizes) + 2, 8, width), F32),
        **{f"dr{j}": v((RING, n, width), BF) for j, (n, _) in enumerate(sizes)},
        ag=v((RING, [n for n, h in sizes if h][-1], width), BF),
        freed=pltpu.SemaphoreType.REGULAR((len(sizes), RING)),
        dssem=pltpu.SemaphoreType.DMA((2 * len(sizes), RING)),
        drsem=pltpu.SemaphoreType.DMA((2 * len(sizes), RING)),
        gsem=pltpu.SemaphoreType.DMA((4, pieces)),
        vssem=pltpu.SemaphoreType.DMA((len(sizes) + 2,)),
        vrsem=pltpu.SemaphoreType.DMA((len(sizes) + 2,)),
        insem=pltpu.SemaphoreType.DMA((16,)),
        cotsem=pltpu.SemaphoreType.DMA((CHUNKS,)),
        osem=pltpu.SemaphoreType.DMA((4,)),
        ssem=pltpu.SemaphoreType.DMA((8, CHUNKS)),
        rsem=pltpu.SemaphoreType.DMA((8, CHUNKS)),
    )


INPUTS = (
    "tok", "wk", "wv", "wq", "wo", "mem", "cwk", "cwv", "cwq", "cwo",
    "win", "wout",
)


def layer_kernel(names, copies, *refs):
    dec_ref, enc_ref = refs[:2]
    vec = refs[2:8]
    refs = refs[8:]
    n_in = len(INPUTS)
    srcs = dict(zip(INPUTS, refs[:n_in]))
    cot_h = refs[n_in]
    out_h, tg_h, mg_h, gf_h, gq_h, go_h, vg_h = refs[n_in + 1:n_in + 8]
    S = dict(zip(names, refs[n_in + 8:]))

    rows, width = S["tok"].shape
    slots = S["mem"].shape[0]
    inner = S["wq"].shape[1]
    hidden = S["win"].shape[1]
    heads = inner // HD
    R = rows // CHUNKS
    HF, Q = R // 2, R // 4
    scale = HD ** -0.5
    t = lax.axis_index("tensor")
    yy = t // 2
    kk = t % 2
    core = {"tensor": t + 1 - 2 * kk}
    ypar = {"tensor": t + 2 - 4 * yy}

    me = lax.axis_index("dp")
    sizes = split_sizes(copies)
    bits = len(sizes)
    pieces = (2 * hidden + 2 * width) // PIECE

    def side(weight):
        return lax.rem(lax.div(me, weight), 2)

    def dp_peer(weight):
        return {"dp": me + weight * (1 - 2 * side(weight))}

    def row(c):
        return pl.ds(pl.multiple_of(c * R, R), R)

    def own_rows(c):
        return pl.ds(pl.multiple_of(c * R + kk * HF + yy * Q, Q), Q)

    def y_rows(c):
        return pl.ds(pl.multiple_of(c * R + kk * HF + (1 - yy) * Q, Q), Q)

    loads = {n: pltpu.make_async_copy(srcs[n], S[n], S["insem"].at[j])
             for j, n in enumerate(INPUTS)}
    cots = [pltpu.make_async_copy(cot_h.at[own_rows(c)], S["cot"].at[c], S["cotsem"].at[c])
            for c in range(CHUNKS)]
    for n in INPUTS[:5]:
        loads[n].start()

    barrier = pltpu.get_barrier_semaphore()
    for peer in [core, ypar] + [dp_peer(1 << j) for j in range(bits)]:
        pl.semaphore_signal(barrier, inc=1, device_id=peer, device_id_type=MESH)

    S["vt"][:, HD:, :] = jnp.ones((heads, 16, rows), BF)
    S["cvt"][:, HD:, :] = jnp.ones((heads, 16, slots), BF)
    S["vacc"][...] = jnp.zeros(S["vacc"].shape, F32)

    def wait_for(*which):
        for n in which:
            loads[n].wait()

    def project(c, src, wk, wv, kd, vd, ktd, vtd):
        r = row(c)
        x = src[r, :]
        kf = mm(x, wk[...])
        kd[r, :] = kf.astype(BF)
        kt = kf.T.astype(BF)
        vf = mm(x, wv[...])
        vd[r, :] = vf.astype(BF)
        vtt = vf.T.astype(BF)
        for h in range(heads):
            ktd[h, :, r] = kt[h * HD:(h + 1) * HD, :]
            vtd[h, :HD, r] = vtt[h * HD:(h + 1) * HD, :]

    def lanes(h):
        return pl.ds(pl.multiple_of((h // 2) * 2 * HD, 2 * HD), 2 * HD)

    def pick(x, h):
        lane = lax.broadcasted_iota(jnp.int32, x.shape, 1) // HD
        return jnp.where(lane == h % 2, x, jnp.zeros_like(x))

    def masked(scores, c, causal, length):
        kid = lax.broadcasted_iota(jnp.int32, scores.shape, 0)
        ok = kid < length
        if causal:
            qid = c * R + lax.broadcasted_iota(jnp.int32, scores.shape, 1)
            ok = ok & (kid <= qid)
        return jnp.where(ok, scores * scale, NEGATIVE)

    def head_forward(h, c, q, k, vt, lse, causal, length, keys):
        qm = pick(q[row(c), lanes(h)], h)
        s = masked(mt(k[:keys, lanes(h)], qm), c, causal, length)
        top = jnp.max(s, axis=0, keepdims=True)
        p = jnp.exp(s - top).astype(BF)
        o = mm(vt[h, :, :keys], p)
        total = o[HD:HD + 1, :]
        S["flat"][pl.ds(pl.multiple_of(h * HD, HD), HD), :] = o[:HD, :] / total
        lse[c, h] = top + jnp.log(total)

    def head_backward(h, c, q, k, v, kt, lse, causal, length):
        qm = pick(q[row(c), lanes(h)], h)
        s = masked(mt(k[:, lanes(h)], qm), c, causal, length)
        p = jnp.exp(s - lse[c, h])
        dom = pick(S["dout"][:, lanes(h)], h)
        dp = mt(v[:, lanes(h)], dom)
        S["dv"][:, lanes(h)] += mm(p.astype(BF), dom)
        ds = (p * (dp - S["delta"][h])).astype(BF)
        S["dk"][:, lanes(h)] += mm(ds, qm)
        S["flat"][pl.ds(pl.multiple_of(h * HD, HD), HD), :] = mm(kt[h], ds) * scale

    def unflatten():
        return S["flat"][...].T

    def wide(fn, dst, c):
        block = min(256, width)

        def body(j, carry):
            cols = pl.ds(pl.multiple_of(j * block, block), block)
            dst[c, :, cols] = fn(cols).astype(BF)
            return carry
        lax.fori_loop(0, width // block, body, 0)

    def set_delta(c, mixed, low, w):
        do = mt(low[row(c), :], w[...]).astype(BF)
        S["dout"][...] = do
        prod = do.astype(F32) * mixed[row(c), :].astype(F32)
        sel = (lax.broadcasted_iota(jnp.int32, (8, inner), 1) // HD
               == lax.broadcasted_iota(jnp.int32, (8, inner), 0)).astype(F32)
        d = lax.dot_general(sel, prod, (((1,), (1,)), ((), ())),
                            precision=lax.Precision.HIGHEST, preferred_element_type=F32)
        for h in range(heads):
            S["delta"][h] = d[h:h + 1, :]

    dec = dec_ref[0]
    enc = enc_ref[0]

    def each_head(fn, middle):
        def body(h, carry):
            @pl.when(h == heads // 2)
            def _():
                middle()
            fn(h)
            return carry
        lax.fori_loop(0, heads, body, 0)

    def compute(s, c, middle):
        part = S["part"]
        if s == 0:
            project(c, S["tok"], S["wk"], S["wv"], S["k"], S["v"], S["kt"], S["vt"])
            S["q"][row(c), :] = mm(S["tok"][row(c), :], S["wq"][...]).astype(BF)
            each_head(lambda h: head_forward(h, c, S["q"], S["k"], S["vt"], S["lse"], True, dec,
                                             (c + 1) * R), middle)
            S["mixed"][row(c), :] = unflatten().astype(BF)
            wide(lambda n: mm(S["mixed"][row(c), :], S["wo"][:, n]), part, c)
        elif s == 1:
            S["cq"][row(c), :] = mm(S["low0"][row(c), :], S["cwq"][...]).astype(BF)
            each_head(lambda h: head_forward(h, c, S["cq"], S["ck"], S["cvt"], S["clse"], False, enc, slots), middle)
            S["cmixed"][row(c), :] = unflatten().astype(BF)
            wide(lambda n: mm(S["cmixed"][row(c), :], S["cwo"][:, n]), part, c)
        elif s == 2:
            block = min(256, hidden)

            def body(j, carry):
                n = pl.ds(pl.multiple_of(j * block, block), block)
                v = mm(S["low1"][row(c), :], S["win"][:, n])
                cdf = 0.5 * (1.0 + lax.erf(v * 0.7071067811865476))
                S["hid"][row(c), n] = (v * cdf).astype(BF)
                S["slope"][row(c), n] = (
                    cdf + v * jnp.exp(-0.5 * v * v) * 0.3989422804014327).astype(BF)
                return carry
            lax.fori_loop(0, hidden // block, body, 0)
            middle()
            wide(lambda n: mm(S["hid"][row(c), :], S["wout"][:, n]), part, c)
        elif s == 3:
            block = min(256, hidden)

            def body(j, carry):
                n = pl.ds(pl.multiple_of(j * block, block), block)
                g = mt(S["low2"][row(c), :], S["wout"][n, :])
                S["slope"][row(c), n] = (g * S["slope"][row(c), n].astype(F32)).astype(BF)
                return carry
            lax.fori_loop(0, hidden // block, body, 0)
            middle()
            wide(lambda n: mt(S["slope"][row(c), :], S["win"][n, :]), part, c)
        elif s == 4:
            set_delta(c, S["cmixed"], S["low3"], S["cwo"])
            each_head(lambda h: head_backward(h, c, S["cq"], S["ck"], S["cv"], S["ckt"], S["clse"], False, enc), middle)
            S["cq"][row(c), :] = unflatten().astype(BF)
            wide(lambda n: mt(S["cq"][row(c), :], S["cwq"][n, :]), part, c)
        elif s == 5:
            set_delta(c, S["mixed"], S["low4"], S["wo"])
            each_head(lambda h: head_backward(h, c, S["q"], S["k"], S["v"], S["kt"], S["lse"], True, dec), middle)
            S["q"][row(c), :] = unflatten().astype(BF)
            S["k"][row(c), :] = (S["dk"][row(c), :] * scale).astype(BF)
            S["v"][row(c), :] = S["dv"][row(c), :].astype(BF)
            wide(lambda n: mt(S["q"][row(c), :], S["wq"][n, :])
                 + mt(S["k"][row(c), :], S["wk"][n, :])
                 + mt(S["v"][row(c), :], S["wv"][n, :]), part, c)
        else:
            middle()
            wide(lambda n: mt(S["ck"][row(c), :], S["cwk"][n, :])
                 + mt(S["cv"][row(c), :], S["cwv"][n, :]), part, c)

    lows = [S["low0"], S["low1"], S["low2"], S["low3"], S["low4"], S["low2"], S["low1"]]

    def remote(src, dst, phase, c, peer):
        return pltpu.make_async_remote_copy(
            src_ref=src, dst_ref=dst, send_sem=S["ssem"].at[phase, c],
            recv_sem=S["rsem"].at[phase, c], device_id=peer, device_id_type=MESH)

    def core_part(c):
        theirs = pl.ds(pl.multiple_of((1 - kk) * HF, HF), HF)
        return remote(S["part"].at[c, theirs], S["rc"].at[c], 0, c, core)

    def y_part(c):
        theirs = pl.ds(pl.multiple_of((1 - yy) * Q, Q), Q)
        return remote(S["ys"].at[c, theirs], S["ry"].at[c], 1, c, ypar)

    def gather(buf, c, which, base):
        r = y_rows(c) if which == 2 else own_rows(c)
        return remote(buf.at[r], buf.at[r], base + which, c, ypar if which == 0 else core)

    def p0(c):
        core_part(c).start()

    def p1(c):
        core_part(c).wait()
        step = min(32, HF)

        def body(j, carry):
            r = pl.ds(pl.multiple_of(j * step, step), step)
            m = pl.ds(pl.multiple_of(kk * HF + j * step, step), step)
            S["ys"][c, r, :] = (S["part"][c, m, :].astype(F32)
                                + S["rc"][c, r, :].astype(F32)).astype(BF)
            return carry
        lax.fori_loop(0, HF // step, body, 0)
        y_part(c).start()

    def mean(x):
        return jnp.sum(x, axis=-1, keepdims=True) * (1.0 / width)

    def norm(x, j):
        center = x - mean(x)
        inv = lax.rsqrt(mean(center * center) + EPSILON)
        xhat = center * inv
        return xhat, inv, xhat * vec[2 * j][...] + vec[2 * j + 1][...]

    def fold(x):
        return jnp.sum(x.reshape(x.shape[0] // 8, 8, width), axis=0)

    def norm_back(e, xhat, inv, j):
        S["vacc"][2 * j] += fold(e * xhat)
        S["vacc"][2 * j + 1] += fold(e)
        eg = e * vec[2 * j][...]
        return (eg - mean(eg) - xhat * mean(eg * xhat)) * inv

    def p2(s, c):
        y_part(c).wait()
        if s == 2:
            @pl.when(c == 0)
            def _():
                for x in cots:
                    x.wait()
        step = min(16, Q)
        buf = lows[s]

        def body(j, carry):
            r = pl.ds(pl.multiple_of(j * step, step), step)
            m = pl.ds(pl.multiple_of(yy * Q + j * step, step), step)
            o = pl.ds(pl.multiple_of(c * R + kk * HF + yy * Q + j * step, step), step)
            x = S["ys"][c, m, :].astype(F32) + S["ry"][c, r, :].astype(F32)
            if s == 0:
                xhat, inv, y = norm(S["tok"][o, :].astype(F32) + x, 0)
                S["xh1"][c, r, :] = xhat
                S["rs1"][c, r, :] = inv
                S["res"][c, r, :] = y
            elif s == 1:
                xhat, inv, y = norm(S["res"][c, r, :] + x, 1)
                S["xh2"][c, r, :] = xhat
                S["rs2"][c, r, :] = inv
                S["res"][c, r, :] = y
            elif s == 2:
                xhat, inv, y = norm(S["res"][c, r, :] + x, 2)
                S["outs"][o, :] = y.astype(BF)
                rid = (c * R + kk * HF + yy * Q + j * step
                       + lax.broadcasted_iota(jnp.int32, (step, width), 0))
                seed = jnp.where(rid < dec, S["cot"][c, r, :].astype(F32), 0.0)
                y = norm_back(seed, xhat, inv, 2)
                S["res"][c, r, :] = y
            elif s == 3:
                y = norm_back(S["res"][c, r, :] + x, S["xh2"][c, r, :], S["rs2"][c, r, :], 1)
                S["res"][c, r, :] = y
            elif s == 4:
                y = norm_back(S["res"][c, r, :] + x, S["xh1"][c, r, :], S["rs1"][c, r, :], 0)
                S["res"][c, r, :] = y
            elif s == 5:
                y = S["res"][c, r, :] + x
            else:
                y = x
            buf[o, :] = y.astype(BF)
            return carry
        lax.fori_loop(0, Q // step, body, 0)
        gather(buf, c, 0, 2).start()
        gather(buf, c, 1, 2).start()

    def p3(s, c):
        gather(lows[s], c, 0, 2).wait()
        gather(lows[s], c, 2, 2).start()

    def p4(s, c):
        gather(lows[s], c, 1, 2).wait()
        gather(lows[s], c, 2, 2).wait()

    def grad_piece(g, i):
        n = pl.ds(pl.multiple_of(i * PIECE, PIECE), PIECE)
        r = pl.ds(pl.multiple_of((g * CHUNKS + i) * PIECE, PIECE), PIECE)
        if g == 0:
            S["gbuf"][r, :] = tm(S["hid"][:, n], S["low2"][...]).astype(BF)
        elif g == 1:
            S["gbuf"][r, :] = tm(S["low1"][:, n], S["slope"][...]).astype(BF)
        else:
            if g == 2:
                a, b, d = S["low0"], S["mem"], S["low3"]
                x, y, z, w = S["cq"], S["ck"], S["cv"], S["cmixed"]
            else:
                a, b, d = S["tok"], S["tok"], S["low4"]
                x, y, z, w = S["q"], S["k"], S["v"], S["mixed"]
            S["gbuf"][r, 0 * inner:1 * inner] = tm(a[:, n], x[...]).astype(BF)
            S["gbuf"][r, 1 * inner:2 * inner] = tm(b[:, n], y[...]).astype(BF)
            S["gbuf"][r, 2 * inner:3 * inner] = tm(b[:, n], z[...]).astype(BF)
            S["gbuf"][r, 3 * inner:4 * inner] = tm(w[...], d[:, n]).astype(BF)

    def weight(step, p):
        if bits < 2 or step > 1:
            return 1 << step
        swap = lax.rem(lax.shift_right_logical(SWAPPED, p), 2)
        return 1 + swap if step == 0 else 2 - swap

    def start_of(step, p):
        at = p * PIECE
        for j in range(step):
            if sizes[j][1]:
                at = at + side(weight(j, p)) * sizes[j][0]
        return at

    def piece_rows(at, n):
        return pl.ds(pl.multiple_of(at, n), n)

    def reduce_copy(step, p):
        n, halve = sizes[step]
        w = weight(step, p)
        at = start_of(step, p)
        if halve:
            at = at + (1 - side(w)) * n
        slot = lax.rem(p, RING)
        return pltpu.make_async_remote_copy(
            src_ref=S["gbuf"].at[piece_rows(at, n)], dst_ref=S[f"dr{step}"].at[slot],
            send_sem=S["dssem"].at[step, slot], recv_sem=S["drsem"].at[step, slot],
            device_id=dp_peer(w), device_id_type=MESH)

    def reduce_add(step, p):
        n, halve = sizes[step]
        at = start_of(step + 1, p)
        slot = lax.rem(p, RING)
        block = min(32, n)

        def body(j, carry):
            r = pl.ds(pl.multiple_of(at + j * block, block), block)
            m = pl.ds(pl.multiple_of(j * block, block), block)
            S["gbuf"][r, :] = (S["gbuf"][r, :].astype(F32)
                               + S[f"dr{step}"][slot, m, :].astype(F32)).astype(BF)
            return carry
        lax.fori_loop(0, n // block, body, 0)

    halved = sum(1 for _, h in sizes if h)
    steps = bits + halved

    def gather_copy(step, p):
        n, _ = sizes[step]
        r = S["gbuf"].at[piece_rows(start_of(step + 1, p), n)]
        slot = lax.rem(p, RING)
        return pltpu.make_async_remote_copy(
            src_ref=r, dst_ref=S["ag"].at[slot] if step == halved - 1 else r,
            send_sem=S["dssem"].at[bits + step, slot], recv_sem=S["drsem"].at[bits + step, slot],
            device_id=dp_peer(weight(step, p)), device_id_type=MESH)

    def gather_end(step, p):
        gather_copy(step, p).wait()
        if step == halved - 1:
            n, _ = sizes[step]
            at = start_of(step, p) + (1 - side(weight(step, p))) * n
            S["gbuf"][piece_rows(at, n), :] = S["ag"][lax.rem(p, RING)]

    def gather_begin(step, p):
        if step < halved - 1:
            pl.semaphore_wait(S["freed"].at[step, lax.rem(p, RING)], 1)
        gather_copy(step, p).start()

    def result_copies(p, ff):
        r = pl.ds(pl.multiple_of(p * PIECE, PIECE), PIECE)
        if ff:
            return [pltpu.make_async_copy(S["gbuf"].at[r], gf_h.at[r], S["gsem"].at[0, p])]
        g = lax.div(p - 2 * CHUNKS, CHUNKS)
        n = pl.ds(pl.multiple_of(lax.rem(p, CHUNKS) * PIECE, PIECE), PIECE)
        block = [S["gbuf"].at[r, pl.ds(j * inner, inner)] for j in range(4)]
        return [pltpu.make_async_copy(block[j], gq_h.at[g, j, n], S["gsem"].at[j, p])
                for j in range(3)] + [
            pltpu.make_async_copy(block[3], go_h.at[g, :, n], S["gsem"].at[3, p])]

    def dp_step(k, p):
        if 1 <= k <= bits:
            reduce_copy(k - 1, p).wait()
            if k < halved:
                pl.semaphore_signal(S["freed"].at[k - 1, lax.rem(p, RING)], inc=1,
                                    device_id=dp_peer(weight(k - 1, p)), device_id_type=MESH)
            reduce_add(k - 1, p)
        elif k > bits:
            gather_end(halved - (k - bits), p)
        if k < bits:
            reduce_copy(k, p).start()
        elif k < steps:
            gather_begin(halved - 1 - (k - bits), p)
        else:
            @pl.when(p < 2 * CHUNKS)
            def _():
                for x in result_copies(p, True):
                    x.start()

            @pl.when(p >= 2 * CHUNKS)
            def _():
                for x in result_copies(p, False):
                    x.start()

    waits = WAITS if steps == len(WAITS) else (2,) * steps
    lag = [sum(waits[:k]) for k in range(steps + 1)]
    FIRST = 2 * CHUNKS
    GAP = FIRST + 2
    LAST = GAP + 4 * CHUNKS - 2

    def dp_slot(m):
        for k in range(steps + 1):
            e = m - lag[k]
            early = e < FIRST
            p = jnp.where(early, e, FIRST + lax.div(e - GAP, 2))

            @pl.when((e >= 0) & (e <= LAST)
                     & (early | ((e >= GAP) & (lax.rem(e, 2) == 0))))
            def _(k=k, p=p):
                dp_step(k, p)

    peers = [core, ypar] + [dp_peer(1 << j) for j in range(bits)]

    def vec_copy(k):
        return pltpu.make_async_remote_copy(
            src_ref=S["vsum"], dst_ref=S["vrec"].at[k], send_sem=S["vssem"].at[k],
            recv_sem=S["vrsem"].at[k], device_id=peers[k], device_id_type=MESH)

    def vec_step(k):
        if k == 0:
            S["vsum"][...] = jnp.sum(S["vacc"][...], axis=1)
        else:
            vec_copy(k - 1).wait()
            S["vsum"][...] += S["vrec"][k - 1]
        if k < len(peers):
            vec_copy(k).start()

    def chunk_of(s, i):
        return i if s <= 4 else CHUNKS - 1 - i

    def lagged(i, n, fn, s):
        def now():
            fn(s, chunk_of(s, i - n))

        def before():
            fn(s - 1, chunk_of(s - 1, i - n + CHUNKS))
        fresh = s in (0, 5)
        if isinstance(i, int):
            if i >= n:
                now()
            elif not fresh:
                before()
            return
        pl.when(i >= n)(now)
        if not fresh:
            pl.when(i < n)(before)

    def phases(i, s):
        lagged(i, 1, lambda _, c: p1(c), s)
        lagged(i, 2, p2, s)
        lagged(i, 3, p3, s)

    def ff_piece(m):
        @pl.when(m < CHUNKS)
        def _():
            grad_piece(0, m)

        @pl.when(m >= CHUNKS)
        def _():
            grad_piece(1, m - CHUNKS)

    def slot(i, s):
        c = chunk_of(s, i)
        if s > 0:
            p4(s - 1, c)
        if s == 5:
            gather(S["outs"], c, 0, 5).start()
            gather(S["outs"], c, 1, 5).start()

        def middle():
            phases(i, s)
            if s == 4:
                ff_piece(2 * i)
                dp_slot(2 * i)
            elif s > 4:
                grad_piece(s - 3, i)
                dp_slot(GAP + 2 * CHUNKS * (s - 5) + 2 * i)
            if s == 6:
                gather(S["outs"], c, 0, 5).wait()
                gather(S["outs"], c, 2, 5).start()
                for k in range(CHUNKS):
                    @pl.when(i == k)
                    def _(k=k):
                        vec_step(k)
        compute(s, c, middle)
        if s == 0 and i == 0:
            pl.semaphore_wait(barrier, 2 + bits)
        p0(c)
        if s == 4:
            ff_piece(2 * i + 1)
            dp_slot(2 * i + 1)
        elif s > 4:
            dp_slot(GAP + 2 * CHUNKS * (s - 5) + 2 * i + 1)

    def drain(s, t):
        a, b, d = (chunk_of(s, i) for i in (1, 2, 3))

        @pl.when(t == 0)
        def _():
            p3(s, a)
            p2(s, b)
            p1(d)

        @pl.when(t == 1)
        def _():
            p3(s, b)
            p2(s, d)

        @pl.when(t == 2)
        def _():
            p3(s, d)

    wait_for("tok", "wk", "wv", "wq", "wo")
    for n in INPUTS[5:]:
        loads[n].start()
    for x in cots:
        x.start()
    for i in range(CHUNKS):
        slot(i, 0)
        if i == 0:
            wait_for("mem", "cwk", "cwv")
        project(i, S["mem"], S["cwk"], S["cwv"], S["ck"], S["cv"], S["ckt"], S["cvt"])

    for s in range(1, STAGES):
        if s == 1:
            wait_for("cwq", "cwo")
        if s == 2:
            wait_for("win", "wout")
        if s in (4, 5):
            S["dk"][...] = jnp.zeros(S["dk"].shape, F32)
            S["dv"][...] = jnp.zeros(S["dv"].shape, F32)

        def body(i, carry, s=s):
            slot(i, s)
            return carry
        lax.fori_loop(0, CHUNKS, body, 0)
        if s == 4:
            S["ck"][...] = (S["dk"][...] * scale).astype(BF)
            S["cv"][...] = S["dv"][...].astype(BF)

            def between(t, carry):
                drain(4, t)

                @pl.when(t < 2)
                def _():
                    dp_slot(FIRST + t)
                return carry
            lax.fori_loop(0, 3, between, 0)

    last = STAGES - 1
    tail = LAST + 2
    outputs = [pltpu.make_async_copy(a, b, S["osem"].at[j])
               for j, (a, b) in enumerate(((S["outs"], out_h), (lows[5], tg_h), (lows[6], mg_h)))]

    def ending(m, carry):
        t = m - tail
        dp_slot(m)
        drain(last, t)

        @pl.when(t == 0)
        def _():
            for c in range(CHUNKS):
                gather(S["outs"], c, 1, 5).wait()
                gather(S["outs"], c, 2, 5).wait()
            outputs[0].start()
            outputs[1].start()

        @pl.when(t == 3)
        def _():
            for c in range(CHUNKS):
                p4(last, c)
            outputs[2].start()
        for k in range(CHUNKS, len(peers) + 1):
            @pl.when(t == k - CHUNKS)
            def _(k=k):
                vec_step(k)
        return carry
    lax.fori_loop(tail, LAST + lag[-1] + 1, ending, 0)
    vg_h[...] = S["vsum"][...]

    def finish(p, carry, ff):
        for x in result_copies(p, ff):
            x.wait()
        return carry
    lax.fori_loop(0, 2 * CHUNKS, lambda p, x: finish(p, x, True), 0)
    lax.fori_loop(2 * CHUNKS, pieces, lambda p, x: finish(p, x, False), 0)
    for x in outputs:
        x.wait()


def widen(out, tg, mg, gf, gq, go):
    parts = 16
    width = out.shape[1]
    hidden = gf.shape[0] // 2
    inner = gq.shape[-1]
    row_specs, shapes, ins, in_specs = [], [], [], []

    def add(x, rows, columns, spec, dtype=F32):
        ins.append(x)
        in_specs.append(spec)
        row_specs.append(pl.BlockSpec((rows // parts, columns), lambda i: (i, 0)))
        shapes.append(jax.ShapeDtypeStruct((rows, columns), dtype))

    for x, dtype in ((out, BF), (tg, F32), (mg, F32)):
        n = x.shape[0]
        add(x, n, width, pl.BlockSpec((n // parts, width), lambda i: (i, 0)), dtype)
    for g in (1, 0):
        for j in range(3):
            add(gq, width, inner, pl.BlockSpec(
                (None, None, width // parts, inner), lambda i, g=g, j=j: (g, j, i, 0)))
        add(go, inner, width, pl.BlockSpec(
            (None, inner // parts, width), lambda i, g=g: (g, i, 0)))
    for g in range(2):
        add(gf, hidden, width, pl.BlockSpec(
            (hidden // parts, width), lambda i, g=g: (g * parts + i, 0)))

    def body(*refs):
        n = len(ins)
        for a, b in zip(refs[:n], refs[n:]):
            b[...] = a[...].astype(b.dtype)

    return pl.pallas_call(
        body, out_shape=tuple(shapes), grid=(parts,), in_specs=in_specs,
        out_specs=tuple(row_specs), name="widen",
        compiler_params=pltpu.CompilerParams(dimension_semantics=("arbitrary",)),
    )(*ins)


def shards(
    tokens, memory, decoder_length, memory_length,
    self_query, self_key, self_value, self_output, self_gain, self_bias,
    cross_query, cross_key, cross_value, cross_output, cross_gain, cross_bias,
    feed_in, feed_out, feed_gain, feed_bias, cotangent,
):
    rows, width = tokens.shape
    slots = memory.shape[0]
    inner = self_query.shape[1]
    hidden = feed_in.shape[1]
    vecs = [x.reshape(1, width) for x in (
        self_gain, self_bias, cross_gain, cross_bias, feed_gain, feed_bias)]
    copies = lax.axis_size("dp")
    scratch = layout(rows, slots, width, inner, hidden, copies)
    names = tuple(scratch)
    given = dict(tok=tokens, mem=memory, wq=self_query, wk=self_key, wv=self_value,
                 wo=self_output, cwq=cross_query, cwk=cross_key, cwv=cross_value,
                 cwo=cross_output, win=feed_in, wout=feed_out)
    any_spec = pl.BlockSpec(memory_space=pl.ANY)

    def kernel(*refs):
        layer_kernel(names, copies, *refs)

    out, tg, mg, gf, gq, go, vg = pl.pallas_call(
        kernel,
        out_shape=(
            jax.ShapeDtypeStruct((rows, width), BF),
            jax.ShapeDtypeStruct((rows, width), BF),
            jax.ShapeDtypeStruct((slots, width), BF),
            jax.ShapeDtypeStruct((2 * hidden, width), BF),
            jax.ShapeDtypeStruct((2, 3, width, inner), BF),
            jax.ShapeDtypeStruct((2, inner, width), BF),
            jax.ShapeDtypeStruct((8, width), F32),
        ),
        in_specs=[pl.BlockSpec(memory_space=pltpu.SMEM)] * 2
        + [pl.BlockSpec(memory_space=pltpu.VMEM)] * 6 + [any_spec] * (len(INPUTS) + 1),
        out_specs=(any_spec,) * 6 + (pl.BlockSpec(memory_space=pltpu.VMEM),),
        scratch_shapes=list(scratch.values()),
        compiler_params=pltpu.CompilerParams(
            collective_id=0, has_side_effects=True, vmem_limit_bytes=67043328),
        name="layer",
    )(decoder_length, memory_length, *vecs, *[given[n] for n in INPUTS], cotangent)

    wide = widen(out, tg, mg, gf, gq, go)
    return (
        *wide[:3],
        *wide[3:7], vg[0], vg[1],
        *wide[7:11], vg[2], vg[3],
        wide[12], wide[11], vg[4], vg[5],
    )


def solution(mesh):
    rows = P("dp", None)
    tail = P(None, "tensor")
    head = P("tensor", None)
    whole = P()
    return jax.shard_map(
        shards,
        mesh=mesh,
        in_specs=(
            rows, rows, P("dp"), P("dp"),
            tail, tail, tail, head, whole, whole,
            tail, tail, tail, head, whole, whole,
            tail, head, whole, whole, rows,
        ),
        out_specs=(
            rows, rows, rows,
            tail, tail, tail, head, whole, whole,
            tail, tail, tail, head, whole, whole,
            tail, head, whole, whole,
        ),
        check_vma=False,
    )
```

```python
import jax
import jax.numpy as jnp
from jax import lax
from jax.experimental import pallas as pl
from jax.experimental.pallas import tpu as pltpu
from jax.sharding import PartitionSpec as P

BF = jnp.bfloat16
F32 = jnp.float32
HD = 64
CHUNKS = 4
EPSILON = 1e-05
NEGATIVE = -1e30
MESH = pl.DeviceIdType.MESH
STAGES = 7


def mm(a, b):
    return lax.dot_general(a, b, (((1,), (0,)), ((), ())), preferred_element_type=F32)


def mt(a, b):
    return lax.dot_general(a, b, (((1,), (1,)), ((), ())), preferred_element_type=F32)


def tm(a, b):
    return lax.dot_general(a, b, (((0,), (0,)), ((), ())), preferred_element_type=F32)


PIECE = 256
RING = 12
SWAPPED = 0b1010000000010010
WAITS = (3, 3, 2, 2, 3, 5)
ORDER = (0, 1, 2, 3, 4, 5, 6)


def split_sizes(copies):
    sizes, rows = [], PIECE
    for _ in range(copies.bit_length() - 1):
        halve = rows // 2 >= 16
        rows = rows // 2 if halve else rows
        sizes.append((rows, halve))
    return sizes


def layout(rows, slots, width, inner, hidden, copies):
    sizes = split_sizes(copies)
    pieces = (2 * hidden + 2 * width) // PIECE
    heads = inner // HD
    chunk = rows // CHUNKS
    half, own = chunk // 2, chunk // 4
    v = pltpu.VMEM
    return dict(
        tok=v((rows, width), BF),
        mem=v((slots, width), BF),
        cot=v((CHUNKS, own, width), BF),
        wq=v((width, inner), BF),
        wk=v((width, inner), BF),
        wv=v((width, inner), BF),
        wo=v((inner, width), BF),
        cwq=v((width, inner), BF),
        cwk=v((width, inner), BF),
        cwv=v((width, inner), BF),
        cwo=v((inner, width), BF),
        win=v((width, hidden), BF),
        wout=v((hidden, width), BF),
        q=v((rows, inner), BF),
        k=v((rows, inner), BF),
        v=v((rows, inner), BF),
        kt=v((heads, HD, rows), BF),
        vt=v((heads, HD + 16, rows), BF),
        cq=v((rows, inner), BF),
        ck=v((slots, inner), BF),
        cv=v((slots, inner), BF),
        ckt=v((heads, HD, slots), BF),
        cvt=v((heads, HD + 16, slots), BF),
        mixed=v((rows, inner), BF),
        cmixed=v((rows, inner), BF),
        lse=v((CHUNKS, heads, 1, chunk), F32),
        clse=v((CHUNKS, heads, 1, chunk), F32),
        delta=v((heads, 1, chunk), F32),
        flat=v((inner, chunk), F32),
        dout=v((chunk, inner), BF),
        dk=v((rows, inner), F32),
        dv=v((rows, inner), F32),
        hid=v((rows, hidden), BF),
        slope=v((rows, hidden), BF),
        low0=v((rows, width), BF),
        low1=v((rows, width), BF),
        low2=v((rows, width), BF),
        low3=v((rows, width), BF),
        low4=v((rows, width), BF),
        outs=v((rows, width), BF),
        res=v((CHUNKS, own, width), F32),
        xh1=v((CHUNKS, own, width), F32),
        xh2=v((CHUNKS, own, width), F32),
        rs1=v((CHUNKS, own, 1), F32),
        rs2=v((CHUNKS, own, 1), F32),
        part=v((CHUNKS, chunk, width), BF),
        rc=v((CHUNKS, half, width), BF),
        ys=v((CHUNKS, half, width), BF),
        ry=v((CHUNKS, own, width), BF),
        vacc=v((8, 8, width), F32),
        gbuf=v((2 * hidden + 2 * width, width), BF),
        vsum=v((8, width), F32),
        vrec=v((len(sizes) + 2, 8, width), F32),
        **{f"dr{j}": v((RING, n, width), BF) for j, (n, _) in enumerate(sizes)},
        ag=v((RING, [n for n, h in sizes if h][-1], width), BF),
        freed=pltpu.SemaphoreType.REGULAR((len(sizes), RING)),
        dssem=pltpu.SemaphoreType.DMA((2 * len(sizes), RING)),
        drsem=pltpu.SemaphoreType.DMA((2 * len(sizes), RING)),
        gsem=pltpu.SemaphoreType.DMA((4, pieces)),
        vssem=pltpu.SemaphoreType.DMA((len(sizes) + 2,)),
        vrsem=pltpu.SemaphoreType.DMA((len(sizes) + 2,)),
        insem=pltpu.SemaphoreType.DMA((16,)),
        cotsem=pltpu.SemaphoreType.DMA((CHUNKS,)),
        osem=pltpu.SemaphoreType.DMA((4,)),
        ssem=pltpu.SemaphoreType.DMA((8, CHUNKS)),
        rsem=pltpu.SemaphoreType.DMA((8, CHUNKS)),
    )


INPUTS = (
    "tok", "wk", "wv", "wq", "wo", "mem", "cwk", "cwv", "cwq", "cwo",
    "win", "wout",
)


def layer_kernel(names, copies, *refs):
    dec_ref, enc_ref = refs[:2]
    vec = refs[2:8]
    refs = refs[8:]
    n_in = len(INPUTS)
    srcs = dict(zip(INPUTS, refs[:n_in]))
    cot_h = refs[n_in]
    out_h, tg_h, mg_h, gf_h, gq_h, go_h, vg_h = refs[n_in + 1:n_in + 8]
    S = dict(zip(names, refs[n_in + 8:]))

    rows, width = S["tok"].shape
    slots = S["mem"].shape[0]
    inner = S["wq"].shape[1]
    hidden = S["win"].shape[1]
    heads = inner // HD
    R = rows // CHUNKS
    HF, Q = R // 2, R // 4
    scale = HD ** -0.5
    t = lax.axis_index("tensor")
    yy = t // 2
    kk = t % 2
    core = {"tensor": t + 1 - 2 * kk}
    ypar = {"tensor": t + 2 - 4 * yy}

    me = lax.axis_index("dp")
    sizes = split_sizes(copies)
    bits = len(sizes)
    pieces = (2 * hidden + 2 * width) // PIECE

    def side(weight):
        return lax.rem(lax.div(me, weight), 2)

    def dp_peer(weight):
        return {"dp": me + weight * (1 - 2 * side(weight))}

    def row(c):
        return pl.ds(pl.multiple_of(c * R, R), R)

    def own_rows(c):
        return pl.ds(pl.multiple_of(c * R + kk * HF + yy * Q, Q), Q)

    def y_rows(c):
        return pl.ds(pl.multiple_of(c * R + kk * HF + (1 - yy) * Q, Q), Q)

    loads = {n: pltpu.make_async_copy(srcs[n], S[n], S["insem"].at[j])
             for j, n in enumerate(INPUTS)}
    cots = [pltpu.make_async_copy(cot_h.at[own_rows(c)], S["cot"].at[c], S["cotsem"].at[c])
            for c in range(CHUNKS)]
    for n in INPUTS[:5]:
        loads[n].start()

    barrier = pltpu.get_barrier_semaphore()
    for peer in [core, ypar] + [dp_peer(1 << j) for j in range(bits)]:
        pl.semaphore_signal(barrier, inc=1, device_id=peer, device_id_type=MESH)

    S["vt"][:, HD:, :] = jnp.ones((heads, 16, rows), BF)
    S["cvt"][:, HD:, :] = jnp.ones((heads, 16, slots), BF)
    S["vacc"][...] = jnp.zeros(S["vacc"].shape, F32)

    def wait_for(*which):
        for n in which:
            loads[n].wait()

    def project(c, src, wk, wv, kd, vd, ktd, vtd):
        r = row(c)
        x = src[r, :]
        kf = mm(x, wk[...])
        kd[r, :] = kf.astype(BF)
        kt = kf.T.astype(BF)
        vf = mm(x, wv[...])
        vd[r, :] = vf.astype(BF)
        vtt = vf.T.astype(BF)
        for h in range(heads):
            ktd[h, :, r] = kt[h * HD:(h + 1) * HD, :]
            vtd[h, :HD, r] = vtt[h * HD:(h + 1) * HD, :]

    def lanes(h):
        return pl.ds(pl.multiple_of((h // 2) * 2 * HD, 2 * HD), 2 * HD)

    def pick(x, h):
        lane = lax.broadcasted_iota(jnp.int32, x.shape, 1) // HD
        return jnp.where(lane == h % 2, x, jnp.zeros_like(x))

    def masked(scores, c, causal, length):
        kid = lax.broadcasted_iota(jnp.int32, scores.shape, 0)
        ok = kid < length
        if causal:
            qid = c * R + lax.broadcasted_iota(jnp.int32, scores.shape, 1)
            ok = ok & (kid <= qid)
        return jnp.where(ok, scores * scale, NEGATIVE)

    def head_forward(h, c, q, k, vt, lse, causal, length, keys):
        qm = pick(q[row(c), lanes(h)], h)
        s = masked(mt(k[:keys, lanes(h)], qm), c, causal, length)
        top = jnp.max(s, axis=0, keepdims=True)
        p = jnp.exp(s - top).astype(BF)
        o = mm(vt[h, :, :keys], p)
        total = o[HD:HD + 1, :]
        S["flat"][pl.ds(pl.multiple_of(h * HD, HD), HD), :] = o[:HD, :] / total
        lse[c, h] = top + jnp.log(total)

    def head_backward(h, c, q, k, v, kt, lse, causal, length):
        qm = pick(q[row(c), lanes(h)], h)
        s = masked(mt(k[:, lanes(h)], qm), c, causal, length)
        p = jnp.exp(s - lse[c, h])
        dom = pick(S["dout"][:, lanes(h)], h)
        dp = mt(v[:, lanes(h)], dom)
        S["dv"][:, lanes(h)] += mm(p.astype(BF), dom)
        ds = (p * (dp - S["delta"][h])).astype(BF)
        S["dk"][:, lanes(h)] += mm(ds, qm)
        S["flat"][pl.ds(pl.multiple_of(h * HD, HD), HD), :] = mm(kt[h], ds) * scale

    def unflatten():
        return S["flat"][...].T

    def wide(fn, dst, c):
        block = min(256, width)

        def body(j, carry):
            cols = pl.ds(pl.multiple_of(j * block, block), block)
            dst[c, :, cols] = fn(cols).astype(BF)
            return carry
        lax.fori_loop(0, width // block, body, 0)

    def set_delta(c, mixed, low, w):
        do = mt(low[row(c), :], w[...]).astype(BF)
        S["dout"][...] = do
        prod = do.astype(F32) * mixed[row(c), :].astype(F32)
        sel = (lax.broadcasted_iota(jnp.int32, (8, inner), 1) // HD
               == lax.broadcasted_iota(jnp.int32, (8, inner), 0)).astype(F32)
        d = lax.dot_general(sel, prod, (((1,), (1,)), ((), ())),
                            precision=lax.Precision.HIGHEST, preferred_element_type=F32)
        for h in range(heads):
            S["delta"][h] = d[h:h + 1, :]

    dec = dec_ref[0]
    enc = enc_ref[0]

    def each_head(fn, middle):
        def body(h, carry):
            @pl.when(h == heads // 2)
            def _():
                middle()
            fn(h)
            return carry
        lax.fori_loop(0, heads, body, 0)

    def compute(s, c, middle):
        part = S["part"]
        if s == 0:
            project(c, S["tok"], S["wk"], S["wv"], S["k"], S["v"], S["kt"], S["vt"])
            S["q"][row(c), :] = mm(S["tok"][row(c), :], S["wq"][...]).astype(BF)
            each_head(lambda h: head_forward(h, c, S["q"], S["k"], S["vt"], S["lse"], True, dec,
                                             (c + 1) * R), middle)
            S["mixed"][row(c), :] = unflatten().astype(BF)
            wide(lambda n: mm(S["mixed"][row(c), :], S["wo"][:, n]), part, c)
        elif s == 1:
            S["cq"][row(c), :] = mm(S["low0"][row(c), :], S["cwq"][...]).astype(BF)
            each_head(lambda h: head_forward(h, c, S["cq"], S["ck"], S["cvt"], S["clse"], False, enc, slots), middle)
            S["cmixed"][row(c), :] = unflatten().astype(BF)
            wide(lambda n: mm(S["cmixed"][row(c), :], S["cwo"][:, n]), part, c)
        elif s == 2:
            block = min(256, hidden)

            def body(j, carry):
                n = pl.ds(pl.multiple_of(j * block, block), block)
                v = mm(S["low1"][row(c), :], S["win"][:, n])
                cdf = 0.5 * (1.0 + lax.erf(v * 0.7071067811865476))
                S["hid"][row(c), n] = (v * cdf).astype(BF)
                S["slope"][row(c), n] = (
                    cdf + v * jnp.exp(-0.5 * v * v) * 0.3989422804014327).astype(BF)
                return carry
            lax.fori_loop(0, hidden // block, body, 0)
            middle()
            wide(lambda n: mm(S["hid"][row(c), :], S["wout"][:, n]), part, c)
        elif s == 3:
            block = min(256, hidden)

            def body(j, carry):
                n = pl.ds(pl.multiple_of(j * block, block), block)
                g = mt(S["low2"][row(c), :], S["wout"][n, :])
                S["slope"][row(c), n] = (g * S["slope"][row(c), n].astype(F32)).astype(BF)
                return carry
            lax.fori_loop(0, hidden // block, body, 0)
            middle()
            wide(lambda n: mt(S["slope"][row(c), :], S["win"][n, :]), part, c)
        elif s == 4:
            set_delta(c, S["cmixed"], S["low3"], S["cwo"])
            each_head(lambda h: head_backward(h, c, S["cq"], S["ck"], S["cv"], S["ckt"], S["clse"], False, enc), middle)
            S["cq"][row(c), :] = unflatten().astype(BF)
            wide(lambda n: mt(S["cq"][row(c), :], S["cwq"][n, :]), part, c)
        elif s == 5:
            set_delta(c, S["mixed"], S["low4"], S["wo"])
            each_head(lambda h: head_backward(h, c, S["q"], S["k"], S["v"], S["kt"], S["lse"], True, dec), middle)
            S["q"][row(c), :] = unflatten().astype(BF)
            S["k"][row(c), :] = (S["dk"][row(c), :] * scale).astype(BF)
            S["v"][row(c), :] = S["dv"][row(c), :].astype(BF)
            wide(lambda n: mt(S["q"][row(c), :], S["wq"][n, :])
                 + mt(S["k"][row(c), :], S["wk"][n, :])
                 + mt(S["v"][row(c), :], S["wv"][n, :]), part, c)
        else:
            middle()
            wide(lambda n: mt(S["ck"][row(c), :], S["cwk"][n, :])
                 + mt(S["cv"][row(c), :], S["cwv"][n, :]), part, c)

    lows = [S["low0"], S["low1"], S["low2"], S["low3"], S["low4"], S["low2"], S["low1"]]

    def remote(src, dst, phase, c, peer):
        return pltpu.make_async_remote_copy(
            src_ref=src, dst_ref=dst, send_sem=S["ssem"].at[phase, c],
            recv_sem=S["rsem"].at[phase, c], device_id=peer, device_id_type=MESH)

    def core_part(c):
        theirs = pl.ds(pl.multiple_of((1 - kk) * HF, HF), HF)
        return remote(S["part"].at[c, theirs], S["rc"].at[c], 0, c, core)

    def y_part(c):
        theirs = pl.ds(pl.multiple_of((1 - yy) * Q, Q), Q)
        return remote(S["ys"].at[c, theirs], S["ry"].at[c], 1, c, ypar)

    def gather(buf, c, which, base):
        r = y_rows(c) if which == 2 else own_rows(c)
        return remote(buf.at[r], buf.at[r], base + which, c, ypar if which == 0 else core)

    def p0(c):
        core_part(c).start()

    def p1(c):
        core_part(c).wait()
        step = min(32, HF)

        def body(j, carry):
            r = pl.ds(pl.multiple_of(j * step, step), step)
            m = pl.ds(pl.multiple_of(kk * HF + j * step, step), step)
            S["ys"][c, r, :] = (S["part"][c, m, :].astype(F32)
                                + S["rc"][c, r, :].astype(F32)).astype(BF)
            return carry
        lax.fori_loop(0, HF // step, body, 0)
        y_part(c).start()

    def mean(x):
        return jnp.sum(x, axis=-1, keepdims=True) * (1.0 / width)

    def norm(x, j):
        center = x - mean(x)
        inv = lax.rsqrt(mean(center * center) + EPSILON)
        xhat = center * inv
        return xhat, inv, xhat * vec[2 * j][...] + vec[2 * j + 1][...]

    def fold(x):
        return jnp.sum(x.reshape(x.shape[0] // 8, 8, width), axis=0)

    def norm_back(e, xhat, inv, j):
        S["vacc"][2 * j] += fold(e * xhat)
        S["vacc"][2 * j + 1] += fold(e)
        eg = e * vec[2 * j][...]
        return (eg - mean(eg) - xhat * mean(eg * xhat)) * inv

    def p2(s, c):
        y_part(c).wait()
        if s == 2:
            @pl.when(c == 0)
            def _():
                for x in cots:
                    x.wait()
        step = min(16, Q)
        buf = lows[s]

        def body(j, carry):
            r = pl.ds(pl.multiple_of(j * step, step), step)
            m = pl.ds(pl.multiple_of(yy * Q + j * step, step), step)
            o = pl.ds(pl.multiple_of(c * R + kk * HF + yy * Q + j * step, step), step)
            x = S["ys"][c, m, :].astype(F32) + S["ry"][c, r, :].astype(F32)
            if s == 0:
                xhat, inv, y = norm(S["tok"][o, :].astype(F32) + x, 0)
                S["xh1"][c, r, :] = xhat
                S["rs1"][c, r, :] = inv
                S["res"][c, r, :] = y
            elif s == 1:
                xhat, inv, y = norm(S["res"][c, r, :] + x, 1)
                S["xh2"][c, r, :] = xhat
                S["rs2"][c, r, :] = inv
                S["res"][c, r, :] = y
            elif s == 2:
                xhat, inv, y = norm(S["res"][c, r, :] + x, 2)
                S["outs"][o, :] = y.astype(BF)
                rid = (c * R + kk * HF + yy * Q + j * step
                       + lax.broadcasted_iota(jnp.int32, (step, width), 0))
                seed = jnp.where(rid < dec, S["cot"][c, r, :].astype(F32), 0.0)
                y = norm_back(seed, xhat, inv, 2)
                S["res"][c, r, :] = y
            elif s == 3:
                y = norm_back(S["res"][c, r, :] + x, S["xh2"][c, r, :], S["rs2"][c, r, :], 1)
                S["res"][c, r, :] = y
            elif s == 4:
                y = norm_back(S["res"][c, r, :] + x, S["xh1"][c, r, :], S["rs1"][c, r, :], 0)
                S["res"][c, r, :] = y
            elif s == 5:
                y = S["res"][c, r, :] + x
            else:
                y = x
            buf[o, :] = y.astype(BF)
            return carry
        lax.fori_loop(0, Q // step, body, 0)
        gather(buf, c, 0, 2).start()
        gather(buf, c, 1, 2).start()

    def p3(s, c):
        gather(lows[s], c, 0, 2).wait()
        gather(lows[s], c, 2, 2).start()

    def p4(s, c):
        gather(lows[s], c, 1, 2).wait()
        gather(lows[s], c, 2, 2).wait()

    def grad_piece(g, i):
        n = pl.ds(pl.multiple_of(i * PIECE, PIECE), PIECE)
        r = pl.ds(pl.multiple_of((g * CHUNKS + i) * PIECE, PIECE), PIECE)
        if g == 0:
            S["gbuf"][r, :] = tm(S["hid"][:, n], S["low2"][...]).astype(BF)
        elif g == 1:
            S["gbuf"][r, :] = tm(S["low1"][:, n], S["slope"][...]).astype(BF)
        else:
            if g == 2:
                a, b, d = S["low0"], S["mem"], S["low3"]
                x, y, z, w = S["cq"], S["ck"], S["cv"], S["cmixed"]
            else:
                a, b, d = S["tok"], S["tok"], S["low4"]
                x, y, z, w = S["q"], S["k"], S["v"], S["mixed"]
            S["gbuf"][r, 0 * inner:1 * inner] = tm(a[:, n], x[...]).astype(BF)
            S["gbuf"][r, 1 * inner:2 * inner] = tm(b[:, n], y[...]).astype(BF)
            S["gbuf"][r, 2 * inner:3 * inner] = tm(b[:, n], z[...]).astype(BF)
            S["gbuf"][r, 3 * inner:4 * inner] = tm(w[...], d[:, n]).astype(BF)

    def weight(step, p):
        if bits < 2 or step > 1:
            return 1 << step
        swap = lax.rem(lax.shift_right_logical(SWAPPED, p), 2)
        return 1 + swap if step == 0 else 2 - swap

    def start_of(step, p):
        at = p * PIECE
        for j in range(step):
            if sizes[j][1]:
                at = at + side(weight(j, p)) * sizes[j][0]
        return at

    def piece_rows(at, n):
        return pl.ds(pl.multiple_of(at, n), n)

    def reduce_copy(step, p):
        n, halve = sizes[step]
        w = weight(step, p)
        at = start_of(step, p)
        if halve:
            at = at + (1 - side(w)) * n
        slot = lax.rem(p, RING)
        return pltpu.make_async_remote_copy(
            src_ref=S["gbuf"].at[piece_rows(at, n)], dst_ref=S[f"dr{step}"].at[slot],
            send_sem=S["dssem"].at[step, slot], recv_sem=S["drsem"].at[step, slot],
            device_id=dp_peer(w), device_id_type=MESH)

    def reduce_add(step, p):
        n, halve = sizes[step]
        at = start_of(step + 1, p)
        slot = lax.rem(p, RING)
        block = min(32, n)

        def body(j, carry):
            r = pl.ds(pl.multiple_of(at + j * block, block), block)
            m = pl.ds(pl.multiple_of(j * block, block), block)
            S["gbuf"][r, :] = (S["gbuf"][r, :].astype(F32)
                               + S[f"dr{step}"][slot, m, :].astype(F32)).astype(BF)
            return carry
        lax.fori_loop(0, n // block, body, 0)

    halved = sum(1 for _, h in sizes if h)
    steps = bits + halved

    def gather_copy(step, p):
        n, _ = sizes[step]
        r = S["gbuf"].at[piece_rows(start_of(step + 1, p), n)]
        slot = lax.rem(p, RING)
        return pltpu.make_async_remote_copy(
            src_ref=r, dst_ref=S["ag"].at[slot] if step == halved - 1 else r,
            send_sem=S["dssem"].at[bits + step, slot], recv_sem=S["drsem"].at[bits + step, slot],
            device_id=dp_peer(weight(step, p)), device_id_type=MESH)

    def gather_end(step, p):
        gather_copy(step, p).wait()
        if step == halved - 1:
            n, _ = sizes[step]
            at = start_of(step, p) + (1 - side(weight(step, p))) * n
            S["gbuf"][piece_rows(at, n), :] = S["ag"][lax.rem(p, RING)]

    def gather_begin(step, p):
        if step < halved - 1:
            pl.semaphore_wait(S["freed"].at[step, lax.rem(p, RING)], 1)
        gather_copy(step, p).start()

    def result_copies(p, ff):
        r = pl.ds(pl.multiple_of(p * PIECE, PIECE), PIECE)
        if ff:
            return [pltpu.make_async_copy(S["gbuf"].at[r], gf_h.at[r], S["gsem"].at[0, p])]
        g = lax.div(p - 2 * CHUNKS, CHUNKS)
        n = pl.ds(pl.multiple_of(lax.rem(p, CHUNKS) * PIECE, PIECE), PIECE)
        block = [S["gbuf"].at[r, pl.ds(j * inner, inner)] for j in range(4)]
        return [pltpu.make_async_copy(block[j], gq_h.at[g, j, n], S["gsem"].at[j, p])
                for j in range(3)] + [
            pltpu.make_async_copy(block[3], go_h.at[g, :, n], S["gsem"].at[3, p])]

    def dp_step(k, p):
        if 1 <= k <= bits:
            reduce_copy(k - 1, p).wait()
            if k < halved:
                pl.semaphore_signal(S["freed"].at[k - 1, lax.rem(p, RING)], inc=1,
                                    device_id=dp_peer(weight(k - 1, p)), device_id_type=MESH)
            reduce_add(k - 1, p)
        elif k > bits:
            gather_end(halved - (k - bits), p)
        if k < bits:
            reduce_copy(k, p).start()
        elif k < steps:
            gather_begin(halved - 1 - (k - bits), p)
        else:
            @pl.when(p < 2 * CHUNKS)
            def _():
                for x in result_copies(p, True):
                    x.start()

            @pl.when(p >= 2 * CHUNKS)
            def _():
                for x in result_copies(p, False):
                    x.start()

    waits = WAITS if steps == len(WAITS) else (2,) * steps
    lag = [sum(waits[:k]) for k in range(steps + 1)]
    FIRST = 2 * CHUNKS
    GAP = FIRST + 4
    LAST = GAP + 4 * CHUNKS - 2

    def dp_slot(m):
        for k in ORDER if steps == len(WAITS) else range(steps + 1):
            e = m - lag[k]
            early = e < FIRST
            p = jnp.where(early, e, FIRST + lax.div(e - GAP, 2))

            @pl.when((e >= 0) & (e <= LAST)
                     & (early | ((e >= GAP) & (lax.rem(e, 2) == 0))))
            def _(k=k, p=p):
                dp_step(k, p)

    peers = [core, ypar] + [dp_peer(1 << j) for j in range(bits)]

    def vec_copy(k):
        return pltpu.make_async_remote_copy(
            src_ref=S["vsum"], dst_ref=S["vrec"].at[k], send_sem=S["vssem"].at[k],
            recv_sem=S["vrsem"].at[k], device_id=peers[k], device_id_type=MESH)

    def vec_step(k):
        if k == 0:
            S["vsum"][...] = jnp.sum(S["vacc"][...], axis=1)
        else:
            vec_copy(k - 1).wait()
            S["vsum"][...] += S["vrec"][k - 1]
        if k < len(peers):
            vec_copy(k).start()

    def chunk_of(s, i):
        return i if s <= 4 else CHUNKS - 1 - i

    def lagged(i, n, fn, s):
        def now():
            fn(s, chunk_of(s, i - n))

        def before():
            fn(s - 1, chunk_of(s - 1, i - n + CHUNKS))
        fresh = s in (0, 5)
        if isinstance(i, int):
            if i >= n:
                now()
            elif not fresh:
                before()
            return
        pl.when(i >= n)(now)
        if not fresh:
            pl.when(i < n)(before)

    def phases(i, s):
        lagged(i, 1, lambda _, c: p1(c), s)
        lagged(i, 2, p2, s)
        lagged(i, 3, p3, s)

    def ff_piece(m):
        @pl.when(m < CHUNKS)
        def _():
            grad_piece(0, m)

        @pl.when((m >= CHUNKS) & (m < FIRST))
        def _():
            grad_piece(1, m - CHUNKS)

    def ff_slot(m):
        ff_piece(m)
        dp_slot(m)

    def slot(i, s):
        c = chunk_of(s, i)
        if s > 0:
            p4(s - 1, c)
        if s == 5:
            gather(S["outs"], c, 0, 5).start()
            gather(S["outs"], c, 1, 5).start()

        def middle():
            phases(i, s)
            if s == 4:
                ff_slot(2 * i + 2)
            elif s > 4:
                grad_piece(s - 3, i)
                dp_slot(GAP + 2 * CHUNKS * (s - 5) + 2 * i)
            if s == 6:
                gather(S["outs"], c, 0, 5).wait()
                gather(S["outs"], c, 2, 5).start()
                for k in range(CHUNKS):
                    @pl.when(i == k)
                    def _(k=k):
                        vec_step(k)
        compute(s, c, middle)
        if s == 0 and i == 0:
            pl.semaphore_wait(barrier, 2 + bits)
        p0(c)
        if s == 4:
            ff_slot(2 * i + 3)
        elif s > 4:
            dp_slot(GAP + 2 * CHUNKS * (s - 5) + 2 * i + 1)

    def drain(s, t):
        a, b, d = (chunk_of(s, i) for i in (1, 2, 3))

        @pl.when(t == 0)
        def _():
            p3(s, a)
            p2(s, b)
            p1(d)

        @pl.when(t == 1)
        def _():
            p3(s, b)
            p2(s, d)

        @pl.when(t == 2)
        def _():
            p3(s, d)

    wait_for("tok", "wk", "wv", "wq", "wo")
    for n in INPUTS[5:]:
        loads[n].start()
    for x in cots:
        x.start()
    for i in range(CHUNKS):
        slot(i, 0)
        if i == 0:
            wait_for("mem", "cwk", "cwv")
        project(i, S["mem"], S["cwk"], S["cwv"], S["ck"], S["cv"], S["ckt"], S["cvt"])

    for s in range(1, STAGES):
        if s == 1:
            wait_for("cwq", "cwo")
        if s == 2:
            wait_for("win", "wout")
        if s == 4:
            def ahead(m, carry):
                grad_piece(0, m)
                dp_slot(m)
                return carry
            lax.fori_loop(0, 2, ahead, 0)
        if s in (4, 5):
            S["dk"][...] = jnp.zeros(S["dk"].shape, F32)
            S["dv"][...] = jnp.zeros(S["dv"].shape, F32)

        def body(i, carry, s=s):
            slot(i, s)
            return carry
        lax.fori_loop(0, CHUNKS, body, 0)
        if s == 4:
            S["ck"][...] = (S["dk"][...] * scale).astype(BF)
            S["cv"][...] = S["dv"][...].astype(BF)

            def between(t, carry):
                drain(4, t)

                @pl.when(t < 2)
                def _():
                    dp_slot(FIRST + 2 + t)
                return carry
            lax.fori_loop(0, 3, between, 0)

    last = STAGES - 1
    tail = LAST + 2
    outputs = [pltpu.make_async_copy(a, b, S["osem"].at[j])
               for j, (a, b) in enumerate(((S["outs"], out_h), (lows[5], tg_h), (lows[6], mg_h)))]

    def ending(m, carry):
        t = m - tail
        dp_slot(m)
        drain(last, t)

        @pl.when(t == 0)
        def _():
            for c in range(CHUNKS):
                gather(S["outs"], c, 1, 5).wait()
                gather(S["outs"], c, 2, 5).wait()
            outputs[0].start()
            outputs[1].start()

        @pl.when(t == 3)
        def _():
            for c in range(CHUNKS):
                p4(last, c)
            outputs[2].start()
        for k in range(CHUNKS, len(peers) + 1):
            @pl.when(t == k - CHUNKS)
            def _(k=k):
                vec_step(k)
        return carry
    lax.fori_loop(tail, LAST + lag[-1] + 1, ending, 0)
    vg_h[...] = S["vsum"][...]

    def finish(p, carry, ff):
        for x in result_copies(p, ff):
            x.wait()
        return carry
    lax.fori_loop(0, 2 * CHUNKS, lambda p, x: finish(p, x, True), 0)
    lax.fori_loop(2 * CHUNKS, pieces, lambda p, x: finish(p, x, False), 0)
    for x in outputs:
        x.wait()


def widen(out, tg, mg, gf, gq, go, vg):
    parts = 8
    width = out.shape[1]
    hidden = gf.shape[0] // 2
    inner = gq.shape[-1]
    rows, slots = out.shape[0], mg.shape[0]

    def tall(n, columns):
        return pl.BlockSpec((n // parts, columns), lambda i: (i, 0))

    shapes = [jax.ShapeDtypeStruct((rows, width), BF)]
    shapes += [jax.ShapeDtypeStruct(x.shape, F32) for x in (tg, mg)]
    out_specs = [tall(rows, width), tall(rows, width), tall(slots, width)]
    for _ in range(2):
        shapes += [jax.ShapeDtypeStruct((width, inner), F32)] * 3
        shapes += [jax.ShapeDtypeStruct((inner, width), F32)]
        out_specs += [tall(width, inner)] * 3 + [tall(inner, width)]
    shapes += [jax.ShapeDtypeStruct((hidden, width), F32)] * 2
    out_specs += [tall(hidden, width)] * 2
    shapes += [jax.ShapeDtypeStruct((width,), F32)] * 6
    out_specs += [pl.BlockSpec((width,), lambda i: (0,))] * 6

    def body(o, t, m, q, w, f, v, *res):
        res[0][...] = o[...]
        res[1][...] = t[...].astype(F32)
        res[2][...] = m[...].astype(F32)
        for a, g in enumerate((1, 0)):
            for j in range(3):
                res[3 + 4 * a + j][...] = q[g, j].astype(F32)
            res[6 + 4 * a][...] = w[g].astype(F32)
        for g in range(2):
            res[11 + g][...] = f[g].astype(F32)

        @pl.when(pl.program_id(0) == 0)
        def _():
            for j in range(6):
                res[13 + j][...] = v[j]

    return pl.pallas_call(
        body, out_shape=tuple(shapes), grid=(parts,),
        in_specs=[
            tall(rows, width), tall(rows, width), tall(slots, width),
            pl.BlockSpec((2, 3, width // parts, inner), lambda i: (0, 0, i, 0)),
            pl.BlockSpec((2, inner // parts, width), lambda i: (0, i, 0)),
            pl.BlockSpec((2, hidden // parts, width), lambda i: (0, i, 0)),
            pl.BlockSpec((8, width), lambda i: (0, 0)),
        ],
        out_specs=tuple(out_specs), name="widen",
        compiler_params=pltpu.CompilerParams(dimension_semantics=("arbitrary",)),
    )(out, tg, mg, gq, go, gf.reshape(2, hidden, width), vg)


def shards(
    tokens, memory, decoder_length, memory_length,
    self_query, self_key, self_value, self_output, self_gain, self_bias,
    cross_query, cross_key, cross_value, cross_output, cross_gain, cross_bias,
    feed_in, feed_out, feed_gain, feed_bias, cotangent,
):
    rows, width = tokens.shape
    slots = memory.shape[0]
    inner = self_query.shape[1]
    hidden = feed_in.shape[1]
    vecs = [x.reshape(1, width) for x in (
        self_gain, self_bias, cross_gain, cross_bias, feed_gain, feed_bias)]
    copies = lax.axis_size("dp")
    scratch = layout(rows, slots, width, inner, hidden, copies)
    names = tuple(scratch)
    given = dict(tok=tokens, mem=memory, wq=self_query, wk=self_key, wv=self_value,
                 wo=self_output, cwq=cross_query, cwk=cross_key, cwv=cross_value,
                 cwo=cross_output, win=feed_in, wout=feed_out)
    any_spec = pl.BlockSpec(memory_space=pl.ANY)

    def kernel(*refs):
        layer_kernel(names, copies, *refs)

    out, tg, mg, gf, gq, go, vg = pl.pallas_call(
        kernel,
        out_shape=(
            jax.ShapeDtypeStruct((rows, width), BF),
            jax.ShapeDtypeStruct((rows, width), BF),
            jax.ShapeDtypeStruct((slots, width), BF),
            jax.ShapeDtypeStruct((2 * hidden, width), BF),
            jax.ShapeDtypeStruct((2, 3, width, inner), BF),
            jax.ShapeDtypeStruct((2, inner, width), BF),
            jax.ShapeDtypeStruct((8, width), F32),
        ),
        in_specs=[pl.BlockSpec(memory_space=pltpu.SMEM)] * 2
        + [pl.BlockSpec(memory_space=pltpu.VMEM)] * 6 + [any_spec] * (len(INPUTS) + 1),
        out_specs=(any_spec,) * 6 + (pl.BlockSpec(memory_space=pltpu.VMEM),),
        scratch_shapes=list(scratch.values()),
        compiler_params=pltpu.CompilerParams(
            collective_id=0, has_side_effects=True, vmem_limit_bytes=67043328),
        name="layer",
    )(decoder_length, memory_length, *vecs, *[given[n] for n in INPUTS], cotangent)

    wide = widen(out, tg, mg, gf, gq, go, vg)
    return (
        *wide[:3],
        *wide[3:7], wide[13], wide[14],
        *wide[7:11], wide[15], wide[16],
        wide[12], wide[11], wide[17], wide[18],
    )


def solution(mesh):
    rows = P("dp", None)
    tail = P(None, "tensor")
    head = P("tensor", None)
    whole = P()
    return jax.shard_map(
        shards,
        mesh=mesh,
        in_specs=(
            rows, rows, P("dp"), P("dp"),
            tail, tail, tail, head, whole, whole,
            tail, tail, tail, head, whole, whole,
            tail, head, whole, whole, rows,
        ),
        out_specs=(
            rows, rows, rows,
            tail, tail, tail, head, whole, whole,
            tail, tail, tail, head, whole, whole,
            tail, head, whole, whole,
        ),
        check_vma=False,
    )
```
